128 devices in a mesh: grp: 4 (over z), dev: 32 (over y, x, core).
Axes of the slice: x: 4, y: 4, z: 4, core: 2. Of those that a mesh axis runs over, the one named last changes fastest.
Arguments:
- old_state: float32 [32768, 4, 512], P(('grp', 'dev')), may hold values from -6 to 6
- dest_row: int32 [32768], P(('grp', 'dev')), may hold values from -1 to 16383, as said below
- neighbours: int32 [6, 16384], P(None, ('grp', 'dev')), may hold values from 0 to 16383, as said below
- orientation: int32 [6, 16384], P(None, ('grp', 'dev')), may hold values from 0 to 7
- wall_flags: int32 [6, 16384], P(None, ('grp', 'dev')), may hold values from 0 to 1, as said below
- bulk_modulus: float32 [16384], P(('grp', 'dev')), may hold values from 0.5 to 2
- density: float32 [16384], P(('grp', 'dev')), may hold values from 0.5 to 2
Outputs:
- tendency: float32 [16384, 4, 512], P(('grp', 'dev'))
The draws below stay inside these ranges and needn't reach their ends.
Inputs may be any that keep to these rules, and one draw needn't show every extreme that they name: `dest_row`: each of the 16384 new rows appears exactly once. On half of the devices every slot is used, on the others every slot is -1. The slots of one device whose new rows lie on one device number either 0 or 8. The elements form a grid of 16 x 32 x 32 cubes along x, y, z, cut into blocks of 4 x 4 x 8, faces 0 to 5 looking to -x, +x, -y, +y, -z, +z; a face on the grid's outside has the row itself as neighbour. If neighbours[f, r] = m differs from r then neighbours[f xor 1, m] = r. Each device holds the rows of one whole block, in rows 128 * i to 128 * (i + 1) - 1 for device index i = g * 32 + d (g of grp, d of dev); which block lies on which device is arbitrary. One device's rows and faces have at most 32 neighbours on any one other device. wall_flags[f, r] is 1 exactly where neighbours[f, r] = r.
All inputs are finite; a program needn't handle non-finite values.
Results may differ from the reference program's by a relative error of at most 0.0001.
Values sent between devices are 32-bit elements; how exact they have to be, the bound alone decides.
No kernel may reach another device: no remote copies, remote signals or barrier semaphores. Data moves between devices by JAX's collectives and lax.ppermute only.
A program may use at most 128 MiB of HBM per device.

```python
import math
import jax
import jax.numpy as jnp
import numpy as np
from jax import lax

NP = 8
BX = 4
BY = 4
BZ = 8
PZ = 4
PIECES = 16
NODES = 512
PX = 4
PY = 8
ELEM_DEV = 128
ELEMS = 16384
CAP = 8
OLD_CAP = 256
OLD_ALL = 32768


def grid_rows(key):
    device_count = PX * PY * PZ
    key_list = jax.random.split(jax.random.fold_in(key, 11), device_count)
    box_orders = jax.vmap(lambda sub_key: jax.random.permutation(sub_key, ELEM_DEV))(key_list)
    block_order = jax.random.permutation(jax.random.fold_in(key, 14), device_count)
    coord_x, coord_y, coord_z = jnp.meshgrid(jnp.arange(BX * PX), jnp.arange(BY * PY), jnp.arange(BZ * PZ), indexing='ij')
    block_id = coord_x // BX * (PY * PZ) + coord_y // BY * PZ + coord_z // BZ
    owner_dev = block_order[block_id]
    local_id = coord_x % BX * (BY * BZ) + coord_y % BY * BZ + coord_z % BZ
    row_grid = owner_dev * ELEM_DEV + box_orders[owner_dev, local_id]
    return row_grid.astype(jnp.int32)


def face_shift(row_grid, face_id):
    axis_id = face_id // 2
    extent = row_grid.shape[axis_id]
    position = lax.broadcasted_iota(jnp.int32, row_grid.shape, axis_id)
    if face_id % 2 == 0:
        first_slab = lax.slice_in_dim(row_grid, 0, 1, axis=axis_id)
        rest_slab = lax.slice_in_dim(row_grid, 0, extent - 1, axis=axis_id)
        shifted = jnp.concatenate([first_slab, rest_slab], axis=axis_id)
        at_edge = position == 0
    else:
        rest_slab = lax.slice_in_dim(row_grid, 1, extent, axis=axis_id)
        first_slab = lax.slice_in_dim(row_grid, extent - 1, extent, axis=axis_id)
        shifted = jnp.concatenate([rest_slab, first_slab], axis=axis_id)
        at_edge = position == extent - 1
    return (shifted, at_edge)


def draw_neighbours(key, part):
    row_grid = grid_rows(key)
    result = jnp.zeros((6, ELEM_DEV * PX * PY * PZ), jnp.int32)
    for face_id in range(6):
        shifted, at_edge = face_shift(row_grid, face_id)
        result = result.at[face_id, row_grid.reshape(-1)].set(shifted.reshape(-1))
    return result


def draw_wall_flags(key, part):
    row_grid = grid_rows(key)
    result = jnp.zeros((6, ELEM_DEV * PX * PY * PZ), jnp.int32)
    for face_id in range(6):
        shifted, at_edge = face_shift(row_grid, face_id)
        result = result.at[face_id, row_grid.reshape(-1)].set(at_edge.reshape(-1).astype(jnp.int32))
    return result


def draw_dest_row(key, part):
    device_count = PX * PY * PZ
    source_order = jax.random.permutation(jax.random.fold_in(key, 12), device_count)
    heavy_src = source_order[:device_count // 2]
    run_length = 2 * PIECES
    piece_ids = jnp.arange(device_count * PIECES)
    sources = jnp.repeat(heavy_src, run_length, total_repeat_length=device_count * PIECES)
    target_dev = piece_ids % device_count
    piece_number = piece_ids // device_count
    within = piece_ids % run_length
    slot_keys = jax.random.split(jax.random.fold_in(key, 13), device_count)
    slot_orders = jax.vmap(lambda sub_key: jax.random.permutation(sub_key, OLD_CAP))(slot_keys)
    offsets = jnp.arange(CAP)
    new_rows = target_dev[:, None] * ELEM_DEV + piece_number[:, None] * CAP + offsets[None, :]
    old_rows = sources[:, None] * OLD_CAP + slot_orders[sources[:, None], within[:, None] * CAP + offsets[None, :]]
    empty_rows = jnp.full((device_count * OLD_CAP,), -1, jnp.int32)
    return empty_rows.at[old_rows.reshape(-1)].set(new_rows.reshape(-1).astype(jnp.int32))


def with_ends(array, key, least, top_value):
    longest = array.shape.index(max(array.shape))
    spots = []
    for shift in (0, 1):
        where = [jax.random.randint(jax.random.fold_in(key, axis), (), 0, length) for axis, length in enumerate(array.shape)]
        where[longest] = (where[longest] + shift) % array.shape[longest]
        spots.append(tuple(where))
    return array.at[spots[0]].set(least).at[spots[1]].set(top_value)


def levels(key, shape, cuts, smallest, largest):
    def one(axis_at, blocks):
        heights = jax.random.uniform(jax.random.fold_in(jax.random.fold_in(key, 6), axis_at), (blocks,), jnp.float32, smallest / len(cuts), largest / len(cuts))
        return jnp.repeat(jnp.exp(heights), shape[axis_at] // blocks).reshape((-1,) + (1,) * (len(shape) - axis_at - 1))

    level = one(*cuts[0])
    for cut in cuts[1:]:
        level = level * one(*cut)
    return level


def centred(rng, shape, spread, most, shards=(), kind=jnp.bfloat16):
    values = spread * jax.random.normal(rng, shape, jnp.float32)
    if shards:
        values = values * levels(rng, shape, shards, -0.22, 0.18)
    return jnp.clip(values, -most, most).astype(kind)


def setup_inputs(seed: int = 0) -> dict:
    splits = jax.random.split(jax.random.key(seed), 8)
    old_state = centred(splits[0], (OLD_ALL, 4, NODES), 1.0, 6.0, ((0, 128),), jnp.float32)
    dest_row = draw_dest_row(jax.random.fold_in(splits[7], 71), 0)
    neighbours = draw_neighbours(jax.random.fold_in(splits[7], 71), 0)
    orientation = with_ends(jax.random.randint(splits[3], (6, ELEMS), 0, 8), jax.random.fold_in(splits[3], 1), 0, 7).astype(jnp.int32)
    wall_flags = draw_wall_flags(jax.random.fold_in(splits[7], 71), 0)
    bulk_modulus = jnp.clip(jnp.exp(math.log(2.0) - 1.3862944 * jax.random.uniform(splits[5], (ELEMS,), jnp.float32) ** levels(splits[5], (ELEMS,), ((0, 128),), -0.2, 0.2)), 0.5, 2.0)
    density = jnp.clip(jnp.exp(math.log(2.0) - 1.3862944 * jax.random.uniform(splits[6], (ELEMS,), jnp.float32) ** levels(splits[6], (ELEMS,), ((0, 128),), -0.2, 0.2)), 0.5, 2.0)
    return {"old_state": old_state, "dest_row": dest_row, "neighbours": neighbours, "orientation": orientation, "wall_flags": wall_flags, "bulk_modulus": bulk_modulus, "density": density}


metric_scale = 0.25

def gll_tables(poly_order):
    num_points = poly_order + 1
    points = -np.cos(np.pi * np.arange(num_points) / poly_order)
    legendre = np.zeros((num_points, num_points))
    for sweeps in range(101):
        legendre[:, 0] = 1.0
        legendre[:, 1] = points
        for degree in range(2, num_points):
            legendre[:, degree] = ((2 * degree - 1) * points * legendre[:, degree - 1] - (degree - 1) * legendre[:, degree - 2]) / degree
        if sweeps < 100:
            points = points - (points * legendre[:, poly_order] - legendre[:, poly_order - 1]) / (num_points * legendre[:, poly_order])
    end_values = legendre[:, poly_order]
    weights = 2.0 / (poly_order * num_points * end_values ** 2)
    distance = points[:, None] - points[None, :] + np.eye(num_points)
    derivative = end_values[:, None] / end_values[None, :] / distance
    derivative = derivative * (1.0 - np.eye(num_points))
    derivative[0, 0] = -poly_order * num_points / 4.0
    derivative[poly_order, poly_order] = poly_order * num_points / 4.0
    return (points, weights, derivative)

def face_index(face_id):
    picked = [slice(None), slice(None), slice(None)]
    picked[face_id // 2] = 0 if face_id % 2 == 0 else NP - 1
    return tuple(picked)

def face_traces(volume):
    return jnp.stack([volume[(slice(None), slice(None)) + face_index(face_id)] for face_id in range(6)])

def orient_trace(values, orient_code):
    shaped = orient_code[:, None, None, None]
    values = jnp.where(shaped % 2 == 1, values[:, :, ::-1, :], values)
    values = jnp.where(shaped // 2 % 2 == 1, values[:, :, :, ::-1], values)
    return jnp.where(shaped >= 4, jnp.swapaxes(values, 2, 3), values)

def derivative_along(scalar_field, matrix, axis_id):
    einsum_forms = ['ai,eijk->eajk', 'aj,eijk->eiak', 'ak,eijk->eija']
    return jnp.einsum(einsum_forms[axis_id], matrix, scalar_field, precision=lax.Precision.HIGHEST)

def right_side(volume, inner_faces, outer_faces, outer_impedance, orientation, wall_flags, bulk_modulus, density):
    points, weights, derivative = gll_tables(NP - 1)
    matrix = jnp.asarray(derivative, jnp.float32)
    lift_factor = metric_scale / float(weights[0])
    bulk_vol = bulk_modulus[:, None, None, None]
    dens_vol = density[:, None, None, None]
    divergence = derivative_along(volume[:, 1], matrix, 0) + derivative_along(volume[:, 2], matrix, 1) + derivative_along(volume[:, 3], matrix, 2)
    pieces_list = [-metric_scale * bulk_vol * divergence]
    for axis_id in range(3):
        pieces_list.append(-(metric_scale / dens_vol) * derivative_along(volume[:, 0], matrix, axis_id))
    result = jnp.stack(pieces_list, axis=1)
    inner_impedance = jnp.sqrt(bulk_modulus * density)
    for face_id in range(6):
        axis_id = face_id // 2
        normal_sign = 2.0 * (face_id % 2) - 1.0
        own_face = inner_faces[face_id]
        far_face = orient_trace(outer_faces[face_id], orientation[face_id])
        is_wall = wall_flags[face_id] == 1
        wall_face = is_wall[:, None, None]
        press_in = own_face[:, 0]
        normal_in = normal_sign * own_face[:, 1 + axis_id]
        press_out = jnp.where(wall_face, press_in, far_face[:, 0])
        normal_out = jnp.where(wall_face, -normal_in, normal_sign * far_face[:, 1 + axis_id])
        imped_in = inner_impedance[:, None, None]
        imped_out = jnp.where(is_wall, inner_impedance, outer_impedance[face_id])[:, None, None]
        imped_sum = imped_in + imped_out
        press_star = (imped_out * press_in + imped_in * press_out + imped_in * imped_out * (normal_in - normal_out)) / imped_sum
        normal_star = (imped_in * normal_in + imped_out * normal_out + press_in - press_out) / imped_sum
        result = result.at[(slice(None), 0) + face_index(face_id)].add(-lift_factor * bulk_modulus[:, None, None] * (normal_star - normal_in))
        result = result.at[(slice(None), 1 + axis_id) + face_index(face_id)].add(-(normal_sign * lift_factor) * (press_star - press_in) / density[:, None, None])
    return result.reshape(result.shape[0], 4, -1)

def reference(old_state, dest_row, neighbours, orientation, wall_flags, bulk_modulus, density):
    elem_count = bulk_modulus.shape[0]
    target = jnp.where(dest_row >= 0, dest_row, elem_count)
    new_state = jnp.zeros((elem_count, 4, old_state.shape[2]), jnp.float32).at[target].set(old_state, mode='drop')
    volume = new_state.reshape(elem_count, 4, NP, NP, NP)
    inner_faces = face_traces(volume)
    outer_faces = jnp.stack([inner_faces[face_id ^ 1][neighbours[face_id]] for face_id in range(6)])
    impedance = jnp.sqrt(bulk_modulus * density)
    outer_impedance = impedance[neighbours]
    return right_side(volume, inner_faces, outer_faces, outer_impedance, orientation, wall_flags, bulk_modulus, density)
```

```python
import jax
import jax.numpy as jnp
import numpy as np
from jax import lax
from jax.experimental import pallas as pl
from jax.experimental.pallas import tpu as pltpu
from jax.sharding import PartitionSpec as P

NP = 8
DEVS = 128
LANES = 128
AXES = ("grp", "dev")
metric_scale = 0.25
F32 = jnp.float32
I32 = jnp.int32
BF16 = jnp.bfloat16
VMEM = pltpu.MemorySpace.VMEM
SMEM = pltpu.MemorySpace.SMEM
ANY = pl.ANY


def gll_tables(poly_order):
    num_points = poly_order + 1
    points = -np.cos(np.pi * np.arange(num_points) / poly_order)
    legendre = np.zeros((num_points, num_points))
    for sweeps in range(101):
        legendre[:, 0] = 1.0
        legendre[:, 1] = points
        for degree in range(2, num_points):
            legendre[:, degree] = (
                (2 * degree - 1) * points * legendre[:, degree - 1]
                - (degree - 1) * legendre[:, degree - 2]
            ) / degree
        if sweeps < 100:
            points = points - (points * legendre[:, poly_order] - legendre[:, poly_order - 1]) / (
                num_points * legendre[:, poly_order]
            )
    end_values = legendre[:, poly_order]
    weights = 2.0 / (poly_order * num_points * end_values**2)
    distance = points[:, None] - points[None, :] + np.eye(num_points)
    derivative = end_values[:, None] / end_values[None, :] / distance
    derivative = derivative * (1.0 - np.eye(num_points))
    derivative[0, 0] = -poly_order * num_points / 4.0
    derivative[poly_order, poly_order] = poly_order * num_points / 4.0
    return (points, weights, derivative)


POINTS, WEIGHTS, DERIV = gll_tables(NP - 1)
DERIV = DERIV.astype(np.float32)
LIFT = metric_scale / float(WEIGHTS[0])


def derivative_tables():
    eye2, eye8 = np.eye(2, dtype=np.float32), np.eye(8, dtype=np.float32)
    along_y = np.kron(eye2, np.kron(DERIV.T, eye8))
    along_z = np.kron(eye2, np.kron(eye8, DERIV.T))
    side = np.concatenate([along_y, along_z], axis=1)
    stacked = np.concatenate([along_y, along_z], axis=0)
    coef = np.zeros((4, 4, 2, LANES), np.float32)
    for out_chunk in range(4):
        for in_chunk in range(4):
            for half in range(2):
                lanes = slice(64 * half, 64 * half + 64)
                coef[out_chunk, in_chunk, 0, lanes] = DERIV[2 * out_chunk + half, 2 * in_chunk + half]
                coef[out_chunk, in_chunk, 1, lanes] = DERIV[
                    2 * out_chunk + half, 2 * in_chunk + 1 - half
                ]
    return side, stacked, coef.reshape(32, LANES)


SIDE, STACKED, COEF = derivative_tables()


def iota(shape, axis):
    return lax.broadcasted_iota(I32, shape, axis)


def small_dot(left, right):
    return jnp.dot(left.astype(BF16), right.astype(BF16), preferred_element_type=F32)


def split3(value):
    high = value.astype(BF16)
    rest = value - high.astype(F32)
    middle = rest.astype(BF16)
    low = (rest - middle.astype(F32)).astype(BF16)
    return high, middle, low


def pick_dot(pick, value):
    pick = pick.astype(BF16)
    high, middle, low = split3(value)
    total = jnp.dot(pick, high, preferred_element_type=F32)
    total = total + jnp.dot(pick, middle, preferred_element_type=F32)
    return total + jnp.dot(pick, low, preferred_element_type=F32)


def order_kernel(dest_ref, info_ref, pos_ref):
    dest = dest_ref[...]
    sub = iota((LANES, LANES), 0)
    lane = iota((LANES, LANES), 1)
    diag = sub == lane
    key_row, key_col, dev_row, dev_col, lab_col = [], [], [], [], []
    for half in range(2):
        row = jnp.broadcast_to(dest[half : half + 1, :], (LANES, LANES))
        owner = (row >> 7).astype(F32)
        local = (row & 127).astype(F32) + 1.0
        key = owner * 256.0 + (lane + 128 * half).astype(F32)
        key_row.append(key)
        dev_row.append(owner)
        key_col.append(jnp.sum(jnp.where(diag, key, 0.0), axis=1, keepdims=True))
        dev_col.append(jnp.sum(jnp.where(diag, owner, 0.0), axis=1, keepdims=True))
        lab_col.append(jnp.sum(jnp.where(diag, local, 0.0), axis=1, keepdims=True))
    labels = jnp.zeros((LANES, LANES), F32)
    targets = jnp.zeros((1, LANES), F32)
    for half in range(2):
        before_col = jnp.zeros((LANES, 1), F32)
        before_row = jnp.zeros((1, LANES), F32)
        for other in range(2):
            before_col = before_col + jnp.sum(
                jnp.where(key_row[other] < key_col[half], 1.0, 0.0), axis=1, keepdims=True
            )
            before_row = before_row + jnp.sum(
                jnp.where(key_col[other] < key_row[half], 1.0, 0.0), axis=0, keepdims=True
            )
        pos_ref[half : half + 1, :] = before_row.astype(I32)
        place = before_col.astype(I32)
        is_target = (place == 8 * lane) & (lane < 32)
        targets = targets + jnp.sum(jnp.where(is_target, dev_col[half], 0.0), axis=0, keepdims=True)
        is_label = (place & 7) == lane - 32
        mine = jnp.where(dev_row[half] == sub.astype(F32), 1.0, 0.0)
        labels = labels + small_dot(mine, jnp.where(is_label, lab_col[half], 0.0))
    info_ref[...] = (labels + targets).astype(I32)


def pack_kernel(pos_ref, dest_ref, state_ref, out_ref):
    @pl.when(dest_ref[0, 0] >= 0)
    def _():
        def one(slot, carry):
            place = pos_ref[slot >> 7, slot & 127]
            start = (place & 7) * 512 + (place >> 3)
            out_ref[pl.ds(start, 16, stride=32), :] = state_ref[pl.ds(pl.multiple_of(slot * 16, 16), 16), :]
            return carry

        lax.fori_loop(0, 256, one, 0, unroll=8)


def table_kernel(me_ref, info_ref, nbr_ref, wall_ref, out_ref, scr):
    sub = iota((LANES, LANES), 0)
    lane = iota((LANES, LANES), 1)
    info = info_ref[...]
    present = jnp.zeros((LANES, LANES), F32)
    for j in range(32):
        present = jnp.where(info[:, j : j + 1] == lane, 1.0, present)
    below = jnp.where(lane < sub, 1.0, 0.0)
    rank = small_dot(below, present)
    target = jnp.clip(info, 0, LANES - 1)
    slot = target * 16 + jnp.take_along_axis(rank.astype(I32), target, axis=1)
    slot = jnp.where(info >= 0, slot, -1)
    out_ref[0:32, :] = slot.astype(F32).T[0:32, :].astype(I32)
    is_source = jnp.broadcast_to(jnp.where(info[:, 32:33] > 0, 1.0, 0.0), (LANES, LANES))
    order = small_dot(below, is_source)
    order_row = jnp.where(is_source > 0.0, order, -1.0).T[0:16, :]
    pick = jnp.where(order_row == iota((16, LANES), 0).astype(F32), 1.0, 0.0)
    out_ref[32:48, :] = small_dot(pick, info.astype(F32)).astype(I32)
    scr[...] = jnp.zeros((8, LANES), F32)
    nbr = nbr_ref[...]
    owner = nbr >> 7
    remote = (owner != me_ref[0]) & (wall_ref[...] == 0)
    scr[0:6, :] = jnp.where(remote, 1.0, 0.0)
    flags = scr[...]
    before = small_dot(flags, jnp.where(sub < lane, 1.0, 0.0))
    out_ref[48:56, :] = jnp.where(flags > 0.0, before, -1.0).astype(I32)
    scr[...] = jnp.full((8, LANES), -1.0, F32)
    scr[0:6, :] = jnp.where(remote, owner, -1).astype(F32)
    out_ref[56:64, :] = jnp.broadcast_to(
        jnp.max(scr[...], axis=1, keepdims=True), (8, LANES)
    ).astype(I32)


def forward_kernel(tab_ref, in_ref, out_ref):
    def one(source, carry):
        @pl.when(tab_ref[0, source] >= 0)
        def _():
            base = pl.multiple_of(source * 32, 32)
            for j in range(32):
                out_ref[pl.ds(tab_ref[j, source], 1), :] = in_ref[pl.ds(base + j, 1), :]

        return carry

    lax.fori_loop(0, DEVS, one, 0)


def half_sign(shape):
    return jnp.where(iota(shape, 1) < 64, -1.0, 1.0)


def arrive_kernel(
    tab_ref, in_ref, rank_ref, bulk_ref, dens_ref, state_ref, press_ref, norm_ref, wave_ref, send_ref, blk, sem
):
    def one(number, carry):
        source = number >> 3
        k = number & 7
        row = tab_ref[32 + source, 32 + k] - 1
        piece = in_ref[pl.ds(k * 256 + source, 16, stride=16), :]
        state_ref[pl.ds(row, 16, stride=128), :] = piece
        return carry

    lax.fori_loop(0, DEVS, one, 0, unroll=8)

    shape = (LANES, LANES)
    lane = iota(shape, 1)
    zed_row = jnp.sqrt(bulk_ref[...] * dens_ref[...])
    diag = iota(shape, 0) == lane
    zed = jnp.sum(jnp.where(diag, jnp.broadcast_to(zed_row, shape), 0.0), axis=1, keepdims=True)
    sign = half_sign(shape)

    def chunk(field, n4):
        start = (n4 * 4 + field) * LANES
        return state_ref[start : start + LANES, :]

    half = lane >> 6
    face_i = (lane >> 3) & 7
    face_b = lane & 7
    from_y = (face_i & 1) * 64 + half * 56 + face_b
    from_z = (face_i & 1) * 64 + face_b * 8 + half * 7
    for axis in range(3):
        values = []
        for field in (0, 1 + axis):
            if axis == 0:
                value = jnp.where(lane < 64, chunk(field, 0), chunk(field, 3))
            else:
                index = from_y if axis == 1 else from_z
                value = jnp.take_along_axis(chunk(field, 0), index, axis=1)
                for n4 in range(1, 4):
                    other = jnp.take_along_axis(chunk(field, n4), index, axis=1)
                    value = jnp.where(face_i >> 1 == n4, other, value)
            values.append(value)
        rows = slice(axis * LANES, axis * LANES + LANES)
        normal = sign * values[1]
        wave = values[0] + zed * normal
        press_ref[rows, :] = values[0]
        norm_ref[rows, :] = normal
        wave_ref[rows, :] = wave
        for side in range(2):
            face = 2 * axis + side
            rank = rank_ref[face : face + 1, :]
            pick = jnp.where(rank == iota((32, LANES), 0), 1.0, 0.0)
            got = pick_dot(pick, wave)
            first, second = got[0:16], got[16:32]
            if side == 0:
                second = pltpu.roll(second, 64, 1)
            else:
                first = pltpu.roll(first, 64, 1)
            block = jnp.where(iota((16, LANES), 1) < 64, first, second)
            for t in range(16):
                blk[face, t] = block[t : t + 1, :]
            rank_col = jnp.sum(
                jnp.where(diag, jnp.broadcast_to(rank, shape).astype(F32), 0.0), axis=1, keepdims=True
            )
            blk[face, 16] = jnp.sum(jnp.where(rank_col == lane.astype(F32), zed, 0.0), axis=0, keepdims=True)
    for face in range(6):
        owner = tab_ref[56 + face, 0]

        @pl.when(owner >= 0)
        def _():
            pltpu.make_async_copy(blk.at[face], send_ref.at[owner], sem.at[face]).start()

    for face in range(6):
        owner = tab_ref[56 + face, 0]

        @pl.when(owner >= 0)
        def _():
            pltpu.make_async_copy(blk.at[face], send_ref.at[owner], sem.at[face]).wait()


def column(row, diag):
    wide = jnp.broadcast_to(row, (LANES, LANES))
    return jnp.sum(jnp.where(diag, wide, 0.0), axis=1, keepdims=True)


def volume_kernel(
    me_ref, state_ref, wave_ref, nbr_ref, wall_ref, orient_ref, bulk_ref, dens_ref, side_ref, stack_ref,
    coef_ref, vol_ref, near_ref, index_ref, zed_ref, pick_ref,
):
    shape = (LANES, LANES)
    lane = iota(shape, 1)
    diag = iota(shape, 0) == lane
    zed_row = jnp.sqrt(bulk_ref[...] * dens_ref[...])
    zed = column(zed_row, diag)
    bulk = column(bulk_ref[...], diag)
    dens = column(dens_ref[...], diag)

    def chunk(field, n4):
        start = (n4 * 4 + field) * LANES
        return state_ref[start : start + LANES, :]

    high = lax.Precision.HIGHEST
    by_bulk = -metric_scale * bulk
    by_dens = -(metric_scale / dens)
    swapped = {}
    for field in (0, 1):
        for n4 in range(4):
            swapped[field, n4] = pltpu.roll(chunk(field, n4), 64, 1)
    for n4 in range(4):
        along = {}
        for field in (0, 1):
            total = None
            for m4 in range(4):
                at = (n4 * 4 + m4) * 2
                term = chunk(field, m4) * coef_ref[at : at + 1, :]
                term = term + swapped[field, m4] * coef_ref[at + 1 : at + 2, :]
                total = term if total is None else total + term
            along[field] = total
        both = jnp.concatenate([chunk(2, n4), chunk(3, n4)], axis=1)
        div = along[1] + jnp.dot(both, stack_ref[...], precision=high, preferred_element_type=F32)
        grad = jnp.dot(chunk(0, n4), side_ref[...], precision=high, preferred_element_type=F32)
        start = n4 * 4 * LANES
        vol_ref[start : start + LANES, :] = by_bulk * div
        vol_ref[start + LANES : start + 2 * LANES, :] = by_dens * along[0]
        vol_ref[start + 2 * LANES : start + 3 * LANES, :] = by_dens * grad[:, 0:LANES]
        vol_ref[start + 3 * LANES : start + 4 * LANES, :] = by_dens * grad[:, LANES:]

    me = me_ref[0]
    low_half = lane < 64
    for axis in range(3):
        rows = slice(axis * LANES, axis * LANES + LANES)
        wave = wave_ref[rows, :]
        parts, zeds, walls, codes = [], [], [], []
        for side in range(2):
            face = 2 * axis + side
            nbr = nbr_ref[face : face + 1, :]
            is_wall = wall_ref[face : face + 1, :] == 1
            remote = ((nbr >> 7) != me) & jnp.logical_not(is_wall)
            local_row = (nbr & 127).astype(F32)
            local_col = column(local_row, diag)
            remote_row = jnp.where(remote, 1.0, 0.0)
            remote_col = column(remote_row, diag) > 0.0
            wall_col = column(jnp.where(is_wall, 1.0, 0.0), diag) > 0.0
            code_col = column(orient_ref[face : face + 1, :].astype(F32), diag).astype(I32)
            near = (local_col == lane.astype(F32)) & jnp.logical_not(remote_col)
            masked = jnp.where(low_half, 0.0, wave) if side == 0 else jnp.where(low_half, wave, 0.0)
            parts.append(pick_dot(jnp.where(near, 1.0, 0.0), masked))
            zed_near = jnp.sum(jnp.where(near, jnp.broadcast_to(zed_row, shape), 0.0), axis=1, keepdims=True)
            zeds.append(jnp.where(wall_col, zed, zed_near))
            walls.append(wall_col)
            codes.append(jnp.where(wall_col, 0, code_col))
            rank = jnp.sum(
                jnp.where((jnp.broadcast_to(local_row, shape) < local_col), remote_row, 0.0),
                axis=1, keepdims=True,
            )
            pick = (rank == lane.astype(F32)) & remote_col & (lane < 32)
            pick_ref[face * LANES : face * LANES + LANES, :] = jnp.where(pick, 1.0, 0.0)
        own = pltpu.roll(wave, 64, 1)
        near_ref[rows, :] = jnp.where(
            jnp.where(low_half, jnp.where(walls[1], 1, 0), jnp.where(walls[0], 1, 0)) == 1, own, parts[0] + parts[1]
        )
        zed_ref[rows, :] = jnp.where(low_half, zeds[0], zeds[1])
        code = jnp.where(low_half, codes[0], codes[1])
        a, b = (lane >> 3) & 7, lane & 7
        swap = code >= 4
        a1, b1 = jnp.where(swap, b, a), jnp.where(swap, a, b)
        a2 = jnp.where((code & 1) == 1, 7 - a1, a1)
        b2 = jnp.where((code & 2) == 2, 7 - b1, b1)
        index_ref[rows, :] = jnp.where(low_half, 64, 0) + a2 * 8 + b2


def flux_kernel(
    tab_ref, recv_ref, vol_ref, near_ref, index_ref, zed_ref, pick_ref, press_ref, norm_ref, bulk_ref,
    dens_ref, out_ref, blk, flat, sem,
):
    for face in range(6):
        owner = tab_ref[56 + face, 0]

        @pl.when(owner >= 0)
        def _():
            pltpu.make_async_copy(recv_ref.at[owner], blk.at[face], sem.at[face]).start()

    shape = (LANES, LANES)
    lane = iota(shape, 1)
    diag = iota(shape, 0) == lane
    zed = column(jnp.sqrt(bulk_ref[...] * dens_ref[...]), diag)
    up = LIFT * column(bulk_ref[...], diag)
    across = -LIFT * zed / column(dens_ref[...], diag)
    for face in range(6):
        owner = tab_ref[56 + face, 0]

        @pl.when(owner >= 0)
        def _():
            pltpu.make_async_copy(recv_ref.at[owner], blk.at[face], sem.at[face]).wait()
            for t in range(17):
                flat[face, t : t + 1, :] = blk[face, t]

        @pl.when(owner < 0)
        def _():
            flat[face] = jnp.zeros((24, LANES), F32)

    low_half = lane < 64
    thin = iota((32, LANES), 1) < 64
    i2 = lane >> 6
    j = (lane >> 3) & 7
    k = lane & 7
    sign = half_sign(shape)
    lifts = []
    for axis in range(3):
        rows = slice(axis * LANES, axis * LANES + LANES)
        far = near_ref[rows, :]
        zeds = []
        for side in range(2):
            face = 2 * axis + side
            block = flat[face, 0:16, :]
            turned = pltpu.roll(block, 64, 1)
            if side == 0:
                table = jnp.where(thin, 0.0, jnp.concatenate([turned, block], axis=0))
            else:
                table = jnp.where(thin, jnp.concatenate([block, turned], axis=0), 0.0)
            pick = pick_ref[face * LANES : face * LANES + LANES, :]
            far = far + pick_dot(pick[:, 0:32], table)
            zeds.append(jnp.sum(jnp.where(pick > 0.0, flat[face, 16:17, :], 0.0), axis=1, keepdims=True))
        far = jnp.take_along_axis(far, index_ref[rows, :], axis=1)
        zed_out = zed_ref[rows, :] + jnp.where(low_half, zeds[0], zeds[1])
        jump = (far - press_ref[rows, :] + zed_out * norm_ref[rows, :]) / (zed + zed_out)
        lifts.append((jump, sign * jump))
    for n4 in range(4):
        face_i = 2 * n4 + i2
        from_y = jnp.where(j == 7, 64, 0) + face_i * 8 + k
        from_z = jnp.where(k == 7, 64, 0) + face_i * 8 + j
        on_y = (j == 0) | (j == 7)
        on_z = (k == 0) | (k == 7)
        total = None
        for axis in range(3):
            jump = lifts[axis][0]
            if axis == 0:
                if n4 == 0:
                    here = jnp.where(low_half, jump, 0.0)
                    turn = -here
                elif n4 == 3:
                    here = jnp.where(low_half, 0.0, jump)
                    turn = here
                else:
                    here = None
            elif axis == 1:
                here = jnp.where(on_y, jnp.take_along_axis(jump, from_y, axis=1), 0.0)
                turn = jnp.where(j == 0, -here, here)
            else:
                here = jnp.where(on_z, jnp.take_along_axis(jump, from_z, axis=1), 0.0)
                turn = jnp.where(k == 0, -here, here)
            at = n4 * 4 + 1 + axis
            value = vol_ref[at * LANES : at * LANES + LANES, :]
            if here is not None:
                value = value + across * turn
                total = here if total is None else total + here
            out_ref[pl.ds(at, LANES, stride=16), :] = value
        at = n4 * 4
        out_ref[pl.ds(at, LANES, stride=16), :] = vol_ref[at * LANES : at * LANES + LANES, :] + up * total


def vm():
    return pl.BlockSpec(memory_space=VMEM)


def sm():
    return pl.BlockSpec(memory_space=SMEM)


def anyspace():
    return pl.BlockSpec(memory_space=ANY)


def shaped(shape, dtype=F32):
    return jax.ShapeDtypeStruct(shape, dtype)


def exchange(value):
    return lax.all_to_all(value, AXES, split_axis=0, concat_axis=0, tiled=True)


def body(old_state, dest_row, neighbours, orientation, wall_flags, bulk_modulus, density):
    me = (lax.axis_index("grp") * lax.axis_size("dev") + lax.axis_index("dev")).astype(I32).reshape(1)
    dest = dest_row.reshape(2, LANES)
    bulk = bulk_modulus.reshape(1, LANES)
    dens = density.reshape(1, LANES)
    state = old_state.reshape(256, 4, 4, LANES).transpose(0, 2, 1, 3).reshape(4096, LANES)

    info, pos = pl.pallas_call(
        order_kernel,
        in_specs=[vm()],
        out_specs=[vm(), vm()],
        out_shape=[shaped((DEVS, LANES), I32), shaped((2, LANES), I32)],
        name="order",
    )(dest)
    heard = exchange(info.reshape(DEVS, 1, LANES)).reshape(DEVS, LANES)
    pieces = pl.pallas_call(
        pack_kernel,
        in_specs=[sm(), sm(), vm()],
        out_specs=vm(),
        out_shape=shaped((4096, LANES)),
        name="pack",
    )(pos, dest, state)
    spread = exchange(pieces.reshape(DEVS, 32, LANES)).reshape(4096, LANES)
    table = pl.pallas_call(
        table_kernel,
        in_specs=[sm(), vm(), vm(), vm()],
        out_specs=vm(),
        out_shape=shaped((64, LANES), I32),
        scratch_shapes=[pltpu.VMEM((8, LANES), F32)],
        name="table",
    )(me, heard, neighbours, wall_flags)
    passed = pl.pallas_call(
        forward_kernel,
        in_specs=[sm(), vm()],
        out_specs=vm(),
        out_shape=shaped((2048, LANES)),
        name="forward",
    )(table, spread)
    arrived = exchange(passed.reshape(DEVS, 16, LANES)).reshape(2048, LANES)
    new_state, press, norm, wave, halo_out = pl.pallas_call(
        arrive_kernel,
        in_specs=[sm(), vm(), vm(), vm(), vm()],
        out_specs=[vm(), vm(), vm(), vm(), anyspace()],
        out_shape=[
            shaped((2048, LANES)),
            shaped((384, LANES)),
            shaped((384, LANES)),
            shaped((384, LANES)),
            shaped((DEVS, 17, 1, LANES)),
        ],
        scratch_shapes=[pltpu.VMEM((6, 17, 1, LANES), F32), pltpu.SemaphoreType.DMA((6,))],
        name="arrive",
    )(table, arrived, table[48:56], bulk, dens)
    halo_in = exchange(halo_out)
    vol, near, index, zed_out, pick = pl.pallas_call(
        volume_kernel,
        in_specs=[sm()] + [vm()] * 10,
        out_specs=[vm()] * 5,
        out_shape=[
            shaped((2048, LANES)),
            shaped((384, LANES)),
            shaped((384, LANES), I32),
            shaped((384, LANES)),
            shaped((768, LANES)),
        ],
        name="volume",
    )(
        me, new_state, wave, neighbours, wall_flags, orientation, bulk, dens,
        jnp.asarray(SIDE), jnp.asarray(STACKED), jnp.asarray(COEF),
    )
    result = pl.pallas_call(
        flux_kernel,
        in_specs=[sm(), anyspace()] + [vm()] * 9,
        out_specs=vm(),
        out_shape=shaped((2048, LANES)),
        scratch_shapes=[
            pltpu.VMEM((6, 17, 1, LANES), F32),
            pltpu.VMEM((6, 24, LANES), F32),
            pltpu.SemaphoreType.DMA((6,)),
        ],
        name="flux",
    )(table, halo_in, vol, near, index, zed_out, pick, press, norm, bulk, dens)
    return result.reshape(128, 4, 4, LANES).transpose(0, 2, 1, 3).reshape(128, 4, 512)


def solution(mesh):
    both = P(AXES)
    faces = P(None, AXES)
    in_specs = (P(AXES, None, None), both, faces, faces, faces, both, both)
    return jax.shard_map(
        body, mesh=mesh, in_specs=in_specs, out_specs=P(AXES, None, None), check_vma=False
    )
```

```python
import jax
import jax.numpy as jnp
import numpy as np
from jax import lax
from jax.experimental import pallas as pl
from jax.experimental.pallas import tpu as pltpu
from jax.sharding import PartitionSpec as P

NP = 8
DEVS = 128
LANES = 128
AXES = ("grp", "dev")
metric_scale = 0.25
F32 = jnp.float32
I32 = jnp.int32
BF16 = jnp.bfloat16
VMEM = pltpu.MemorySpace.VMEM
SMEM = pltpu.MemorySpace.SMEM
HBM = pltpu.MemorySpace.HBM


def gll_tables(poly_order):
    num_points = poly_order + 1
    points = -np.cos(np.pi * np.arange(num_points) / poly_order)
    legendre = np.zeros((num_points, num_points))
    for sweeps in range(101):
        legendre[:, 0] = 1.0
        legendre[:, 1] = points
        for degree in range(2, num_points):
            legendre[:, degree] = (
                (2 * degree - 1) * points * legendre[:, degree - 1]
                - (degree - 1) * legendre[:, degree - 2]
            ) / degree
        if sweeps < 100:
            points = points - (points * legendre[:, poly_order] - legendre[:, poly_order - 1]) / (
                num_points * legendre[:, poly_order]
            )
    end_values = legendre[:, poly_order]
    weights = 2.0 / (poly_order * num_points * end_values**2)
    distance = points[:, None] - points[None, :] + np.eye(num_points)
    derivative = end_values[:, None] / end_values[None, :] / distance
    derivative = derivative * (1.0 - np.eye(num_points))
    derivative[0, 0] = -poly_order * num_points / 4.0
    derivative[poly_order, poly_order] = poly_order * num_points / 4.0
    return (points, weights, derivative)


POINTS, WEIGHTS, DERIV = gll_tables(NP - 1)
DERIV = DERIV.astype(np.float32)
LIFT = metric_scale / float(WEIGHTS[0])


def derivative_tables():
    eye2, eye8 = np.eye(2, dtype=np.float32), np.eye(8, dtype=np.float32)
    along_y = np.kron(eye2, np.kron(DERIV.T, eye8))
    along_z = np.kron(eye2, np.kron(eye8, DERIV.T))
    side = np.concatenate([along_y, along_z], axis=1)
    stacked = np.concatenate([along_y, along_z], axis=0)
    coef = np.zeros((4, 4, 2, LANES), np.float32)
    for out_chunk in range(4):
        for in_chunk in range(4):
            for half in range(2):
                lanes = slice(64 * half, 64 * half + 64)
                coef[out_chunk, in_chunk, 0, lanes] = DERIV[2 * out_chunk + half, 2 * in_chunk + half]
                coef[out_chunk, in_chunk, 1, lanes] = DERIV[
                    2 * out_chunk + half, 2 * in_chunk + 1 - half
                ]
    return side, stacked, coef.reshape(32, LANES)


SIDE, STACKED, COEF = derivative_tables()


def iota(shape, axis):
    return lax.broadcasted_iota(I32, shape, axis)


def small_dot(left, right):
    return jnp.dot(left.astype(BF16), right.astype(BF16), preferred_element_type=F32)


def split3(value):
    high = value.astype(BF16)
    rest = value - high.astype(F32)
    middle = rest.astype(BF16)
    low = (rest - middle.astype(F32)).astype(BF16)
    return high, middle, low


def pick_dot(pick, value):
    pick = pick.astype(BF16)
    high, middle, low = split3(value)
    total = jnp.dot(pick, high, preferred_element_type=F32)
    total = total + jnp.dot(pick, middle, preferred_element_type=F32)
    return total + jnp.dot(pick, low, preferred_element_type=F32)


def column(row, diag):
    wide = jnp.broadcast_to(row, (LANES, LANES))
    return jnp.sum(jnp.where(diag, wide, 0.0), axis=1, keepdims=True)


def half_sign(shape):
    return jnp.where(iota(shape, 1) < 64, -1.0, 1.0)


def face_pair(chunk, axis, zed):
    lane = iota((LANES, LANES), 1)
    half, face_i, face_b = lane >> 6, (lane >> 3) & 7, lane & 7
    from_y = (face_i & 1) * 64 + half * 56 + face_b
    from_z = (face_i & 1) * 64 + face_b * 8 + half * 7
    values = []
    for field in (0, 1 + axis):
        if axis == 0:
            value = jnp.where(lane < 64, chunk(field, 0), chunk(field, 3))
        else:
            index = from_y if axis == 1 else from_z
            value = jnp.take_along_axis(chunk(field, 0), index, axis=1)
            for n4 in range(1, 4):
                other = jnp.take_along_axis(chunk(field, n4), index, axis=1)
                value = jnp.where(face_i >> 1 == n4, other, value)
        values.append(value)
    normal = half_sign((LANES, LANES)) * values[1]
    return values[0], normal, values[0] + zed * normal


def order_kernel(dest_ref, info_ref, pos_ref):
    dest = dest_ref[...]
    sub = iota((LANES, LANES), 0)
    lane = iota((LANES, LANES), 1)
    diag = sub == lane
    key_row, key_col, dev_row, dev_col, lab_col = [], [], [], [], []
    for half in range(2):
        row = jnp.broadcast_to(dest[half : half + 1, :], (LANES, LANES))
        owner = (row >> 7).astype(F32)
        local = (row & 127).astype(F32) + 1.0
        key = owner * 256.0 + (lane + 128 * half).astype(F32)
        key_row.append(key)
        dev_row.append(owner)
        key_col.append(jnp.sum(jnp.where(diag, key, 0.0), axis=1, keepdims=True))
        dev_col.append(jnp.sum(jnp.where(diag, owner, 0.0), axis=1, keepdims=True))
        lab_col.append(jnp.sum(jnp.where(diag, local, 0.0), axis=1, keepdims=True))
    labels = jnp.zeros((LANES, LANES), F32)
    targets = jnp.zeros((1, LANES), F32)
    for half in range(2):
        before_col = jnp.zeros((LANES, 1), F32)
        before_row = jnp.zeros((1, LANES), F32)
        for other in range(2):
            before_col = before_col + jnp.sum(
                jnp.where(key_row[other] < key_col[half], 1.0, 0.0), axis=1, keepdims=True
            )
            before_row = before_row + jnp.sum(
                jnp.where(key_col[other] < key_row[half], 1.0, 0.0), axis=0, keepdims=True
            )
        pos_ref[half : half + 1, :] = before_row.astype(I32)
        place = before_col.astype(I32)
        is_target = (place == 8 * lane) & (lane < 32)
        targets = targets + jnp.sum(jnp.where(is_target, dev_col[half], 0.0), axis=0, keepdims=True)
        is_label = (place & 7) == lane - 32
        mine = jnp.where(dev_row[half] == sub.astype(F32), 1.0, 0.0)
        labels = labels + small_dot(mine, jnp.where(is_label, lab_col[half], 0.0))
    info_ref[...] = (labels + targets).astype(I32)


def pack_kernel(pos_ref, dest_ref, state_ref, out_ref):
    @pl.when(dest_ref[0, 0] >= 0)
    def _():
        def one(slot, carry):
            place = pos_ref[slot >> 7, slot & 127]
            start = (place & 7) * 512 + (place >> 3)
            out_ref[pl.ds(start, 16, stride=32), :] = state_ref[pl.ds(pl.multiple_of(slot * 16, 16), 16), :]
            return carry

        lax.fori_loop(0, 256, one, 0, unroll=8)


def table_kernel(
    me_ref, info_ref, nbr_ref, wall_ref, bulk_ref, dens_ref, spot_ref, owner_ref, out_ref, cols_ref, wide, scr
):
    sub = iota((LANES, LANES), 0)
    lane = iota((LANES, LANES), 1)
    diag = sub == lane
    bulk = column(bulk_ref[...], diag)
    dens = column(dens_ref[...], diag)
    zed = column(jnp.sqrt(bulk_ref[...] * dens_ref[...]), diag)
    cols_ref[...] = jnp.where(lane == 0, zed, jnp.where(lane == 1, bulk, dens))
    info = info_ref[...]
    present = jnp.zeros((LANES, LANES), F32)
    for j in range(32):
        present = jnp.where(info[:, j : j + 1] == lane, 1.0, present)
    below = jnp.where(lane < sub, 1.0, 0.0)
    rank = small_dot(below, present)
    target = jnp.clip(info, 0, LANES - 1)
    slot = target * 16 + jnp.take_along_axis(rank.astype(I32), target, axis=1)
    slot = jnp.where(info >= 0, slot, -1)
    wide[...] = slot
    quarter = iota((32, LANES), 1) >> 5
    spots = wide[pl.ds(0, 32, stride=4), :]
    for part in range(1, 4):
        moved = pltpu.roll(wide[pl.ds(part, 32, stride=4), :], 32 * part, 1)
        spots = jnp.where(quarter == part, moved, spots)
    spot_ref[...] = spots
    is_source = jnp.broadcast_to(jnp.where(info[:, 32:33] > 0, 1.0, 0.0), (LANES, LANES))
    order = small_dot(below, is_source)
    label = jnp.take_along_axis(info, 32 + (lane >> 4), axis=1)
    chosen = (is_source > 0.0) & (order == (lane & 15).astype(F32))
    labels = jnp.sum(jnp.where(chosen, label.astype(F32), 0.0), axis=0, keepdims=True)
    out_ref[0:8, :] = jnp.broadcast_to(labels, (8, LANES)).astype(I32) - 1
    scr[...] = jnp.zeros((8, LANES), F32)
    nbr = nbr_ref[...]
    owner = nbr >> 7
    remote = (owner != me_ref[0]) & (wall_ref[...] == 0)
    scr[0:6, :] = jnp.where(remote, 1.0, 0.0)
    flags = scr[...]
    before = small_dot(flags, jnp.where(sub < lane, 1.0, 0.0))
    out_ref[8:16, :] = jnp.where(flags > 0.0, before, -1.0).astype(I32)
    scr[...] = jnp.full((8, LANES), -1.0, F32)
    scr[0:6, :] = jnp.where(remote, owner, -1).astype(F32)
    owner_ref[...] = jnp.broadcast_to(
        jnp.max(scr[...], axis=1, keepdims=True), (8, LANES)
    ).astype(I32)


def forward_kernel(spot_ref, in_ref, out_ref):
    def one(source, carry):
        base = pl.multiple_of(source * 32, 32)

        @pl.when(spot_ref[base] >= 0)
        def _():
            for j in range(32):
                out_ref[pl.ds(spot_ref[base + j], 1), :] = in_ref[pl.ds(base + j, 1), :]

        return carry

    lax.fori_loop(0, DEVS, one, 0)


def arrive_kernel(
    owner_ref, in_ref, row_ref, cols_ref, state_ref, send_ref, blk, sem
):
    place = jnp.where(row_ref[0:1, :] == iota((LANES, LANES), 0), 1.0, 0.0).astype(BF16)
    place = jnp.concatenate([place, place, place], axis=1)
    for chunk_id in range(0, 16, 2):
        pair = []
        for c in (chunk_id, chunk_id + 1):
            rows = [in_ref[(k * 16 + c) * 16 : (k * 16 + c) * 16 + 16, :] for k in range(8)]
            pair.append(jnp.concatenate(rows, axis=0))
        parts = split3(jnp.concatenate(pair, axis=1))
        moved = jnp.dot(place, jnp.concatenate(parts, axis=0), preferred_element_type=F32)
        state_ref[chunk_id * LANES : (chunk_id + 1) * LANES, :] = moved[:, 0:LANES]
        state_ref[(chunk_id + 1) * LANES : (chunk_id + 2) * LANES, :] = moved[:, LANES:]

    shape = (LANES, LANES)
    lane = iota(shape, 1)
    diag = iota(shape, 0) == lane
    zed = cols_ref[:, 0:1]

    def chunk(field, n4):
        start = (n4 * 4 + field) * LANES
        return state_ref[start : start + LANES, :]

    for axis in range(3):
        wave = face_pair(chunk, axis, zed)[2]
        for side in range(2):
            face = 2 * axis + side
            rank = row_ref[8 + face : 9 + face, :]
            pick = jnp.where(rank == iota((32, LANES), 0), 1.0, 0.0)
            got = pick_dot(pick, wave)
            first, second = got[0:16], got[16:32]
            if side == 0:
                second = pltpu.roll(second, 64, 1)
            else:
                first = pltpu.roll(first, 64, 1)
            block = jnp.where(iota((16, LANES), 1) < 64, first, second)
            rank_col = jnp.sum(
                jnp.where(diag, jnp.broadcast_to(rank, shape).astype(F32), 0.0), axis=1, keepdims=True
            )
            zeds = jnp.sum(jnp.where(rank_col == lane.astype(F32), zed, 0.0), axis=0, keepdims=True)
            for t in range(16):
                blk[face, t] = block[t : t + 1, :]
            blk[face, 16] = zeds
            owner = owner_ref[face, 0]

            @pl.when(owner >= 0)
            def _():
                pltpu.make_async_copy(blk.at[face], send_ref.at[owner], sem.at[face]).start()

    for face in range(6):
        owner = owner_ref[face, 0]

        @pl.when(owner >= 0)
        def _():
            pltpu.make_async_copy(blk.at[face], send_ref.at[owner], sem.at[face]).wait()


def volume_kernel(
    me_ref, state_ref, cols_ref, nbr_ref, wall_ref, orient_ref, bulk_ref, dens_ref, side_ref, stack_ref,
    coef_ref, vol_ref, press_ref, norm_ref, near_ref, index_ref, zed_ref, pick_ref,
):
    shape = (LANES, LANES)
    lane = iota(shape, 1)
    diag = iota(shape, 0) == lane
    zed_row = jnp.sqrt(bulk_ref[...] * dens_ref[...])
    zed, bulk, dens = cols_ref[:, 0:1], cols_ref[:, 1:2], cols_ref[:, 2:3]

    def chunk(field, n4):
        start = (n4 * 4 + field) * LANES
        return state_ref[start : start + LANES, :]

    high = lax.Precision.HIGHEST
    by_bulk = -metric_scale * bulk
    by_dens = -(metric_scale / dens)
    swapped = {}
    for field in (0, 1):
        for n4 in range(4):
            swapped[field, n4] = pltpu.roll(chunk(field, n4), 64, 1)
    for n4 in range(4):
        along = {}
        for field in (0, 1):
            total = None
            for m4 in range(4):
                at = (n4 * 4 + m4) * 2
                term = chunk(field, m4) * coef_ref[at : at + 1, :]
                term = term + swapped[field, m4] * coef_ref[at + 1 : at + 2, :]
                total = term if total is None else total + term
            along[field] = total
        both = jnp.concatenate([chunk(2, n4), chunk(3, n4)], axis=1)
        div = along[1] + jnp.dot(both, stack_ref[...], precision=high, preferred_element_type=F32)
        grad = jnp.dot(chunk(0, n4), side_ref[...], precision=high, preferred_element_type=F32)
        start = n4 * 4 * LANES
        vol_ref[start : start + LANES, :] = by_bulk * div
        vol_ref[start + LANES : start + 2 * LANES, :] = by_dens * along[0]
        vol_ref[start + 2 * LANES : start + 3 * LANES, :] = by_dens * grad[:, 0:LANES]
        vol_ref[start + 3 * LANES : start + 4 * LANES, :] = by_dens * grad[:, LANES:]

    me = me_ref[0]
    low_half = lane < 64
    zed_out = jnp.zeros(shape, F32)
    for axis in range(3):
        rows = slice(axis * LANES, axis * LANES + LANES)
        press, norm, wave = face_pair(chunk, axis, zed)
        press_ref[rows, :] = press
        norm_ref[rows, :] = norm
        parts, zeds, walls, codes, picks = [], [], [], [], []
        for side in range(2):
            face = 2 * axis + side
            nbr = nbr_ref[face : face + 1, :]
            is_wall = wall_ref[face : face + 1, :] == 1
            remote = ((nbr >> 7) != me) & jnp.logical_not(is_wall)
            local_row = (nbr & 127).astype(F32)
            local_col = column(local_row, diag)
            remote_row = jnp.where(remote, 1.0, 0.0)
            remote_col = column(remote_row, diag) > 0.0
            wall_col = column(jnp.where(is_wall, 1.0, 0.0), diag) > 0.0
            code_col = column(orient_ref[face : face + 1, :].astype(F32), diag).astype(I32)
            near = (local_col == lane.astype(F32)) & jnp.logical_not(remote_col)
            masked = jnp.where(low_half, 0.0, wave) if side == 0 else jnp.where(low_half, wave, 0.0)
            parts.append(pick_dot(jnp.where(near, 1.0, 0.0), masked))
            zed_near = jnp.sum(jnp.where(near, jnp.broadcast_to(zed_row, shape), 0.0), axis=1, keepdims=True)
            zeds.append(jnp.where(wall_col, zed, zed_near))
            walls.append(wall_col)
            codes.append(jnp.where(wall_col, 0, code_col))
            rank = jnp.sum(
                jnp.where((jnp.broadcast_to(local_row, shape) < local_col), remote_row, 0.0),
                axis=1, keepdims=True,
            )
            pick = (rank == lane.astype(F32)) & remote_col & (lane < 32)
            picks.append(jnp.where(pick, 1.0, 0.0))
        own = pltpu.roll(wave, 64, 1)
        near_ref[rows, :] = jnp.where(
            jnp.where(low_half, jnp.where(walls[1], 1, 0), jnp.where(walls[0], 1, 0)) == 1, own, parts[0] + parts[1]
        )
        zed_out = jnp.where(lane == 2 * axis, zeds[0], jnp.where(lane == 2 * axis + 1, zeds[1], zed_out))
        pick_ref[rows, :] = picks[0] + pltpu.roll(picks[1], 32, 1)
        code = jnp.where(low_half, codes[0], codes[1])
        a, b = (lane >> 3) & 7, lane & 7
        swap = code >= 4
        a1, b1 = jnp.where(swap, b, a), jnp.where(swap, a, b)
        a2 = jnp.where((code & 1) == 1, 7 - a1, a1)
        b2 = jnp.where((code & 2) == 2, 7 - b1, b1)
        index_ref[rows, :] = jnp.where(low_half, 64, 0) + a2 * 8 + b2
    zed_ref[...] = zed_out


def flux_kernel(
    owner_ref, recv_ref, vol_hbm, near_ref, index_ref, zed_ref, pick_ref, press_ref, norm_ref, cols_ref,
    out_ref, flat, vol_ref, sem,
):
    load = pltpu.make_async_copy(vol_hbm, vol_ref, sem)
    load.start()
    shape = (LANES, LANES)
    lane = iota(shape, 1)
    zed = cols_ref[:, 0:1]
    up = LIFT * cols_ref[:, 1:2]
    across = -LIFT * zed / cols_ref[:, 2:3]
    for face in range(6):
        owner = owner_ref[face, 0]

        @pl.when(owner >= 0)
        def _():
            for t in range(17):
                flat[face, t : t + 1, :] = recv_ref[owner, t]

        @pl.when(owner < 0)
        def _():
            flat[face] = jnp.zeros((24, LANES), F32)

    low_half = lane < 64
    thin = iota((32, LANES), 1) < 64
    i2 = lane >> 6
    j = (lane >> 3) & 7
    k = lane & 7
    sign = half_sign(shape)
    lifts = []
    for axis in range(3):
        rows = slice(axis * LANES, axis * LANES + LANES)
        pick = pick_ref[rows, :]
        tables, zeds = [], []
        for side in range(2):
            face = 2 * axis + side
            block = flat[face, 0:16, :]
            turned = pltpu.roll(block, 64, 1)
            if side == 0:
                tables.append(jnp.where(thin, 0.0, jnp.concatenate([turned, block], axis=0)))
            else:
                tables.append(jnp.where(thin, jnp.concatenate([block, turned], axis=0), 0.0))
            zed_row = flat[face, 16:17, :] if side == 0 else pltpu.roll(flat[face, 16:24, :], 32, 1)[0:1, :]
            mine = (lane >> 5 == side) & (pick > 0.0)
            zeds.append(
                zed_ref[:, face : face + 1] + jnp.sum(jnp.where(mine, zed_row, 0.0), axis=1, keepdims=True)
            )
        far = near_ref[rows, :] + pick_dot(pick[:, 0:64], jnp.concatenate(tables, axis=0))
        far = jnp.take_along_axis(far, index_ref[rows, :], axis=1)
        zed_out = jnp.where(low_half, zeds[0], zeds[1])
        jump = (far - press_ref[rows, :] + zed_out * norm_ref[rows, :]) / (zed + zed_out)
        lifts.append((jump, sign * jump))
    load.wait()
    for n4 in range(4):
        face_i = 2 * n4 + i2
        from_y = jnp.where(j == 7, 64, 0) + face_i * 8 + k
        from_z = jnp.where(k == 7, 64, 0) + face_i * 8 + j
        on_y = (j == 0) | (j == 7)
        on_z = (k == 0) | (k == 7)
        total = None
        for axis in range(3):
            jump = lifts[axis][0]
            if axis == 0:
                if n4 == 0:
                    here = jnp.where(low_half, jump, 0.0)
                    turn = -here
                elif n4 == 3:
                    here = jnp.where(low_half, 0.0, jump)
                    turn = here
                else:
                    here = None
            elif axis == 1:
                here = jnp.where(on_y, jnp.take_along_axis(jump, from_y, axis=1), 0.0)
                turn = jnp.where(j == 0, -here, here)
            else:
                here = jnp.where(on_z, jnp.take_along_axis(jump, from_z, axis=1), 0.0)
                turn = jnp.where(k == 0, -here, here)
            at = n4 * 4 + 1 + axis
            value = vol_ref[at * LANES : at * LANES + LANES, :]
            if here is not None:
                value = value + across * turn
                total = here if total is None else total + here
            out_ref[pl.ds(at, LANES, stride=16), :] = value
        at = n4 * 4
        out_ref[pl.ds(at, LANES, stride=16), :] = vol_ref[at * LANES : at * LANES + LANES, :] + up * total


def vm():
    return pl.BlockSpec(memory_space=VMEM)


def sm():
    return pl.BlockSpec(memory_space=SMEM)


def shaped(shape, dtype=F32):
    return VMEM(shape, dtype)


def away(value):
    return pltpu.with_memory_space_constraint(value, HBM)


GRANT = pltpu.CompilerParams(vmem_limit_bytes=24 * 1024 * 1024)


def plain(shape, dtype=F32):
    return jax.ShapeDtypeStruct(shape, dtype)


def near(value):
    return pltpu.with_memory_space_constraint(value, VMEM)


def exchange(value):
    return lax.all_to_all(value, AXES, split_axis=0, concat_axis=0, tiled=True)


def body(old_state, dest_row, neighbours, orientation, wall_flags, bulk_modulus, density):
    me = (lax.axis_index("grp") * lax.axis_size("dev") + lax.axis_index("dev")).astype(I32).reshape(1)
    dest = dest_row.reshape(2, LANES)
    bulk = bulk_modulus.reshape(1, LANES)
    dens = density.reshape(1, LANES)
    state = old_state.reshape(256, 4, 4, LANES).transpose(0, 2, 1, 3).reshape(4096, LANES)

    info, pos = pl.pallas_call(
        order_kernel,
        in_specs=[vm()],
        out_specs=[vm(), vm()],
        out_shape=[plain((DEVS, LANES), I32), plain((2, LANES), I32)],
        name="order",
        compiler_params=GRANT,
    )(dest)
    heard = exchange(info.reshape(DEVS, 1, LANES)).reshape(DEVS, LANES)
    pieces = pl.pallas_call(
        pack_kernel,
        in_specs=[sm(), sm(), vm()],
        out_specs=vm(),
        out_shape=plain((4096, LANES)),
        name="pack",
        compiler_params=GRANT,
    )(pos, dest, state)
    spread = exchange(pieces.reshape(DEVS, 32, LANES)).reshape(4096, LANES)
    spots, owners, rows, cols = pl.pallas_call(
        table_kernel,
        in_specs=[sm()] + [vm()] * 5,
        out_specs=[vm()] * 4,
        out_shape=[
            shaped((32, LANES), I32),
            shaped((8, LANES), I32),
            shaped((16, LANES), I32),
            shaped((LANES, LANES)),
        ],
        scratch_shapes=[pltpu.VMEM((LANES, LANES), I32), pltpu.VMEM((8, LANES), F32)],
        name="table",
        compiler_params=GRANT,
    )(me, near(heard), away(neighbours), away(wall_flags), away(bulk), away(dens))
    passed = pl.pallas_call(
        forward_kernel,
        in_specs=[sm(), vm()],
        out_specs=vm(),
        out_shape=shaped((2048, LANES)),
        name="forward",
        compiler_params=GRANT,
    )(spots.reshape(4096), near(spread))
    arrived = exchange(passed.reshape(DEVS, 16, LANES)).reshape(2048, LANES)
    new_state, halo_out = pl.pallas_call(
        arrive_kernel,
        in_specs=[sm()] + [vm()] * 3,
        out_specs=[vm(), pl.BlockSpec(memory_space=pl.ANY)],
        out_shape=[shaped((2048, LANES)), plain((DEVS, 17, 1, LANES))],
        scratch_shapes=[pltpu.VMEM((6, 17, 1, LANES), F32), pltpu.SemaphoreType.DMA((6,))],
        name="arrive",
        compiler_params=GRANT,
    )(owners, near(arrived), near(rows), near(cols))
    halo_in = exchange(halo_out)
    vol, press, norm, here, index, zed_out, pick = pl.pallas_call(
        volume_kernel,
        in_specs=[sm()] + [vm()] * 10,
        out_specs=[vm()] * 7,
        out_shape=[
            HBM((2048, LANES), F32),
            shaped((384, LANES)),
            shaped((384, LANES)),
            shaped((384, LANES)),
            shaped((384, LANES), I32),
            shaped((LANES, LANES)),
            shaped((384, LANES)),
        ],
        name="volume",
        compiler_params=GRANT,
    )(
        me, near(new_state), near(cols), away(neighbours), away(wall_flags), away(orientation), away(bulk),
        away(dens), away(jnp.asarray(SIDE)), away(jnp.asarray(STACKED)), away(jnp.asarray(COEF)),
    )
    result = pl.pallas_call(
        flux_kernel,
        in_specs=[sm(), vm(), pl.BlockSpec(memory_space=pl.ANY)] + [vm()] * 7,
        out_specs=vm(),
        out_shape=plain((2048, LANES)),
        scratch_shapes=[
            pltpu.VMEM((6, 24, LANES), F32),
            pltpu.VMEM((2048, LANES), F32),
            pltpu.SemaphoreType.DMA,
        ],
        name="flux",
        compiler_params=GRANT,
    )(
        owners, near(halo_in), away(vol), near(here), near(index), near(zed_out), near(pick), near(press),
        near(norm), near(cols),
    )
    return result.reshape(128, 4, 4, LANES).transpose(0, 2, 1, 3).reshape(128, 4, 512)


def solution(mesh):
    both = P(AXES)
    faces = P(None, AXES)
    in_specs = (P(AXES, None, None), both, faces, faces, faces, both, both)
    return jax.shard_map(
        body, mesh=mesh, in_specs=in_specs, out_specs=P(AXES, None, None), check_vma=False
    )
```

```python
import jax
import jax.numpy as jnp
import numpy as np
from jax import lax
from jax.experimental import pallas as pl
from jax.experimental.pallas import tpu as pltpu
from jax.sharding import PartitionSpec as P

NP = 8
DEVS = 128
LANES = 128
AXES = ("grp", "dev")
metric_scale = 0.25
F32 = jnp.float32
I32 = jnp.int32
BF16 = jnp.bfloat16
VMEM = pltpu.MemorySpace.VMEM
SMEM = pltpu.MemorySpace.SMEM
HBM = pltpu.MemorySpace.HBM


def gll_tables(poly_order):
    num_points = poly_order + 1
    points = -np.cos(np.pi * np.arange(num_points) / poly_order)
    legendre = np.zeros((num_points, num_points))
    for sweeps in range(101):
        legendre[:, 0] = 1.0
        legendre[:, 1] = points
        for degree in range(2, num_points):
            legendre[:, degree] = (
                (2 * degree - 1) * points * legendre[:, degree - 1]
                - (degree - 1) * legendre[:, degree - 2]
            ) / degree
        if sweeps < 100:
            points = points - (points * legendre[:, poly_order] - legendre[:, poly_order - 1]) / (
                num_points * legendre[:, poly_order]
            )
    end_values = legendre[:, poly_order]
    weights = 2.0 / (poly_order * num_points * end_values**2)
    distance = points[:, None] - points[None, :] + np.eye(num_points)
    derivative = end_values[:, None] / end_values[None, :] / distance
    derivative = derivative * (1.0 - np.eye(num_points))
    derivative[0, 0] = -poly_order * num_points / 4.0
    derivative[poly_order, poly_order] = poly_order * num_points / 4.0
    return (points, weights, derivative)


POINTS, WEIGHTS, DERIV = gll_tables(NP - 1)
DERIV = DERIV.astype(np.float32)
LIFT = metric_scale / float(WEIGHTS[0])


def derivative_tables():
    eye2, eye8 = np.eye(2, dtype=np.float32), np.eye(8, dtype=np.float32)
    along_y = np.kron(eye2, np.kron(DERIV.T, eye8))
    along_z = np.kron(eye2, np.kron(eye8, DERIV.T))
    side = np.concatenate([along_y, along_z], axis=1)
    stacked = np.concatenate([along_y, along_z], axis=0)
    coef = np.zeros((4, 4, 2, LANES), np.float32)
    for out_chunk in range(4):
        for in_chunk in range(4):
            for half in range(2):
                lanes = slice(64 * half, 64 * half + 64)
                coef[out_chunk, in_chunk, 0, lanes] = DERIV[2 * out_chunk + half, 2 * in_chunk + half]
                coef[out_chunk, in_chunk, 1, lanes] = DERIV[
                    2 * out_chunk + half, 2 * in_chunk + 1 - half
                ]
    return side, stacked, coef.reshape(32, LANES)


SIDE, STACKED, COEF = derivative_tables()


def iota(shape, axis):
    return lax.broadcasted_iota(I32, shape, axis)


def small_dot(left, right):
    return jnp.dot(left.astype(BF16), right.astype(BF16), preferred_element_type=F32)


def split3(value):
    high = value.astype(BF16)
    rest = value - high.astype(F32)
    middle = rest.astype(BF16)
    low = (rest - middle.astype(F32)).astype(BF16)
    return high, middle, low


def pick_dot(pick, value):
    pick = pick.astype(BF16)
    high, middle, low = split3(value)
    total = jnp.dot(pick, high, preferred_element_type=F32)
    total = total + jnp.dot(pick, middle, preferred_element_type=F32)
    return total + jnp.dot(pick, low, preferred_element_type=F32)


def column(row, diag):
    wide = jnp.broadcast_to(row, (LANES, LANES))
    return jnp.sum(jnp.where(diag, wide, 0.0), axis=1, keepdims=True)


def half_sign(shape):
    return jnp.where(iota(shape, 1) < 64, -1.0, 1.0)


def face_pair(chunk, axis, zed):
    lane = iota((LANES, LANES), 1)
    half, face_i, face_b = lane >> 6, (lane >> 3) & 7, lane & 7
    from_y = (face_i & 1) * 64 + half * 56 + face_b
    from_z = (face_i & 1) * 64 + face_b * 8 + half * 7
    values = []
    for field in (0, 1 + axis):
        if axis == 0:
            value = jnp.where(lane < 64, chunk(field, 0), chunk(field, 3))
        else:
            index = from_y if axis == 1 else from_z
            value = jnp.take_along_axis(chunk(field, 0), index, axis=1)
            for n4 in range(1, 4):
                other = jnp.take_along_axis(chunk(field, n4), index, axis=1)
                value = jnp.where(face_i >> 1 == n4, other, value)
        values.append(value)
    normal = half_sign((LANES, LANES)) * values[1]
    return values[0], normal, values[0] + zed * normal


def cross(arrays, bit1, bit0):
    first = [jnp.where(bit0, arrays[t ^ 1], arrays[t]) for t in range(4)]
    return [jnp.where(bit1, first[t ^ 2], first[t]) for t in range(4)]


def lane_bit(lane, bit):
    return ((lane >> bit) & 1) == 1


def regroup(arrays, back):
    lane = iota(arrays[0].shape, 1)
    own = (lane >> 3) & 3
    plain = (lane_bit(lane, 1), lane_bit(lane, 0))
    mixed = (lane_bit(lane ^ (lane >> 3), 1), lane_bit(lane ^ (lane >> 3), 0))
    enter, leave = (plain, mixed) if back else (mixed, plain)
    result = [None] * 16
    for top in range(4):
        four = cross(arrays[4 * top : 4 * top + 4], *enter)
        four = [jnp.take_along_axis(four[t], lane ^ t ^ own, axis=1) for t in range(4)]
        result[4 * top : 4 * top + 4] = cross(four, *leave)
    j2, k2 = lane_bit(lane, 5), lane_bit(lane, 2)
    final = [None] * 16
    for t in range(4):
        final[t::4] = cross(result[t::4], j2, k2)
    return final


def order_kernel(me_ref, dest_ref, nbr_ref, wall_ref, info_ref, pos_ref, scr):
    dest = dest_ref[...]
    sub = iota((LANES, LANES), 0)
    lane = iota((LANES, LANES), 1)
    diag = sub == lane
    key_row, key_col, dest_col = [], [], []
    for half in range(2):
        row = jnp.broadcast_to(dest[half : half + 1, :], (LANES, LANES))
        key = (row >> 7).astype(F32) * 256.0 + (lane + 128 * half).astype(F32)
        key_row.append(key)
        key_col.append(jnp.sum(jnp.where(diag, key, 0.0), axis=1, keepdims=True))
        dest_col.append(jnp.sum(jnp.where(diag, row.astype(F32), 0.0), axis=1, keepdims=True))
    lists = [jnp.zeros((1, LANES), F32), jnp.zeros((1, LANES), F32)]
    for half in range(2):
        before_col = jnp.zeros((LANES, 1), F32)
        before_row = jnp.zeros((1, LANES), F32)
        for other in range(2):
            before_col = before_col + jnp.sum(
                jnp.where(key_row[other] < key_col[half], 1.0, 0.0), axis=1, keepdims=True
            )
            before_row = before_row + jnp.sum(
                jnp.where(key_col[other] < key_row[half], 1.0, 0.0), axis=0, keepdims=True
            )
        pos_ref[half : half + 1, :] = before_row.astype(I32)
        place = before_col.astype(I32)
        k = place & 7
        spot = (k & 3) * 32 + (place >> 3)
        for part in range(2):
            hit = (spot == lane) & (k >> 2 == part)
            lists[part] = lists[part] + jnp.sum(jnp.where(hit, dest_col[half], 0.0), axis=0, keepdims=True)
    scr[...] = jnp.full((8, LANES), -1.0, F32)
    owner = nbr_ref[...] >> 7
    remote = (owner != me_ref[0]) & (wall_ref[...] == 0)
    scr[0:6, :] = jnp.where(remote, owner, -1).astype(F32)
    owners = jnp.max(scr[...], axis=1, keepdims=True)
    spread = iota((8, LANES), 0) == iota((8, LANES), 1)
    owner_row = jnp.sum(jnp.where(spread, owners, 0.0), axis=0, keepdims=True)
    for part, row in enumerate((lists[0], lists[1], owner_row)):
        info_ref[pl.ds(part, LANES, stride=3), :] = jnp.broadcast_to(row, (LANES, LANES)).astype(I32)


def pack_kernel(pos_ref, dest_ref, state_ref, bulk_ref, dens_ref, out_ref, scr):
    zed = jnp.sqrt(bulk_ref[...] * dens_ref[...])
    out_ref[pl.ds(32, LANES, stride=33), :] = jnp.broadcast_to(zed, (LANES, LANES))

    @pl.when(dest_ref[0, 0] >= 0)
    def _():
        def one(slot, carry):
            place = pos_ref[slot >> 7, slot & 127]
            start = (place & 7) * 512 + (place >> 3)
            scr[pl.ds(start, 16, stride=32), :] = state_ref[pl.ds(pl.multiple_of(slot * 16, 16), 16), :]
            return carry

        lax.fori_loop(0, 256, one, 0, unroll=8)
        for k in range(8):
            for block in range(4):
                at = [(k * 16 + c) * 32 + block * 8 for c in range(16)]
                groups = regroup([scr[a : a + 8, :] for a in at], False)
                for g in range(16):
                    row = (k * 16 + g) * 33 + block * 8
                    out_ref[row : row + 8, :] = groups[g]


def table_kernel(
    me_ref, info_ref, nbr_ref, wall_ref, orient_ref, bulk_ref, dens_ref,
    spot_ref, owner_ref, row_ref, label_ref, cols_ref, far_ref, near_ref, pick_ref, wide, scr,
):
    shape = (LANES, LANES)
    sub = iota(shape, 0)
    lane = iota(shape, 1)
    diag = sub == lane
    me = me_ref[0]
    bulk = column(bulk_ref[...], diag)
    dens = column(dens_ref[...], diag)
    zed = column(jnp.sqrt(bulk_ref[...] * dens_ref[...]), diag)
    cols_ref[...] = jnp.where(lane == 0, zed, jnp.where(lane == 1, bulk, dens))

    lists = [info_ref[pl.ds(0, LANES, stride=3), :], info_ref[pl.ds(1, LANES, stride=3), :]]
    owners = info_ref[pl.ds(2, LANES, stride=3), :].astype(F32)
    owner_ref[...] = owners.T[0:8, :].astype(I32)
    target = lists[0] >> 7
    my_k = me >> 4
    mine = jnp.where(my_k >= 4, lists[1], lists[0])
    mine = jnp.take_along_axis(mine, (my_k & 3) * 32 + (lane & 31), axis=1) & 127
    present = jnp.zeros(shape, F32)
    label = jnp.zeros(shape, F32)
    mine = mine.astype(F32)
    for j in range(32):
        hit = target[:, j : j + 1] == lane
        present = jnp.where(hit, 1.0, present)
        label = jnp.where(hit, mine[:, j : j + 1], label)
    below = jnp.where(lane < sub, 1.0, 0.0)
    rank = small_dot(below, present)
    safe = jnp.clip(target, 0, LANES - 1)
    slot = safe * 16 + jnp.take_along_axis(rank.astype(I32), safe, axis=1)
    wide[...] = jnp.where(target >= 0, slot, -1)
    quarter = iota((32, LANES), 1) >> 5
    spots = wide[pl.ds(0, 32, stride=4), :]
    for part in range(1, 4):
        moved = pltpu.roll(wide[pl.ds(part, 32, stride=4), :], 32 * part, 1)
        spots = jnp.where(quarter == part, moved, spots)
    spot_ref[...] = spots
    order = jnp.where(present > 0.0, rank, -1.0)
    labels = jnp.zeros(shape, F32)
    for i in range(16):
        row = jnp.sum(jnp.where(order == float(i), label, 0.0), axis=0, keepdims=True)
        labels = jnp.where(sub == i, row, labels)
    label_ref[...] = labels.T.astype(I32)

    gather = [jnp.where((sub >> 5) + 4 * part == lane >> 4, 1.0, 0.0) for part in range(2)]

    def rows_of(block):
        value = jnp.zeros(shape, F32)
        for part in range(2):
            held = jnp.where(lists[part] >> 7 == block, (lists[part] & 127).astype(F32), 0.0)
            value = value + small_dot(held, gather[part])
        source = jnp.sum(jnp.where(lane == block, order, 0.0), axis=1, keepdims=True)
        chosen = source == (lane & 15).astype(F32)
        return jnp.sum(jnp.where(chosen, value, 0.0), axis=0, keepdims=True)

    row_ref[...] = jnp.broadcast_to(rows_of(me), (8, LANES)).astype(I32)
    scr[...] = jnp.full((8, LANES), -1.0, F32)
    nbr_all = nbr_ref[...]
    away_all = ((nbr_all >> 7) != me) & (wall_ref[...] == 0)
    scr[0:6, :] = jnp.where(away_all, nbr_all >> 7, -1).astype(F32)
    neighbour = jnp.max(scr[...], axis=1, keepdims=True).astype(I32)
    low_half = lane < 64
    picks = jnp.zeros(shape, F32)
    for axis in range(3):
        lanes = slice(axis * LANES, axis * LANES + LANES)
        places, codes, walls = [], [], []
        for side in range(2):
            face = 2 * axis + side
            nbr = nbr_ref[face : face + 1, :]
            is_wall = wall_ref[face : face + 1, :] == 1
            remote = ((nbr >> 7) != me) & jnp.logical_not(is_wall)
            wanted = column(jnp.where(remote, nbr & 127, -1).astype(F32), diag)
            hit = rows_of(neighbour[face : face + 1, :]) == wanted
            place = jnp.sum(jnp.where(hit, lane.astype(F32), 0.0), axis=1, keepdims=True).astype(I32)
            places.append(place >> 4)
            chosen = (lane >> 4 == face) & (lane & 15 == place & 15) & (wanted >= 0.0)
            picks = jnp.where(chosen, 1.0, picks)
            codes.append(column(orient_ref[face : face + 1, :].astype(F32), diag).astype(I32))
            walls.append(column(jnp.where(is_wall, 1.0, 0.0), diag))
        code = jnp.where(low_half, codes[0], codes[1])
        code = jnp.where(jnp.where(low_half, walls[0], walls[1]) > 0.0, 0, code)
        a, b = (lane >> 3) & 7, lane & 7
        swap = code >= 4
        a1, b1 = jnp.where(swap, b, a), jnp.where(swap, a, b)
        a2 = jnp.where((code & 1) == 1, 7 - a1, a1)
        b2 = jnp.where((code & 2) == 2, 7 - b1, b1)
        near_ref[lanes, :] = jnp.where(low_half, 64, 0) + a2 * 8 + b2
        h = jnp.where(low_half, 1, 0)
        if axis == 0:
            top = ((a2 >> 2) ^ h) * 8 + ((b2 >> 2) ^ h) * 4
            group, v = top + ((a2 ^ b2) & 3), a2 & 3
        elif axis == 1:
            top = ((a2 >> 2) ^ h) * 8 + (((a2 >> 1) & 1) ^ (b2 >> 2)) * 4
            group, v = top + ((b2 & 3) ^ (h * 3)), (a2 & 1) * 2 + (b2 >> 2)
        else:
            top = ((a2 >> 2) ^ (b2 >> 2)) * 8 + (((a2 >> 1) & 1) ^ h) * 4
            group, v = top + ((b2 & 3) ^ (h * 3)), (a2 & 1) * 2 + (b2 >> 2)
        far_ref[lanes, :] = jnp.where(low_half, places[0], places[1]) * 16 + group + 128 * v
    pick_ref[...] = picks


SHIFT_A, SHIFT_B = (3, 9)


def shift_of(i):
    return (i & 3) ^ ((i >> 2) & 1) * (4 * SHIFT_A) ^ (i >> 3) * (4 * SHIFT_B)


def forward_kernel(me_ref, spot_ref, owner_ref, in_ref, label_ref, out_ref, zed_ref, held, faces):
    def one(source, carry):
        base = pl.multiple_of(source * 32, 32)

        @pl.when(spot_ref[base] >= 0)
        def _():
            for j in range(32):
                held[pl.ds(spot_ref[base + j], 1), :] = in_ref[pl.ds(source * 33 + j, 1), :]

        return carry

    lax.fori_loop(0, DEVS, one, 0)
    shape = (LANES, LANES)
    lane = iota(shape, 1)
    zeds = in_ref[pl.ds(32, LANES, stride=33), :]
    zed_ref[...] = zeds
    zed = jnp.take_along_axis(zeds, label_ref[...], axis=1)
    me = me_ref[0]
    g3, g2, g1, g0 = (me >> 3) & 1, (me >> 2) & 1, (me >> 1) & 1, me & 1
    lane = iota((8, LANES), 1)
    h, v1, v0 = lane >> 6, (lane >> 1) & 1, lane & 1
    nodes = [
        h * 16 + (g3 ^ h) * 8 + v1 * 4 + v0 * 2 + (g2 ^ h),
        v1 * 16 + h * 14 + v0,
        v1 * 16 + v0 * 8 + (g1 ^ h) * 4 + (g0 ^ h) * 2 + h,
    ]
    here = (lane >> 2) & 15
    shift = (here & 3) ^ ((here >> 2) & 1) * (4 * SHIFT_A) ^ (here >> 3) * (4 * SHIFT_B)
    which = []
    for axis in range(3):
        for field in (0, 1 + axis):
            value = jnp.full((8, LANES), -1, I32)
            for i in range(16):
                spot = lane ^ shift_of(i)
                n = spot >> 2
                i0, j2, j1, j0, k2 = (n >> 4) & 1, (n >> 3) & 1, (n >> 2) & 1, (n >> 1) & 1, n & 1
                if axis == 0:
                    hit = (j2 == g3 ^ i0) & (k2 == g2 ^ i0)
                elif axis == 1:
                    hit = (j2 == j1) & (j1 == j0)
                else:
                    hit = (j1 == g1 ^ k2) & (j0 == g0 ^ k2)
                value = jnp.where(hit & (spot & 3 == field), i, value)
            which.append(value)
    sign = half_sign((8, LANES))
    for block in range(16):
        merged = [jnp.zeros((8, LANES), F32)] * 6
        for i in range(16):
            rows = held[pl.ds(block * 128 + i, 8, stride=16), :]
            rows = jnp.take_along_axis(rows, lane ^ shift_of(i), axis=1)
            for m in range(6):
                merged[m] = jnp.where(which[m] == i, rows, merged[m])
        wide = jnp.take_along_axis(zed[block * 8 : block * 8 + 8, :], here, axis=1) * sign
        for axis in range(3):
            press = jnp.take_along_axis(merged[2 * axis], (nodes[axis] * 4) ^ shift, axis=1)
            speed = jnp.take_along_axis(merged[2 * axis + 1], (nodes[axis] * 4 + 1 + axis) ^ shift, axis=1)
            at = axis * LANES + block * 8
            faces[at : at + 8, :] = press + wide * speed
        for target in range(block * 8, block * 8 + 8):
            out_ref[target * 19 : target * 19 + 16, :] = held[target * 16 : target * 16 + 16, :]
    low = iota((1, LANES), 1) < 64

    def two(target, carry):
        for axis in range(3):
            lower = jnp.maximum(owner_ref[2 * axis * LANES + target], 0)
            upper = jnp.maximum(owner_ref[(2 * axis + 1) * LANES + target], 0)
            row = jnp.where(
                low, faces[pl.ds(axis * LANES + upper, 1), :], faces[pl.ds(axis * LANES + lower, 1), :]
            )
            out_ref[pl.ds(target * 19 + 16 + axis, 1), :] = row
        return carry

    lax.fori_loop(0, DEVS, two, 0, unroll=4)


def across_kernel(me_ref, owner_ref, zed_ref, nbr_ref, wall_ref, out_ref):
    shape = (LANES, LANES)
    lane = iota(shape, 1)
    diag = iota(shape, 0) == lane
    me = me_ref[0]
    own = zed_ref[pl.ds(me, 1), :]
    total = jnp.zeros(shape, F32)
    for face in range(6):
        other = zed_ref[pl.ds(jnp.maximum(owner_ref[face * LANES + me], 0), 1), :]
        nbr = nbr_ref[face : face + 1, :]
        remote = ((nbr >> 7) != me) & (wall_ref[face : face + 1, :] == 0)
        far = column(jnp.where(remote, 1.0, 0.0), diag) > 0.0
        spot = column((nbr & 127).astype(F32), diag) == lane.astype(F32)
        value = jnp.where(spot, jnp.where(far, other, own), 0.0)
        total = jnp.where(lane == face, jnp.sum(value, axis=1, keepdims=True), total)
    out_ref[...] = total


def final_kernel(
    me_ref, in_ref, row_ref, cols_ref, zed_ref, far_ref, near_ref, pick_ref, nbr_ref, wall_ref,
    side_ref, stack_ref, coef_ref, out_ref, state, turned,
):
    shape = (LANES, LANES)
    lane = iota(shape, 1)
    diag = iota(shape, 0) == lane
    low_half = lane < 64
    place = jnp.where(row_ref[0:1, :] == iota(shape, 0), 1.0, 0.0).astype(BF16)
    place = jnp.concatenate([place, place, place], axis=1)
    for group in range(0, 16, 2):
        pair = []
        for g in (group, group + 1):
            rows = [in_ref[(k * 16 + g) * 19 : (k * 16 + g) * 19 + 16, :] for k in range(8)]
            pair.append(jnp.concatenate(rows, axis=0))
        parts = split3(jnp.concatenate(pair, axis=1))
        moved = jnp.dot(place, jnp.concatenate(parts, axis=0), preferred_element_type=F32)
        state[group * LANES : (group + 1) * LANES, :] = moved[:, 0:LANES]
        state[(group + 1) * LANES : (group + 2) * LANES, :] = moved[:, LANES:]
    for block in range(16):
        at = [c * LANES + block * 8 for c in range(16)]
        chunks = regroup([state[a : a + 8, :] for a in at], True)
        for c in range(16):
            state[at[c] : at[c] + 8, :] = chunks[c]

    def chunk(field, n4):
        start = (n4 * 4 + field) * LANES
        return state[start : start + LANES, :]

    zed, bulk, dens = cols_ref[:, 0:1], cols_ref[:, 1:2], cols_ref[:, 2:3]
    me = me_ref[0]
    i2, j, k = lane >> 6, (lane >> 3) & 7, lane & 7
    sign = half_sign(shape)
    lifts = []
    for axis in range(3):
        rows = slice(axis * LANES, axis * LANES + LANES)
        press, norm, wave = face_pair(chunk, axis, zed)
        turned[...] = in_ref[pl.ds(16 + axis, LANES, stride=19), :].T
        nears, walls, fars = [], [], []
        for side in range(2):
            face = 2 * axis + side
            nbr = nbr_ref[face : face + 1, :]
            is_wall = wall_ref[face : face + 1, :] == 1
            local = ((nbr >> 7) == me) & jnp.logical_not(is_wall)
            spot = column(jnp.where(local, nbr & 127, -1).astype(F32), diag)
            nears.append(jnp.where(spot == lane.astype(F32), 1.0, 0.0))
            walls.append(column(jnp.where(is_wall, 1.0, 0.0), diag))
            table = [turned[pl.ds((1 - side) * 64 + v, 16, stride=4), :] for v in range(4)]
            pick = pick_ref[:, face * 16 : face * 16 + 16]
            fars.append(pick_dot(pick, jnp.concatenate(table, axis=1)))
        masked = jnp.concatenate([jnp.where(low_half, 0.0, wave), jnp.where(low_half, wave, 0.0)], axis=0)
        near = pick_dot(jnp.concatenate(nears, axis=1), masked)
        own = jnp.where(low_half, walls[1], walls[0]) > 0.0
        near = jnp.where(own, pltpu.roll(wave, 64, 1), near)
        wave_out = jnp.take_along_axis(near, near_ref[rows, :], axis=1)
        code = far_ref[rows, :]
        index, part = code & 127, code >> 7
        far = jnp.zeros(shape, F32)
        for v in range(4):
            below = jnp.take_along_axis(fars[0][:, v * LANES : (v + 1) * LANES], index, axis=1)
            above = jnp.take_along_axis(fars[1][:, v * LANES : (v + 1) * LANES], index, axis=1)
            far = jnp.where(part == v, jnp.where(low_half, below, above), far)
        zed_out = jnp.where(low_half, zed_ref[:, 2 * axis : 2 * axis + 1], zed_ref[:, 2 * axis + 1 : 2 * axis + 2])
        lifts.append((wave_out + far - press + zed_out * norm) / (zed + zed_out))

    high = lax.Precision.HIGHEST
    by_bulk = -metric_scale * bulk
    by_dens = -(metric_scale / dens)
    up = LIFT * bulk
    across = -LIFT * zed / dens
    swapped = {}
    for field in (0, 1):
        for n4 in range(4):
            swapped[field, n4] = pltpu.roll(chunk(field, n4), 64, 1)
    for n4 in range(4):
        along = {}
        for field in (0, 1):
            total = None
            for m4 in range(4):
                at = (n4 * 4 + m4) * 2
                term = chunk(field, m4) * coef_ref[at : at + 1, :]
                term = term + swapped[field, m4] * coef_ref[at + 1 : at + 2, :]
                total = term if total is None else total + term
            along[field] = total
        both = jnp.concatenate([chunk(2, n4), chunk(3, n4)], axis=1)
        div = along[1] + jnp.dot(both, stack_ref[...], precision=high, preferred_element_type=F32)
        grad = jnp.dot(chunk(0, n4), side_ref[...], precision=high, preferred_element_type=F32)
        grads = [along[0], grad[:, 0:LANES], grad[:, LANES:]]
        face_i = 2 * n4 + i2
        from_y = jnp.where(j == 7, 64, 0) + face_i * 8 + k
        from_z = jnp.where(k == 7, 64, 0) + face_i * 8 + j
        on_y = (j == 0) | (j == 7)
        on_z = (k == 0) | (k == 7)
        total = jnp.zeros(shape, F32)
        for axis in range(3):
            jump = lifts[axis]
            value = by_dens * grads[axis]
            here = None
            if axis == 0 and n4 == 0:
                here = jnp.where(low_half, jump, 0.0)
                turn = -here
            elif axis == 0 and n4 == 3:
                here = jnp.where(low_half, 0.0, jump)
                turn = here
            elif axis == 1:
                here = jnp.where(on_y, jnp.take_along_axis(jump, from_y, axis=1), 0.0)
                turn = jnp.where(j == 0, -here, here)
            elif axis == 2:
                here = jnp.where(on_z, jnp.take_along_axis(jump, from_z, axis=1), 0.0)
                turn = jnp.where(k == 0, -here, here)
            if here is not None:
                value = value + across * turn
                total = total + here
            out_ref[pl.ds(n4 * 4 + 1 + axis, LANES, stride=16), :] = value
        out_ref[pl.ds(n4 * 4, LANES, stride=16), :] = by_bulk * div + up * total


def vm():
    return pl.BlockSpec(memory_space=VMEM)


def sm():
    return pl.BlockSpec(memory_space=SMEM)


def shaped(shape, dtype=F32):
    return VMEM(shape, dtype)


def plain(shape, dtype=F32):
    return jax.ShapeDtypeStruct(shape, dtype)


def near(value):
    return pltpu.with_memory_space_constraint(value, VMEM)


def away(value):
    return pltpu.with_memory_space_constraint(value, HBM)


GRANT = pltpu.CompilerParams(vmem_limit_bytes=24 * 1024 * 1024)


def exchange(flat, rows):
    blocks = flat.reshape(DEVS, rows, 1, LANES)
    return lax.all_to_all(blocks, AXES, split_axis=0, concat_axis=0, tiled=True).reshape(flat.shape)


def body(old_state, dest_row, neighbours, orientation, wall_flags, bulk_modulus, density):
    me = (lax.axis_index("grp") * lax.axis_size("dev") + lax.axis_index("dev")).astype(I32).reshape(1)
    dest = dest_row.reshape(2, LANES)
    bulk = away(bulk_modulus.reshape(1, LANES))
    dens = away(density.reshape(1, LANES))
    nbr, wall, orient = away(neighbours), away(wall_flags), away(orientation)
    state = old_state.reshape(256, 4, 4, LANES).transpose(0, 2, 1, 3).reshape(4096, LANES)

    info, pos = pl.pallas_call(
        order_kernel,
        in_specs=[sm()] + [vm()] * 3,
        out_specs=[vm()] * 2,
        out_shape=[shaped((384, LANES), I32), plain((2, LANES), I32)],
        scratch_shapes=[pltpu.VMEM((8, LANES), F32)],
        name="order",
        compiler_params=GRANT,
    )(me, away(dest), nbr, wall)
    heard = exchange(info, 3)
    pieces = pl.pallas_call(
        pack_kernel,
        in_specs=[sm(), sm()] + [vm()] * 3,
        out_specs=vm(),
        out_shape=HBM((4224, LANES), F32),
        scratch_shapes=[pltpu.VMEM((4096, LANES), F32)],
        name="pack",
        compiler_params=GRANT,
    )(pos, dest, away(state), bulk, dens)
    spread = exchange(pieces, 33)
    spots, owners, rows, labels, cols, far, close, pick = pl.pallas_call(
        table_kernel,
        in_specs=[sm()] + [vm()] * 6,
        out_specs=[vm()] * 8,
        out_shape=[
            shaped((32, LANES), I32),
            shaped((8, LANES), I32),
            shaped((8, LANES), I32),
            shaped((LANES, LANES), I32),
            shaped((LANES, LANES)),
            HBM((384, LANES), I32),
            HBM((384, LANES), I32),
            shaped((LANES, LANES)),
        ],
        scratch_shapes=[pltpu.VMEM((LANES, LANES), I32), pltpu.VMEM((8, LANES), F32)],
        name="table",
        compiler_params=GRANT,
    )(me, near(heard), nbr, wall, orient, bulk, dens)
    owners = owners.reshape(1024)
    passed, zeds = pl.pallas_call(
        forward_kernel,
        in_specs=[sm()] * 3 + [vm()] * 2,
        out_specs=[vm()] * 2,
        out_shape=[shaped((2432, LANES)), shaped((LANES, LANES))],
        scratch_shapes=[pltpu.VMEM((2048, LANES), F32), pltpu.VMEM((384, LANES), F32)],
        name="forward",
        compiler_params=GRANT,
    )(me, spots.reshape(4096), owners, near(spread), near(labels))
    arrived = exchange(passed, 19)
    zed_out = pl.pallas_call(
        across_kernel,
        in_specs=[sm()] * 2 + [vm()] * 3,
        out_specs=vm(),
        out_shape=shaped((LANES, LANES)),
        name="across",
        compiler_params=GRANT,
    )(me, owners, near(zeds), nbr, wall)
    result = pl.pallas_call(
        final_kernel,
        in_specs=[sm()] + [vm()] * 12,
        out_specs=vm(),
        out_shape=plain((2048, LANES)),
        scratch_shapes=[pltpu.VMEM((2048, LANES), F32), pltpu.VMEM((LANES, LANES), F32)],
        name="final",
        compiler_params=GRANT,
    )(
        me, near(arrived), near(rows), near(cols), near(zed_out), away(far), away(close), near(pick), nbr, wall,
        away(jnp.asarray(SIDE)), away(jnp.asarray(STACKED)), away(jnp.asarray(COEF)),
    )
    return result.reshape(128, 4, 4, LANES).transpose(0, 2, 1, 3).reshape(128, 4, 512)


def solution(mesh):
    both = P(AXES)
    faces = P(None, AXES)
    in_specs = (P(AXES, None, None), both, faces, faces, faces, both, both)
    return jax.shard_map(
        body, mesh=mesh, in_specs=in_specs, out_specs=P(AXES, None, None), check_vma=False
    )
```

```python
import jax
import jax.numpy as jnp
import numpy as np
from jax import lax
from jax.experimental import pallas as pl
from jax.experimental.pallas import tpu as pltpu
from jax.sharding import PartitionSpec as P

NP = 8
DEVS = 128
LANES = 128
AXES = ("grp", "dev")
metric_scale = 0.25
F32 = jnp.float32
I32 = jnp.int32
BF16 = jnp.bfloat16
VMEM = pltpu.MemorySpace.VMEM
SMEM = pltpu.MemorySpace.SMEM
HBM = pltpu.MemorySpace.HBM


def gll_tables(poly_order):
    num_points = poly_order + 1
    points = -np.cos(np.pi * np.arange(num_points) / poly_order)
    legendre = np.zeros((num_points, num_points))
    for sweeps in range(101):
        legendre[:, 0] = 1.0
        legendre[:, 1] = points
        for degree in range(2, num_points):
            legendre[:, degree] = (
                (2 * degree - 1) * points * legendre[:, degree - 1]
                - (degree - 1) * legendre[:, degree - 2]
            ) / degree
        if sweeps < 100:
            points = points - (points * legendre[:, poly_order] - legendre[:, poly_order - 1]) / (
                num_points * legendre[:, poly_order]
            )
    end_values = legendre[:, poly_order]
    weights = 2.0 / (poly_order * num_points * end_values**2)
    distance = points[:, None] - points[None, :] + np.eye(num_points)
    derivative = end_values[:, None] / end_values[None, :] / distance
    derivative = derivative * (1.0 - np.eye(num_points))
    derivative[0, 0] = -poly_order * num_points / 4.0
    derivative[poly_order, poly_order] = poly_order * num_points / 4.0
    return (points, weights, derivative)


POINTS, WEIGHTS, DERIV = gll_tables(NP - 1)
DERIV = DERIV.astype(np.float32)
LIFT = metric_scale / float(WEIGHTS[0])


def derivative_tables():
    eye2, eye8 = np.eye(2, dtype=np.float32), np.eye(8, dtype=np.float32)
    along_y = np.kron(eye2, np.kron(DERIV.T, eye8))
    along_z = np.kron(eye2, np.kron(eye8, DERIV.T))
    side = np.concatenate([along_y, along_z], axis=1)
    stacked = np.concatenate([along_y, along_z], axis=0)
    coef = np.zeros((4, 4, 2, LANES), np.float32)
    for out_chunk in range(4):
        for in_chunk in range(4):
            for half in range(2):
                lanes = slice(64 * half, 64 * half + 64)
                coef[out_chunk, in_chunk, 0, lanes] = DERIV[2 * out_chunk + half, 2 * in_chunk + half]
                coef[out_chunk, in_chunk, 1, lanes] = DERIV[
                    2 * out_chunk + half, 2 * in_chunk + 1 - half
                ]
    return side, stacked, coef.reshape(32, LANES)


SIDE, STACKED, COEF = derivative_tables()


def three_parts(table):
    high = table.astype(jnp.bfloat16)
    low = (table - high.astype(np.float32)).astype(jnp.bfloat16)
    return np.concatenate([high, high, low], axis=0)


SIDE3, STACKED3 = three_parts(SIDE), three_parts(STACKED)


def iota(shape, axis):
    return lax.broadcasted_iota(I32, shape, axis)


def small_dot(left, right):
    return jnp.dot(left.astype(BF16), right.astype(BF16), preferred_element_type=F32)


def split3(value):
    high = value.astype(BF16)
    rest = value - high.astype(F32)
    middle = rest.astype(BF16)
    low = (rest - middle.astype(F32)).astype(BF16)
    return high, middle, low


def pick_dot(pick, value):
    pick = pick.astype(BF16)
    high, middle, low = split3(value)
    total = jnp.dot(pick, high, preferred_element_type=F32)
    total = total + jnp.dot(pick, middle, preferred_element_type=F32)
    return total + jnp.dot(pick, low, preferred_element_type=F32)


def column(row, diag):
    wide = jnp.broadcast_to(row, (LANES, LANES))
    return jnp.sum(jnp.where(diag, wide, 0.0), axis=1, keepdims=True)


def half_sign(shape):
    return jnp.where(iota(shape, 1) < 64, -1.0, 1.0)


def face_pair(chunk, axis, zed):
    lane = iota((LANES, LANES), 1)
    half, face_i, face_b = lane >> 6, (lane >> 3) & 7, lane & 7
    from_y = (face_i & 1) * 64 + half * 56 + face_b
    from_z = (face_i & 1) * 64 + face_b * 8 + half * 7
    values = []
    for field in (0, 1 + axis):
        if axis == 0:
            value = jnp.where(lane < 64, chunk(field, 0), chunk(field, 3))
        else:
            index = from_y if axis == 1 else from_z
            value = jnp.take_along_axis(chunk(field, 0), index, axis=1)
            for n4 in range(1, 4):
                other = jnp.take_along_axis(chunk(field, n4), index, axis=1)
                value = jnp.where(face_i >> 1 == n4, other, value)
        values.append(value)
    normal = half_sign((LANES, LANES)) * values[1]
    return values[0], normal, values[0] + zed * normal


def cross(arrays, bit1, bit0):
    first = [jnp.where(bit0, arrays[t ^ 1], arrays[t]) for t in range(4)]
    return [jnp.where(bit1, first[t ^ 2], first[t]) for t in range(4)]


def lane_bit(lane, bit):
    return ((lane >> bit) & 1) == 1


def regroup(arrays, back):
    lane = iota(arrays[0].shape, 1)
    own = (lane >> 3) & 3
    plain = (lane_bit(lane, 1), lane_bit(lane, 0))
    mixed = (lane_bit(lane ^ (lane >> 3), 1), lane_bit(lane ^ (lane >> 3), 0))
    enter, leave = (plain, mixed) if back else (mixed, plain)
    result = [None] * 16
    for top in range(4):
        four = cross(arrays[4 * top : 4 * top + 4], *enter)
        four = [jnp.take_along_axis(four[t], lane ^ t ^ own, axis=1) for t in range(4)]
        result[4 * top : 4 * top + 4] = cross(four, *leave)
    j2, k2 = lane_bit(lane, 5), lane_bit(lane, 2)
    final = [None] * 16
    for t in range(4):
        final[t::4] = cross(result[t::4], j2, k2)
    return final


def order_kernel(me_ref, dest_ref, nbr_ref, wall_ref, info_ref, pos_ref, scr):
    dest = dest_ref[...]
    sub = iota((LANES, LANES), 0)
    lane = iota((LANES, LANES), 1)
    diag = sub == lane
    key_row, key_col, dest_col = [], [], []
    for half in range(2):
        row = jnp.broadcast_to(dest[half : half + 1, :], (LANES, LANES))
        key = (row >> 7).astype(F32) * 256.0 + (lane + 128 * half).astype(F32)
        key_row.append(key)
        key_col.append(jnp.sum(jnp.where(diag, key, 0.0), axis=1, keepdims=True))
        dest_col.append(jnp.sum(jnp.where(diag, row.astype(F32), 0.0), axis=1, keepdims=True))
    lists = [jnp.zeros((1, LANES), F32), jnp.zeros((1, LANES), F32)]
    for half in range(2):
        before_col = jnp.zeros((LANES, 1), F32)
        before_row = jnp.zeros((1, LANES), F32)
        for other in range(2):
            before_col = before_col + jnp.sum(
                jnp.where(key_row[other] < key_col[half], 1.0, 0.0), axis=1, keepdims=True
            )
            before_row = before_row + jnp.sum(
                jnp.where(key_col[other] < key_row[half], 1.0, 0.0), axis=0, keepdims=True
            )
        pos_ref[half : half + 1, :] = before_row.astype(I32)
        place = before_col.astype(I32)
        k = place & 7
        spot = (k & 3) * 32 + (place >> 3)
        for part in range(2):
            hit = (spot == lane) & (k >> 2 == part)
            lists[part] = lists[part] + jnp.sum(jnp.where(hit, dest_col[half], 0.0), axis=0, keepdims=True)
    scr[...] = jnp.full((8, LANES), -1.0, F32)
    owner = nbr_ref[...] >> 7
    remote = (owner != me_ref[0]) & (wall_ref[...] == 0)
    scr[0:6, :] = jnp.where(remote, owner, -1).astype(F32)
    owners = jnp.max(scr[...], axis=1, keepdims=True)
    spread = iota((8, LANES), 0) == iota((8, LANES), 1)
    owner_row = jnp.sum(jnp.where(spread, owners, 0.0), axis=0, keepdims=True)
    for part, row in enumerate((lists[0], lists[1], owner_row)):
        info_ref[pl.ds(part, LANES, stride=3), :] = jnp.broadcast_to(row, (LANES, LANES)).astype(I32)


def pack_kernel(pos_ref, dest_ref, state_ref, bulk_ref, dens_ref, out_ref, scr):
    zed = jnp.sqrt(bulk_ref[...] * dens_ref[...])
    out_ref[pl.ds(32, LANES, stride=33), :] = jnp.broadcast_to(zed, (LANES, LANES))

    @pl.when(dest_ref[0, 0] >= 0)
    def _():
        def one(slot, carry):
            place = pos_ref[slot >> 7, slot & 127]
            start = (place & 7) * 512 + (place >> 3)
            scr[pl.ds(start, 16, stride=32), :] = state_ref[pl.ds(pl.multiple_of(slot * 16, 16), 16), :]
            return carry

        lax.fori_loop(0, 256, one, 0, unroll=8)
        for k in range(8):
            for block in range(4):
                at = [(k * 16 + c) * 32 + block * 8 for c in range(16)]
                groups = regroup([scr[a : a + 8, :] for a in at], False)
                for g in range(16):
                    row = (k * 16 + g) * 33 + block * 8
                    out_ref[row : row + 8, :] = groups[g]


def table_kernel(
    me_ref, info_ref, nbr_ref, wall_ref, orient_ref, bulk_ref, dens_ref,
    spot_ref, owner_ref, column_ref, row_ref, label_ref, cols_ref, far_ref, near_ref, pick_ref, wide, scr,
):
    shape = (LANES, LANES)
    sub = iota(shape, 0)
    lane = iota(shape, 1)
    diag = sub == lane
    me = me_ref[0]
    bulk = column(bulk_ref[...], diag)
    dens = column(dens_ref[...], diag)
    zed = column(jnp.sqrt(bulk_ref[...] * dens_ref[...]), diag)
    cols_ref[...] = jnp.where(lane == 0, zed, jnp.where(lane == 1, bulk, dens))

    lists = [info_ref[pl.ds(0, LANES, stride=3), :], info_ref[pl.ds(1, LANES, stride=3), :]]
    owners = info_ref[pl.ds(2, LANES, stride=3), :].astype(F32)
    owner_ref[...] = owners.T[0:8, :].astype(I32)
    column_ref[...] = owners
    target = lists[0] >> 7
    my_k = me >> 4
    mine = jnp.where(my_k >= 4, lists[1], lists[0])
    mine = jnp.take_along_axis(mine, (my_k & 3) * 32 + (lane & 31), axis=1) & 127
    present = jnp.zeros(shape, F32)
    label = jnp.zeros(shape, F32)
    mine = mine.astype(F32)
    for j in range(32):
        hit = target[:, j : j + 1] == lane
        present = jnp.where(hit, 1.0, present)
        label = jnp.where(hit, mine[:, j : j + 1], label)
    below = jnp.where(lane < sub, 1.0, 0.0)
    rank = small_dot(below, present)
    safe = jnp.clip(target, 0, LANES - 1)
    slot = safe * 16 + jnp.take_along_axis(rank.astype(I32), safe, axis=1)
    is_source = jnp.broadcast_to(jnp.where(target[:, 0:1] >= 0, 1.0, 0.0), shape)
    source_rank = jnp.where(is_source > 0.0, small_dot(below, is_source), -1.0)
    chosen = jnp.where(source_rank.T == sub.astype(F32), 1.0, 0.0)
    wide[...] = pick_dot(chosen, jnp.where(lane == 32, sub, slot).astype(F32)).astype(I32)
    quarter = iota((16, LANES), 1) >> 5
    spots = wide[pl.ds(0, 16, stride=4), :]
    for part in range(1, 4):
        moved = pltpu.roll(wide[pl.ds(part, 16, stride=4), :], 32 * part, 1)
        spots = jnp.where(quarter == part, moved, spots)
    spot_ref[0:16, :] = spots
    sources = jnp.where(diag, jnp.broadcast_to(wide[:, 32:33], shape).astype(F32), 0.0)
    sources = jnp.sum(sources, axis=0, keepdims=True).astype(I32)
    spot_ref[16:24, :] = jnp.broadcast_to(sources, (8, LANES))
    order = jnp.where(present > 0.0, rank, -1.0)
    labels = jnp.zeros(shape, F32)
    for i in range(16):
        row = jnp.sum(jnp.where(order == float(i), label, 0.0), axis=0, keepdims=True)
        labels = jnp.where(sub == i, row, labels)
    label_ref[...] = labels.T.astype(I32)

    gather = [jnp.where((sub >> 5) + 4 * part == lane >> 4, 1.0, 0.0) for part in range(2)]

    def rows_of(block):
        value = jnp.zeros(shape, F32)
        for part in range(2):
            held = jnp.where(lists[part] >> 7 == block, (lists[part] & 127).astype(F32), 0.0)
            value = value + small_dot(held, gather[part])
        source = jnp.sum(jnp.where(lane == block, order, 0.0), axis=1, keepdims=True)
        chosen = source == (lane & 15).astype(F32)
        return jnp.sum(jnp.where(chosen, value, 0.0), axis=0, keepdims=True)

    row_ref[...] = jnp.broadcast_to(rows_of(me), (8, LANES)).astype(I32)
    scr[...] = jnp.full((8, LANES), -1.0, F32)
    nbr_all = nbr_ref[...]
    away_all = ((nbr_all >> 7) != me) & (wall_ref[...] == 0)
    scr[0:6, :] = jnp.where(away_all, nbr_all >> 7, -1).astype(F32)
    neighbour = jnp.max(scr[...], axis=1, keepdims=True).astype(I32)
    low_half = lane < 64
    picks = jnp.zeros(shape, F32)
    for axis in range(3):
        lanes = slice(axis * LANES, axis * LANES + LANES)
        places, codes, walls = [], [], []
        for side in range(2):
            face = 2 * axis + side
            nbr = nbr_ref[face : face + 1, :]
            is_wall = wall_ref[face : face + 1, :] == 1
            remote = ((nbr >> 7) != me) & jnp.logical_not(is_wall)
            wanted = column(jnp.where(remote, nbr & 127, -1).astype(F32), diag)
            hit = rows_of(neighbour[face : face + 1, :]) == wanted
            place = jnp.sum(jnp.where(hit, lane.astype(F32), 0.0), axis=1, keepdims=True).astype(I32)
            places.append(place >> 4)
            chosen = (lane >> 4 == face) & (lane & 15 == place & 15) & (wanted >= 0.0)
            picks = jnp.where(chosen, 1.0, picks)
            codes.append(column(orient_ref[face : face + 1, :].astype(F32), diag).astype(I32))
            walls.append(column(jnp.where(is_wall, 1.0, 0.0), diag))
        code = jnp.where(low_half, codes[0], codes[1])
        code = jnp.where(jnp.where(low_half, walls[0], walls[1]) > 0.0, 0, code)
        a, b = (lane >> 3) & 7, lane & 7
        swap = code >= 4
        a1, b1 = jnp.where(swap, b, a), jnp.where(swap, a, b)
        a2 = jnp.where((code & 1) == 1, 7 - a1, a1)
        b2 = jnp.where((code & 2) == 2, 7 - b1, b1)
        near_ref[lanes, :] = jnp.where(low_half, 64, 0) + a2 * 8 + b2
        h = jnp.where(low_half, 1, 0)
        if axis == 0:
            top = ((a2 >> 2) ^ h) * 8 + ((b2 >> 2) ^ h) * 4
            group, v = top + ((a2 ^ b2) & 3), a2 & 3
        elif axis == 1:
            top = ((a2 >> 2) ^ h) * 8 + (((a2 >> 1) & 1) ^ (b2 >> 2)) * 4
            group, v = top + ((b2 & 3) ^ (h * 3)), (a2 & 1) * 2 + (b2 >> 2)
        else:
            top = ((a2 >> 2) ^ (b2 >> 2)) * 8 + (((a2 >> 1) & 1) ^ h) * 4
            group, v = top + ((b2 & 3) ^ (h * 3)), (a2 & 1) * 2 + (b2 >> 2)
        far_ref[lanes, :] = jnp.where(low_half, places[0], places[1]) * 16 + group + 128 * v
    pick_ref[...] = picks


SHIFT_A, SHIFT_B = (3, 9)


def shift_of(i):
    return (i & 3) ^ ((i >> 2) & 1) * (4 * SHIFT_A) ^ (i >> 3) * (4 * SHIFT_B)


def forward_kernel(me_ref, spot_ref, in_ref, label_ref, column_ref, out_ref, zed_ref, held, made, sem):
    def one(number, carry):
        base = number * 32
        start = spot_ref[2048 + number] * 33
        for j in range(32):
            held[pl.ds(spot_ref[base + j], 1), :] = in_ref[pl.ds(start + j, 1), :]
        return carry

    lax.fori_loop(0, DEVS // 2, one, 0, unroll=2)
    shape = (LANES, LANES)
    lane = iota(shape, 1)
    zeds = in_ref[pl.ds(32, LANES, stride=33), :]
    zed_ref[...] = zeds
    zed = jnp.take_along_axis(zeds, label_ref[...], axis=1)
    me = me_ref[0]
    g3, g2, g1, g0 = (me >> 3) & 1, (me >> 2) & 1, (me >> 1) & 1, me & 1
    lane = iota((8, LANES), 1)
    h, v1, v0 = lane >> 6, (lane >> 1) & 1, lane & 1
    nodes = [
        h * 16 + (g3 ^ h) * 8 + v1 * 4 + v0 * 2 + (g2 ^ h),
        v1 * 16 + h * 14 + v0,
        v1 * 16 + v0 * 8 + (g1 ^ h) * 4 + (g0 ^ h) * 2 + h,
    ]
    here = (lane >> 2) & 15
    shift = (here & 3) ^ ((here >> 2) & 1) * (4 * SHIFT_A) ^ (here >> 3) * (4 * SHIFT_B)
    which = []
    for axis in range(3):
        for field in (0, 1 + axis):
            value = jnp.full((8, LANES), -1, I32)
            for i in range(16):
                spot = lane ^ shift_of(i)
                n = spot >> 2
                i0, j2, j1, j0, k2 = (n >> 4) & 1, (n >> 3) & 1, (n >> 2) & 1, (n >> 1) & 1, n & 1
                if axis == 0:
                    hit = (j2 == g3 ^ i0) & (k2 == g2 ^ i0)
                elif axis == 1:
                    hit = (j2 == j1) & (j1 == j0)
                else:
                    hit = (j1 == g1 ^ k2) & (j0 == g0 ^ k2)
                value = jnp.where(hit & (spot & 3 == field), i, value)
            which.append(value)
    sign = half_sign((8, LANES))
    waves = [[], [], []]
    for block in range(16):
        merged = [jnp.zeros((8, LANES), F32)] * 6
        for i in range(16):
            rows = held[pl.ds(block * 128 + i, 8, stride=16), :]
            rows = jnp.take_along_axis(rows, lane ^ shift_of(i), axis=1)
            for m in range(6):
                merged[m] = jnp.where(which[m] == i, rows, merged[m])
        wide = jnp.take_along_axis(zed[block * 8 : block * 8 + 8, :], here, axis=1) * sign
        for axis in range(3):
            press = jnp.take_along_axis(merged[2 * axis], (nodes[axis] * 4) ^ shift, axis=1)
            speed = jnp.take_along_axis(merged[2 * axis + 1], (nodes[axis] * 4 + 1 + axis) ^ shift, axis=1)
            waves[axis].append(press + wide * speed)
    low_half = iota(shape, 1) < 64
    lane = iota(shape, 1).astype(F32)
    halos = []
    for axis in range(3):
        wave = jnp.concatenate(waves[axis], axis=0)
        upper = column_ref[:, 2 * axis + 1 : 2 * axis + 2] == lane
        lower = column_ref[:, 2 * axis : 2 * axis + 1] == lane
        pick = jnp.concatenate([jnp.where(upper, 1.0, 0.0), jnp.where(lower, 1.0, 0.0)], axis=1)
        table = jnp.concatenate([jnp.where(low_half, wave, 0.0), jnp.where(low_half, 0.0, wave)], axis=0)
        halos.append(pick_dot(pick, table))
    copies = []
    for part in range(4):
        base = part * 32
        for target in range(base, base + 32):
            made[target * 19 : target * 19 + 16, :] = held[target * 16 : target * 16 + 16, :]
        for axis in range(3):
            made[pl.ds(base * 19 + 16 + axis, 32, stride=19), :] = halos[axis][base : base + 32, :]
        rows = pl.ds(base * 19, 608)
        copies.append(pltpu.make_async_copy(made.at[rows], out_ref.at[rows], sem.at[part]))
        copies[-1].start()
    for copy in copies:
        copy.wait()


def across_kernel(
    me_ref, owner_ref, zed_ref, nbr_ref, wall_ref, row_ref, cols_ref, pick_ref, out_ref, near_ref, place_ref, far_ref
):
    shape = (LANES, LANES)
    lane = iota(shape, 1)
    diag = iota(shape, 0) == lane
    me = me_ref[0]
    own = zed_ref[pl.ds(me, 1), :]
    cols = cols_ref[...]
    total = jnp.where(lane == 16, cols[:, 0:1], jnp.where(lane == 17, cols[:, 1:2], cols[:, 2:3]))
    for face in range(6):
        other = zed_ref[pl.ds(jnp.maximum(owner_ref[face * LANES + me], 0), 1), :]
        nbr = nbr_ref[face : face + 1, :]
        is_wall = wall_ref[face : face + 1, :] == 1
        remote = ((nbr >> 7) != me) & jnp.logical_not(is_wall)
        far = column(jnp.where(remote, 1.0, 0.0), diag) > 0.0
        spot = column((nbr & 127).astype(F32), diag) == lane.astype(F32)
        wall = column(jnp.where(is_wall, 1.0, 0.0), diag)
        value = jnp.where(spot, jnp.where(far, other, own), 0.0)
        total = jnp.where(lane == face, jnp.sum(value, axis=1, keepdims=True), total)
        total = jnp.where(lane == 8 + face, wall, total)
        local = jnp.where(far | (wall > 0.0), 0.0, jnp.where(spot, 1.0, 0.0))
        rows = slice(face // 2 * LANES, face // 2 * LANES + LANES)
        near_ref[rows, face % 2 * LANES : (face % 2 + 1) * LANES] = local.astype(BF16)
        source = face * 16 + (lane & 15)
        pick = jnp.take_along_axis(pick_ref[...], source, axis=1)
        far_ref[face * LANES : (face + 1) * LANES, :] = jnp.where(lane < 48, pick, 0.0).astype(BF16)
    out_ref[...] = total
    place_ref[...] = jnp.where(row_ref[0:1, :] == iota(shape, 0), 1.0, 0.0).astype(BF16)


def final_kernel(
    in_ref, place_ref, misc_ref, hot_ref, pick_ref, far_ref, near_ref, side_ref, stack_ref, coef_ref,
    out_ref, state, turned, lift, loose, made, sem,
):
    shape = (LANES, LANES)
    lane = iota(shape, 1)
    low_half = lane < 64
    place = place_ref[...]
    place = jnp.concatenate([place, place, place], axis=1)
    for group in range(0, 16, 2):
        pair = []
        for g in (group, group + 1):
            rows = [in_ref[(k * 16 + g) * 19 : (k * 16 + g) * 19 + 16, :] for k in range(8)]
            pair.append(jnp.concatenate(rows, axis=0))
        parts = split3(jnp.concatenate(pair, axis=1))
        moved = jnp.dot(place, jnp.concatenate(parts, axis=0), preferred_element_type=F32)
        state[group * LANES : (group + 1) * LANES, :] = moved[:, 0:LANES]
        state[(group + 1) * LANES : (group + 2) * LANES, :] = moved[:, LANES:]
    for block in range(16):
        at = [c * LANES + block * 8 for c in range(16)]
        chunks = regroup([state[a : a + 8, :] for a in at], True)
        for c in range(16):
            state[at[c] : at[c] + 8, :] = chunks[c]

    def chunk(field, n4):
        start = (n4 * 4 + field) * LANES
        return state[start : start + LANES, :]

    zed = misc_ref[:, 16:17]
    for axis in range(3):
        rows = slice(axis * LANES, axis * LANES + LANES)
        press, norm, wave = face_pair(chunk, axis, zed)
        turned[...] = in_ref[pl.ds(16 + axis, LANES, stride=19), :].T
        fars = []
        for side in range(2):
            face = 2 * axis + side
            table = [turned[pl.ds((1 - side) * 64 + v, 16, stride=4), :] for v in range(4)]
            table = jnp.concatenate(split3(jnp.concatenate(table, axis=1)), axis=0)
            pick = pick_ref[face * LANES : (face + 1) * LANES, 0:48]
            fars.append(jnp.dot(pick, table, preferred_element_type=F32))
        masked = jnp.concatenate([jnp.where(low_half, 0.0, wave), jnp.where(low_half, wave, 0.0)], axis=0)
        hot = hot_ref[rows, :]
        near = jnp.dot(
            jnp.concatenate([hot, hot, hot], axis=1),
            jnp.concatenate(split3(masked), axis=0),
            preferred_element_type=F32,
        )
        first, second = 2 * axis, 2 * axis + 1
        wall = jnp.where(low_half, misc_ref[:, 8 + second : 9 + second], misc_ref[:, 8 + first : 9 + first])
        near = jnp.where(wall > 0.0, pltpu.roll(wave, 64, 1), near)
        total = jnp.take_along_axis(near, near_ref[rows, :], axis=1)
        code = far_ref[rows, :]
        index, part = code & 127, code >> 7
        far = jnp.zeros(shape, F32)
        for v in range(4):
            below = jnp.take_along_axis(fars[0][:, v * LANES : (v + 1) * LANES], index, axis=1)
            above = jnp.take_along_axis(fars[1][:, v * LANES : (v + 1) * LANES], index, axis=1)
            far = jnp.where(part == v, jnp.where(low_half, below, above), far)
        zed_out = jnp.where(low_half, misc_ref[:, first : first + 1], misc_ref[:, second : second + 1])
        lift[rows, :] = (total + far - press + zed_out * norm) / (zed + zed_out)

    lane = iota((32, LANES), 1)
    low_half = lane < 64
    i2, j, k = lane >> 6, (lane >> 3) & 7, lane & 7
    on_y, on_z = (j == 0) | (j == 7), (k == 0) | (k == 7)
    copies = []
    for part in range(4):
        rows = slice(part * 32, part * 32 + 32)
        zed, bulk, dens = misc_ref[rows, 16:17], misc_ref[rows, 17:18], misc_ref[rows, 18:19]
        by_bulk = -metric_scale * bulk
        by_dens = -(metric_scale / dens)
        up = LIFT * bulk
        across = -LIFT * zed / dens
        piece = {}
        for field in range(4):
            for n4 in range(4):
                start = (n4 * 4 + field) * LANES + part * 32
                piece[field, n4] = state[start : start + 32, :]
        cut = []
        for field in (0, 2, 3):
            whole = jnp.concatenate([piece[field, n4] for n4 in range(4)], axis=0)
            high = whole.astype(BF16)
            cut.append((high, (whole - high.astype(F32)).astype(BF16)))
        grad = jnp.dot(
            jnp.concatenate([cut[0][0], cut[0][1], cut[0][0]], axis=1), side_ref[...], preferred_element_type=F32
        )
        across_div = jnp.dot(
            jnp.concatenate([cut[1][0], cut[2][0], cut[1][1], cut[2][1], cut[1][0], cut[2][0]], axis=1),
            stack_ref[...],
            preferred_element_type=F32,
        )
        swapped = {}
        for field in (0, 1):
            for n4 in range(4):
                swapped[field, n4] = pltpu.roll(piece[field, n4], 64, 1)
        jumps = [lift[axis * LANES + part * 32 : axis * LANES + part * 32 + 32, :] for axis in range(3)]
        base = part * 544
        for n4 in range(4):
            along = {}
            for field in (0, 1):
                total = None
                for m4 in range(4):
                    at = (n4 * 4 + m4) * 2
                    term = piece[field, m4] * coef_ref[at : at + 1, :]
                    term = term + swapped[field, m4] * coef_ref[at + 1 : at + 2, :]
                    total = term if total is None else total + term
                along[field] = total
            block = slice(n4 * 32, n4 * 32 + 32)
            div = along[1] + across_div[block, :]
            grads = [along[0], grad[block, 0:LANES], grad[block, LANES:]]
            face_i = 2 * n4 + i2
            from_y = jnp.where(j == 7, 64, 0) + face_i * 8 + k
            from_z = jnp.where(k == 7, 64, 0) + face_i * 8 + j
            total = None
            for axis in range(3):
                jump = jumps[axis]
                value = by_dens * grads[axis]
                here = None
                if axis == 0 and n4 == 0:
                    here = jnp.where(low_half, jump, 0.0)
                    turn = -here
                elif axis == 0 and n4 == 3:
                    here = jnp.where(low_half, 0.0, jump)
                    turn = here
                elif axis == 1:
                    here = jnp.where(on_y, jnp.take_along_axis(jump, from_y, axis=1), 0.0)
                    turn = jnp.where(j == 0, -here, here)
                elif axis == 2:
                    here = jnp.where(on_z, jnp.take_along_axis(jump, from_z, axis=1), 0.0)
                    turn = jnp.where(k == 0, -here, here)
                if here is not None:
                    value = value + across * turn
                    total = here if total is None else total + here
                loose[pl.ds(base + n4 * 4 + 1 + axis, 32, stride=17), :] = value
            loose[pl.ds(base + n4 * 4, 32, stride=17), :] = by_bulk * div + up * total
        for row in range(32):
            at = (part * 32 + row) * 16
            made[at : at + 16, :] = loose[base + row * 17 : base + row * 17 + 16, :]
        window = pl.ds(part * 512, 512)
        copies.append(pltpu.make_async_copy(made.at[window], out_ref.at[window], sem.at[part]))
        copies[-1].start()
    for copy in copies:
        copy.wait()


def vm():
    return pl.BlockSpec(memory_space=VMEM)


def sm():
    return pl.BlockSpec(memory_space=SMEM)


def shaped(shape, dtype=F32):
    return VMEM(shape, dtype)


def plain(shape, dtype=F32):
    return jax.ShapeDtypeStruct(shape, dtype)


def near(value):
    return pltpu.with_memory_space_constraint(value, VMEM)


def away(value):
    return pltpu.with_memory_space_constraint(value, HBM)


GRANT = pltpu.CompilerParams(vmem_limit_bytes=24 * 1024 * 1024)


def exchange(flat, rows):
    blocks = flat.reshape(DEVS, rows, 1, LANES)
    return lax.all_to_all(blocks, AXES, split_axis=0, concat_axis=0, tiled=True).reshape(flat.shape)


def body(old_state, dest_row, neighbours, orientation, wall_flags, bulk_modulus, density):
    me = (lax.axis_index("grp") * lax.axis_size("dev") + lax.axis_index("dev")).astype(I32).reshape(1)
    dest = dest_row.reshape(2, LANES)
    bulk = away(bulk_modulus.reshape(1, LANES))
    dens = away(density.reshape(1, LANES))
    nbr, wall, orient = away(neighbours), away(wall_flags), away(orientation)
    state = old_state.reshape(256, 4, 4, LANES).transpose(0, 2, 1, 3).reshape(4096, LANES)

    info, pos = pl.pallas_call(
        order_kernel,
        in_specs=[sm()] + [vm()] * 3,
        out_specs=[vm()] * 2,
        out_shape=[shaped((384, LANES), I32), plain((2, LANES), I32)],
        scratch_shapes=[pltpu.VMEM((8, LANES), F32)],
        name="order",
        compiler_params=GRANT,
    )(me, away(dest), nbr, wall)
    heard = exchange(info, 3)
    pieces = pl.pallas_call(
        pack_kernel,
        in_specs=[sm(), sm()] + [vm()] * 3,
        out_specs=vm(),
        out_shape=HBM((4224, LANES), F32),
        scratch_shapes=[pltpu.VMEM((4096, LANES), F32)],
        name="pack",
        compiler_params=GRANT,
    )(pos, dest, away(state), bulk, dens)
    spread = exchange(pieces, 33)
    spots, owners, blocks, rows, labels, cols, far, close, pick = pl.pallas_call(
        table_kernel,
        in_specs=[sm()] + [vm()] * 6,
        out_specs=[vm()] * 9,
        out_shape=[
            shaped((24, LANES), I32),
            shaped((8, LANES), I32),
            shaped((LANES, LANES)),
            shaped((8, LANES), I32),
            shaped((LANES, LANES), I32),
            shaped((LANES, LANES)),
            shaped((384, LANES), I32),
            shaped((384, LANES), I32),
            shaped((LANES, LANES)),
        ],
        scratch_shapes=[pltpu.VMEM((LANES, LANES), I32), pltpu.VMEM((8, LANES), F32)],
        name="table",
        compiler_params=GRANT,
    )(me, near(heard), nbr, wall, orient, bulk, dens)
    owners = owners.reshape(1024)
    passed, zeds = pl.pallas_call(
        forward_kernel,
        in_specs=[sm()] * 2 + [vm()] * 3,
        out_specs=[pl.BlockSpec(memory_space=pl.ANY), vm()],
        out_shape=[HBM((2432, LANES), F32), shaped((LANES, LANES))],
        scratch_shapes=[
            pltpu.VMEM((2048, LANES), F32),
            pltpu.VMEM((2432, LANES), F32),
            pltpu.SemaphoreType.DMA((4,)),
        ],
        name="forward",
        compiler_params=GRANT,
    )(me, spots.reshape(3072), near(spread), near(labels), near(blocks))
    arrived = exchange(passed, 19)
    misc, hot, place, pick = pl.pallas_call(
        across_kernel,
        in_specs=[sm()] * 2 + [vm()] * 6,
        out_specs=[vm()] * 4,
        out_shape=[
            shaped((LANES, LANES)),
            shaped((384, 2 * LANES), BF16),
            shaped((LANES, LANES), BF16),
            shaped((768, LANES), BF16),
        ],
        name="across",
        compiler_params=GRANT,
    )(me, owners, near(zeds), nbr, wall, near(rows), near(cols), near(pick))
    result = pl.pallas_call(
        final_kernel,
        in_specs=[vm()] * 10,
        out_specs=pl.BlockSpec(memory_space=pl.ANY),
        out_shape=plain((2048, LANES)),
        scratch_shapes=[
            pltpu.VMEM((2048, LANES), F32),
            pltpu.VMEM((LANES, LANES), F32),
            pltpu.VMEM((384, LANES), F32),
            pltpu.VMEM((2176, LANES), F32),
            pltpu.VMEM((2048, LANES), F32),
            pltpu.SemaphoreType.DMA((4,)),
        ],
        name="final",
        compiler_params=GRANT,
    )(
        near(arrived), near(place), near(misc), near(hot), near(pick), near(far), near(close),
        jnp.asarray(SIDE3), jnp.asarray(STACKED3), jnp.asarray(COEF),
    )
    return result.reshape(128, 4, 4, LANES).transpose(0, 2, 1, 3).reshape(128, 4, 512)


def solution(mesh):
    both = P(AXES)
    faces = P(None, AXES)
    in_specs = (P(AXES, None, None), both, faces, faces, faces, both, both)
    return jax.shard_map(
        body, mesh=mesh, in_specs=in_specs, out_specs=P(AXES, None, None), check_vma=False
    )
```

```python
import jax
import jax.numpy as jnp
import numpy as np
from jax import lax
from jax.experimental import pallas as pl
from jax.experimental.pallas import tpu as pltpu
from jax.sharding import PartitionSpec as P

NP = 8
DEVS = 128
LANES = 128
AXES = ("grp", "dev")
metric_scale = 0.25
F32 = jnp.float32
I32 = jnp.int32
BF16 = jnp.bfloat16
VMEM = pltpu.MemorySpace.VMEM
SMEM = pltpu.MemorySpace.SMEM
HBM = pltpu.MemorySpace.HBM


def gll_tables(poly_order):
    num_points = poly_order + 1
    points = -np.cos(np.pi * np.arange(num_points) / poly_order)
    legendre = np.zeros((num_points, num_points))
    for sweeps in range(101):
        legendre[:, 0] = 1.0
        legendre[:, 1] = points
        for degree in range(2, num_points):
            legendre[:, degree] = (
                (2 * degree - 1) * points * legendre[:, degree - 1]
                - (degree - 1) * legendre[:, degree - 2]
            ) / degree
        if sweeps < 100:
            points = points - (points * legendre[:, poly_order] - legendre[:, poly_order - 1]) / (
                num_points * legendre[:, poly_order]
            )
    end_values = legendre[:, poly_order]
    weights = 2.0 / (poly_order * num_points * end_values**2)
    distance = points[:, None] - points[None, :] + np.eye(num_points)
    derivative = end_values[:, None] / end_values[None, :] / distance
    derivative = derivative * (1.0 - np.eye(num_points))
    derivative[0, 0] = -poly_order * num_points / 4.0
    derivative[poly_order, poly_order] = poly_order * num_points / 4.0
    return (points, weights, derivative)


POINTS, WEIGHTS, DERIV = gll_tables(NP - 1)
DERIV = DERIV.astype(np.float32)
LIFT = metric_scale / float(WEIGHTS[0])


def derivative_tables():
    eye2, eye8 = np.eye(2, dtype=np.float32), np.eye(8, dtype=np.float32)
    along_y = np.kron(eye2, np.kron(DERIV.T, eye8))
    along_z = np.kron(eye2, np.kron(eye8, DERIV.T))
    side = np.concatenate([along_y, along_z], axis=1)
    stacked = np.concatenate([along_y, along_z], axis=0)
    coef = np.zeros((4, 4, 2, LANES), np.float32)
    for out_chunk in range(4):
        for in_chunk in range(4):
            for half in range(2):
                lanes = slice(64 * half, 64 * half + 64)
                coef[out_chunk, in_chunk, 0, lanes] = DERIV[2 * out_chunk + half, 2 * in_chunk + half]
                coef[out_chunk, in_chunk, 1, lanes] = DERIV[
                    2 * out_chunk + half, 2 * in_chunk + 1 - half
                ]
    return side, stacked, coef.reshape(32, LANES)


SIDE, STACKED, COEF = derivative_tables()


def three_parts(table):
    high = table.astype(jnp.bfloat16)
    low = (table - high.astype(np.float32)).astype(jnp.bfloat16)
    return np.concatenate([high, high, low], axis=0)


SIDE3, STACKED3 = three_parts(SIDE), three_parts(STACKED)


def iota(shape, axis):
    return lax.broadcasted_iota(I32, shape, axis)


def small_dot(left, right):
    return jnp.dot(left.astype(BF16), right.astype(BF16), preferred_element_type=F32)


def split3(value):
    high = value.astype(BF16)
    rest = value - high.astype(F32)
    middle = rest.astype(BF16)
    low = (rest - middle.astype(F32)).astype(BF16)
    return high, middle, low


def pick_dot(pick, value):
    pick = pick.astype(BF16)
    high, middle, low = split3(value)
    total = jnp.dot(pick, high, preferred_element_type=F32)
    total = total + jnp.dot(pick, middle, preferred_element_type=F32)
    return total + jnp.dot(pick, low, preferred_element_type=F32)


def column(row, diag):
    wide = jnp.broadcast_to(row, (LANES, LANES))
    return jnp.sum(jnp.where(diag, wide, 0.0), axis=1, keepdims=True)


def half_sign(shape):
    return jnp.where(iota(shape, 1) < 64, -1.0, 1.0)


def face_pair(chunk, axis, zed):
    lane = iota((LANES, LANES), 1)
    half, face_i, face_b = lane >> 6, (lane >> 3) & 7, lane & 7
    from_y = (face_i & 1) * 64 + half * 56 + face_b
    from_z = (face_i & 1) * 64 + face_b * 8 + half * 7
    values = []
    for field in (0, 1 + axis):
        if axis == 0:
            value = jnp.where(lane < 64, chunk(field, 0), chunk(field, 3))
        else:
            index = from_y if axis == 1 else from_z
            value = jnp.take_along_axis(chunk(field, 0), index, axis=1)
            for n4 in range(1, 4):
                other = jnp.take_along_axis(chunk(field, n4), index, axis=1)
                value = jnp.where(face_i >> 1 == n4, other, value)
        values.append(value)
    normal = half_sign((LANES, LANES)) * values[1]
    return values[0], normal, values[0] + zed * normal


def cross(arrays, bit1, bit0):
    first = [jnp.where(bit0, arrays[t ^ 1], arrays[t]) for t in range(4)]
    return [jnp.where(bit1, first[t ^ 2], first[t]) for t in range(4)]


def lane_bit(lane, bit):
    return ((lane >> bit) & 1) == 1


def regroup(arrays, back):
    lane = iota(arrays[0].shape, 1)
    own = (lane >> 3) & 3
    plain = (lane_bit(lane, 1), lane_bit(lane, 0))
    mixed = (lane_bit(lane ^ (lane >> 3), 1), lane_bit(lane ^ (lane >> 3), 0))
    enter, leave = (plain, mixed) if back else (mixed, plain)
    result = [None] * 16
    for top in range(4):
        four = cross(arrays[4 * top : 4 * top + 4], *enter)
        four = [jnp.take_along_axis(four[t], lane ^ t ^ own, axis=1) for t in range(4)]
        result[4 * top : 4 * top + 4] = cross(four, *leave)
    j2, k2 = lane_bit(lane, 5), lane_bit(lane, 2)
    final = [None] * 16
    for t in range(4):
        final[t::4] = cross(result[t::4], j2, k2)
    return final


def order_kernel(me_ref, dest_ref, nbr_ref, wall_ref, info_ref, pos_ref, scr):
    dest = dest_ref[...]
    sub = iota((LANES, LANES), 0)
    lane = iota((LANES, LANES), 1)
    diag = sub == lane
    key_row, key_col, dest_col = [], [], []
    for half in range(2):
        row = jnp.broadcast_to(dest[half : half + 1, :], (LANES, LANES))
        key = (row >> 7).astype(F32) * 256.0 + (lane + 128 * half).astype(F32)
        key_row.append(key)
        key_col.append(jnp.sum(jnp.where(diag, key, 0.0), axis=1, keepdims=True))
        dest_col.append(jnp.sum(jnp.where(diag, row.astype(F32), 0.0), axis=1, keepdims=True))
    lists = [jnp.zeros((1, LANES), F32), jnp.zeros((1, LANES), F32)]
    for half in range(2):
        before_col = jnp.zeros((LANES, 1), F32)
        before_row = jnp.zeros((1, LANES), F32)
        for other in range(2):
            before_col = before_col + jnp.sum(
                jnp.where(key_row[other] < key_col[half], 1.0, 0.0), axis=1, keepdims=True
            )
            before_row = before_row + jnp.sum(
                jnp.where(key_col[other] < key_row[half], 1.0, 0.0), axis=0, keepdims=True
            )
        pos_ref[half : half + 1, :] = before_row.astype(I32)
        place = before_col.astype(I32)
        k = place & 7
        spot = (k & 3) * 32 + (place >> 3)
        for part in range(2):
            hit = (spot == lane) & (k >> 2 == part)
            lists[part] = lists[part] + jnp.sum(jnp.where(hit, dest_col[half], 0.0), axis=0, keepdims=True)
    scr[...] = jnp.full((8, LANES), -1.0, F32)
    owner = nbr_ref[...] >> 7
    remote = (owner != me_ref[0]) & (wall_ref[...] == 0)
    scr[0:6, :] = jnp.where(remote, owner, -1).astype(F32)
    owners = jnp.max(scr[...], axis=1, keepdims=True)
    spread = iota((8, LANES), 0) == iota((8, LANES), 1)
    owner_row = jnp.sum(jnp.where(spread, owners, 0.0), axis=0, keepdims=True)
    for part, row in enumerate((lists[0], lists[1], owner_row)):
        info_ref[pl.ds(part, LANES, stride=3), :] = jnp.broadcast_to(row, (LANES, LANES)).astype(I32)


def pack_kernel(pos_ref, dest_ref, state_ref, bulk_ref, dens_ref, out_ref, scr):
    zed = jnp.sqrt(bulk_ref[...] * dens_ref[...])
    out_ref[pl.ds(32, LANES, stride=33), :] = jnp.broadcast_to(zed, (LANES, LANES))

    @pl.when(dest_ref[0, 0] >= 0)
    def _():
        def one(slot, carry):
            place = pos_ref[slot >> 7, slot & 127]
            start = (place & 7) * 512 + (place >> 3)
            scr[pl.ds(start, 16, stride=32), :] = state_ref[pl.ds(pl.multiple_of(slot * 16, 16), 16), :]
            return carry

        lax.fori_loop(0, 256, one, 0, unroll=8)
        for k in range(8):
            for block in range(4):
                at = [(k * 16 + c) * 32 + block * 8 for c in range(16)]
                groups = regroup([scr[a : a + 8, :] for a in at], False)
                for g in range(16):
                    row = (k * 16 + g) * 33 + block * 8
                    out_ref[row : row + 8, :] = groups[g]


def table_kernel(
    me_ref, info_ref, nbr_ref, wall_ref, orient_ref, bulk_ref, dens_ref,
    spot_ref, owner_ref, column_ref, row_ref, label_ref, cols_ref, index_ref, hot_ref, wide, scr,
):
    shape = (LANES, LANES)
    sub = iota(shape, 0)
    lane = iota(shape, 1)
    diag = sub == lane
    me = me_ref[0]
    bulk = column(bulk_ref[...], diag)
    dens = column(dens_ref[...], diag)
    zed = column(jnp.sqrt(bulk_ref[...] * dens_ref[...]), diag)
    cols_ref[...] = jnp.where(lane == 0, zed, jnp.where(lane == 1, bulk, dens))

    lists = [info_ref[pl.ds(0, LANES, stride=3), :], info_ref[pl.ds(1, LANES, stride=3), :]]
    owners = info_ref[pl.ds(2, LANES, stride=3), :].astype(F32)
    owner_ref[...] = owners.T[0:8, :].astype(I32)
    column_ref[...] = owners
    target = lists[0] >> 7
    my_k = me >> 4
    mine = jnp.where(my_k >= 4, lists[1], lists[0])
    mine = jnp.take_along_axis(mine, (my_k & 3) * 32 + (lane & 31), axis=1) & 127
    present = jnp.zeros(shape, F32)
    label = jnp.zeros(shape, F32)
    mine = mine.astype(F32)
    for j in range(32):
        hit = target[:, j : j + 1] == lane
        present = jnp.where(hit, 1.0, present)
        label = jnp.where(hit, mine[:, j : j + 1], label)
    below = jnp.where(lane < sub, 1.0, 0.0)
    rank = small_dot(below, present)
    safe = jnp.clip(target, 0, LANES - 1)
    slot = safe * 17 + jnp.take_along_axis(rank.astype(I32), safe, axis=1)
    is_source = jnp.broadcast_to(jnp.where(target[:, 0:1] >= 0, 1.0, 0.0), shape)
    source_rank = jnp.where(is_source > 0.0, small_dot(below, is_source), -1.0)
    chosen = jnp.where(source_rank.T == sub.astype(F32), 1.0, 0.0)
    wide[...] = pick_dot(chosen, jnp.where(lane == 32, sub, slot).astype(F32)).astype(I32)
    quarter = iota((16, LANES), 1) >> 5
    spots = wide[pl.ds(0, 16, stride=4), :]
    for part in range(1, 4):
        moved = pltpu.roll(wide[pl.ds(part, 16, stride=4), :], 32 * part, 1)
        spots = jnp.where(quarter == part, moved, spots)
    spot_ref[0:16, :] = spots
    sources = jnp.where(diag, jnp.broadcast_to(wide[:, 32:33], shape).astype(F32), 0.0)
    sources = jnp.sum(sources, axis=0, keepdims=True).astype(I32)
    spot_ref[16:24, :] = jnp.broadcast_to(sources, (8, LANES))
    order = jnp.where(present > 0.0, rank, -1.0)
    labels = jnp.zeros(shape, F32)
    for i in range(16):
        row = jnp.sum(jnp.where(order == float(i), label, 0.0), axis=0, keepdims=True)
        labels = jnp.where(sub == i, row, labels)
    label_ref[...] = labels.T.astype(I32)

    gather = [jnp.where((sub >> 5) + 4 * part == lane >> 4, 1.0, 0.0) for part in range(2)]

    def rows_of(block):
        value = jnp.zeros(shape, F32)
        for part in range(2):
            held = jnp.where(lists[part] >> 7 == block, (lists[part] & 127).astype(F32), 0.0)
            value = value + small_dot(held, gather[part])
        source = jnp.sum(jnp.where(lane == block, order, 0.0), axis=1, keepdims=True)
        chosen = source == (lane & 15).astype(F32)
        return jnp.sum(jnp.where(chosen, value, 0.0), axis=0, keepdims=True)

    row_ref[...] = jnp.broadcast_to(rows_of(me), (8, LANES)).astype(I32)
    scr[...] = jnp.full((8, LANES), -1.0, F32)
    nbr_all = nbr_ref[...]
    away_all = ((nbr_all >> 7) != me) & (wall_ref[...] == 0)
    scr[0:6, :] = jnp.where(away_all, nbr_all >> 7, -1).astype(F32)
    neighbour = jnp.max(scr[...], axis=1, keepdims=True).astype(I32)
    low_half = lane < 64
    for axis in range(3):
        rows = slice(axis * LANES, axis * LANES + LANES)
        codes, aways = [], []
        for side in range(2):
            face = 2 * axis + side
            nbr = nbr_ref[face : face + 1, :]
            is_wall = wall_ref[face : face + 1, :] == 1
            remote = ((nbr >> 7) != me) & jnp.logical_not(is_wall)
            wanted = column(jnp.where(remote, nbr & 127, -1).astype(F32), diag)
            hit = rows_of(neighbour[face : face + 1, :]) == wanted
            hot_ref[rows, side * LANES : (side + 1) * LANES] = jnp.where(hit, 1.0, 0.0).astype(BF16)
            codes.append(column(orient_ref[face : face + 1, :].astype(F32), diag).astype(I32))
            aways.append(wanted)
        code = jnp.where(low_half, codes[0], codes[1])
        a, b = (lane >> 3) & 7, lane & 7
        swap = code >= 4
        a1, b1 = jnp.where(swap, b, a), jnp.where(swap, a, b)
        a2 = jnp.where((code & 1) == 1, 7 - a1, a1)
        b2 = jnp.where((code & 2) == 2, 7 - b1, b1)
        h = jnp.where(low_half, 1, 0)
        if axis == 0:
            top = ((a2 >> 2) ^ h) * 8 + ((b2 >> 2) ^ h) * 4
            group, v = top + ((a2 ^ b2) & 3), a2 & 3
        elif axis == 1:
            top = ((a2 >> 2) ^ h) * 8 + (((a2 >> 1) & 1) ^ (b2 >> 2)) * 4
            group, v = top + ((b2 & 3) ^ (h * 3)), (a2 & 1) * 2 + (b2 >> 2)
        else:
            top = ((a2 >> 2) ^ (b2 >> 2)) * 8 + (((a2 >> 1) & 1) ^ h) * 4
            group, v = top + ((b2 & 3) ^ (h * 3)), (a2 & 1) * 2 + (b2 >> 2)
        is_far = jnp.where(low_half, aways[0], aways[1]) >= 0.0
        index_ref[rows, :] = h * 64 + jnp.where(is_far, v * 16 + group, a2 * 8 + b2)


SHIFT_A, SHIFT_B = (3, 9)


def shift_of(i):
    return (i & 3) ^ ((i >> 2) & 1) * (4 * SHIFT_A) ^ (i >> 3) * (4 * SHIFT_B)


def forward_kernel(me_ref, spot_ref, in_ref, label_ref, column_ref, out_ref, zed_ref, held, made, sem):
    for number in range(DEVS // 2):
        start = spot_ref[2048 + number] * 33
        for j in range(32):
            held[pl.ds(spot_ref[number * 32 + j], 1), :] = in_ref[pl.ds(start + j, 1), :]
    shape = (LANES, LANES)
    lane = iota(shape, 1)
    zeds = in_ref[pl.ds(32, LANES, stride=33), :]
    zed_ref[...] = zeds
    zed = jnp.take_along_axis(zeds, label_ref[...], axis=1)
    me = me_ref[0]
    g3, g2, g1, g0 = (me >> 3) & 1, (me >> 2) & 1, (me >> 1) & 1, me & 1
    lane = iota((8, LANES), 1)
    h, v1, v0 = lane >> 6, (lane >> 1) & 1, lane & 1
    nodes = [
        h * 16 + (g3 ^ h) * 8 + v1 * 4 + v0 * 2 + (g2 ^ h),
        v1 * 16 + h * 14 + v0,
        v1 * 16 + v0 * 8 + (g1 ^ h) * 4 + (g0 ^ h) * 2 + h,
    ]
    here = (lane >> 2) & 15
    shift = (here & 3) ^ ((here >> 2) & 1) * (4 * SHIFT_A) ^ (here >> 3) * (4 * SHIFT_B)
    which = []
    for axis in range(3):
        for field in (0, 1 + axis):
            value = jnp.full((8, LANES), -1, I32)
            for i in range(16):
                spot = lane ^ shift_of(i)
                n = spot >> 2
                i0, j2, j1, j0, k2 = (n >> 4) & 1, (n >> 3) & 1, (n >> 2) & 1, (n >> 1) & 1, n & 1
                if axis == 0:
                    hit = (j2 == g3 ^ i0) & (k2 == g2 ^ i0)
                elif axis == 1:
                    hit = (j2 == j1) & (j1 == j0)
                else:
                    hit = (j1 == g1 ^ k2) & (j0 == g0 ^ k2)
                value = jnp.where(hit & (spot & 3 == field), i, value)
            which.append(value)
    sign = half_sign((8, LANES))
    waves = [[], [], []]
    for quad in range(4):
        blocks = range(quad * 4, quad * 4 + 4)
        merged = [[jnp.zeros((8, LANES), F32)] * 6 for _ in blocks]
        for i in range(16):
            hits = [which[m] == i for m in range(6)]
            for b, block in enumerate(blocks):
                rows = held[pl.ds(block * 136 + i, 8, stride=17), :]
                rows = jnp.take_along_axis(rows, lane ^ shift_of(i), axis=1)
                merged[b] = [jnp.where(hits[m], rows, merged[b][m]) for m in range(6)]
        wide = [
            jnp.take_along_axis(zed[block * 8 : block * 8 + 8, :], here, axis=1) * sign for block in blocks
        ]
        for axis in range(3):
            at = (nodes[axis] * 4) ^ shift
            press = [jnp.take_along_axis(merged[b][2 * axis], at, axis=1) for b in range(4)]
            at = (nodes[axis] * 4 + 1 + axis) ^ shift
            speed = [jnp.take_along_axis(merged[b][2 * axis + 1], at, axis=1) for b in range(4)]
            waves[axis] += [press[b] + wide[b] * speed[b] for b in range(4)]
    low_half = iota(shape, 1) < 64
    lane = iota(shape, 1).astype(F32)
    halos = []
    for axis in range(3):
        wave = jnp.concatenate(waves[axis], axis=0)
        upper = column_ref[:, 2 * axis + 1 : 2 * axis + 2] == lane
        lower = column_ref[:, 2 * axis : 2 * axis + 1] == lane
        pick = jnp.concatenate([jnp.where(upper, 1.0, 0.0), jnp.where(lower, 1.0, 0.0)], axis=1)
        table = jnp.concatenate([jnp.where(low_half, wave, 0.0), jnp.where(low_half, 0.0, wave)], axis=0)
        halos.append(pick_dot(pick, table))
    copies = []
    for part in range(4):
        base = part * 32
        for target in range(base, base + 32):
            made[target * 19 : target * 19 + 16, :] = held[target * 17 : target * 17 + 16, :]
        for axis in range(3):
            made[pl.ds(base * 19 + 16 + axis, 32, stride=19), :] = halos[axis][base : base + 32, :]
        rows = pl.ds(base * 19, 608)
        copies.append(pltpu.make_async_copy(made.at[rows], out_ref.at[rows], sem.at[part]))
        copies[-1].start()
    for copy in copies:
        copy.wait()


def across_kernel(me_ref, owner_ref, zed_ref, nbr_ref, wall_ref, row_ref, out_ref, near_ref, place_ref):
    shape = (LANES, LANES)
    lane = iota(shape, 1)
    diag = iota(shape, 0) == lane
    me = me_ref[0]
    own = zed_ref[pl.ds(me, 1), :]
    for axis in range(3):
        rows = slice(axis * LANES, axis * LANES + LANES)
        zeds = []
        for side in range(2):
            face = 2 * axis + side
            other = zed_ref[pl.ds(jnp.maximum(owner_ref[face * LANES + me], 0), 1), :]
            nbr = nbr_ref[face : face + 1, :]
            is_wall = wall_ref[face : face + 1, :] == 1
            remote = ((nbr >> 7) != me) & jnp.logical_not(is_wall)
            far = column(jnp.where(remote, 1.0, 0.0), diag) > 0.0
            spot = column((nbr & 127).astype(F32), diag) == lane.astype(F32)
            wall = column(jnp.where(is_wall, 1.0, 0.0), diag) > 0.0
            value = jnp.where(spot, jnp.where(far, other, own), 0.0)
            zeds.append(jnp.where(wall, -1.0, jnp.sum(value, axis=1, keepdims=True)))
            local = jnp.where(far | wall, 0.0, jnp.where(spot, 1.0, 0.0))
            near_ref[rows, side * LANES : (side + 1) * LANES] = local.astype(BF16)
        out_ref[rows, :] = jnp.where(lane < 64, zeds[0], zeds[1])
    place_ref[...] = jnp.where(row_ref[0:1, :] == iota(shape, 0), 1.0, 0.0).astype(BF16)


def exchange_lanes(arrays):
    lane = iota(arrays[0].shape, 1)
    bits = (lane_bit(lane, 6), lane_bit(lane, 5), lane_bit(lane, 4))

    def mix(eight):
        for step, bit in zip((1, 2, 4), bits[::-1]):
            eight = [jnp.where(bit, eight[t ^ step], eight[t]) for t in range(8)]
        return eight

    turned = mix(arrays)
    turned = [jnp.take_along_axis(turned[t], lane ^ (t * 16), axis=1) for t in range(8)]
    return mix(turned)


def final_kernel(
    in_ref, place_ref, cols_ref, zed_ref, near_ref, far_ref, index_ref, side_ref, stack_ref, coef_ref,
    out_ref, state, turned, lift, loose, made, sem,
):
    shape = (LANES, LANES)
    lane = iota(shape, 1)
    low_half = lane < 64
    place = place_ref[...]
    place = jnp.concatenate([place, place, place], axis=1)
    for group in range(0, 16, 2):
        pair = []
        for g in (group, group + 1):
            rows = [in_ref[(k * 16 + g) * 19 : (k * 16 + g) * 19 + 16, :] for k in range(8)]
            pair.append(jnp.concatenate(rows, axis=0))
        parts = split3(jnp.concatenate(pair, axis=1))
        moved = jnp.dot(place, jnp.concatenate(parts, axis=0), preferred_element_type=F32)
        state[group * LANES : (group + 1) * LANES, :] = moved[:, 0:LANES]
        state[(group + 1) * LANES : (group + 2) * LANES, :] = moved[:, LANES:]
    for block in range(16):
        at = [c * LANES + block * 8 for c in range(16)]
        chunks = regroup([state[a : a + 8, :] for a in at], True)
        for c in range(16):
            state[at[c] : at[c] + 8, :] = chunks[c]

    def chunk(field, n4):
        start = (n4 * 4 + field) * LANES
        return state[start : start + LANES, :]

    zed = cols_ref[:, 0:1]
    for axis in range(3):
        rows = slice(axis * LANES, axis * LANES + LANES)
        press, norm, wave = face_pair(chunk, axis, zed)
        turned[...] = in_ref[pl.ds(16 + axis, LANES, stride=19), :].T
        parts = [turned[pl.ds(h * 64 + v, 16, stride=4), :] for h in range(2) for v in range(4)]
        far = jnp.concatenate(exchange_lanes(parts), axis=0)
        masked = []
        for value in (wave, far):
            masked.append(jnp.where(low_half, 0.0, value))
            masked.append(jnp.where(low_half, value, 0.0))
        hot = [near_ref[rows, :], far_ref[rows, :]]
        both = jnp.dot(
            jnp.concatenate(hot * 3, axis=1),
            jnp.concatenate(split3(jnp.concatenate(masked, axis=0)), axis=0),
            preferred_element_type=F32,
        )
        wave_out = jnp.take_along_axis(both, index_ref[rows, :], axis=1)
        zed_out = zed_ref[rows, :]
        jump = (wave_out - press + zed_out * norm) / (zed + zed_out)
        lift[rows, :] = jnp.where(zed_out < 0.0, norm, jump)

    lane = iota((32, LANES), 1)
    low_half = lane < 64
    i2, j, k = lane >> 6, (lane >> 3) & 7, lane & 7
    on_y, on_z = (j == 0) | (j == 7), (k == 0) | (k == 7)
    copies = []
    for part in range(4):
        rows = slice(part * 32, part * 32 + 32)
        zed, bulk, dens = cols_ref[rows, 0:1], cols_ref[rows, 1:2], cols_ref[rows, 2:3]
        by_bulk = -metric_scale * bulk
        by_dens = -(metric_scale / dens)
        up = LIFT * bulk
        across = -LIFT * zed / dens
        piece = {}
        for field in range(4):
            for n4 in range(4):
                start = (n4 * 4 + field) * LANES + part * 32
                piece[field, n4] = state[start : start + 32, :]
        cut = []
        for field in (0, 2, 3):
            whole = jnp.concatenate([piece[field, n4] for n4 in range(4)], axis=0)
            high = whole.astype(BF16)
            cut.append((high, (whole - high.astype(F32)).astype(BF16)))
        grad = jnp.dot(
            jnp.concatenate([cut[0][0], cut[0][1], cut[0][0]], axis=1), side_ref[...], preferred_element_type=F32
        )
        across_div = jnp.dot(
            jnp.concatenate([cut[1][0], cut[2][0], cut[1][1], cut[2][1], cut[1][0], cut[2][0]], axis=1),
            stack_ref[...],
            preferred_element_type=F32,
        )
        swapped = {}
        for field in (0, 1):
            for n4 in range(4):
                swapped[field, n4] = pltpu.roll(piece[field, n4], 64, 1)
        jumps = [lift[axis * LANES + part * 32 : axis * LANES + part * 32 + 32, :] for axis in range(3)]
        base = part * 544
        for n4 in range(4):
            along = {}
            for field in (0, 1):
                total = None
                for m4 in range(4):
                    at = (n4 * 4 + m4) * 2
                    term = piece[field, m4] * coef_ref[at : at + 1, :]
                    term = term + swapped[field, m4] * coef_ref[at + 1 : at + 2, :]
                    total = term if total is None else total + term
                along[field] = total
            block = slice(n4 * 32, n4 * 32 + 32)
            div = along[1] + across_div[block, :]
            grads = [along[0], grad[block, 0:LANES], grad[block, LANES:]]
            face_i = 2 * n4 + i2
            from_y = jnp.where(j == 7, 64, 0) + face_i * 8 + k
            from_z = jnp.where(k == 7, 64, 0) + face_i * 8 + j
            total = None
            for axis in range(3):
                jump = jumps[axis]
                value = by_dens * grads[axis]
                here = None
                if axis == 0 and n4 == 0:
                    here = jnp.where(low_half, jump, 0.0)
                    turn = -here
                elif axis == 0 and n4 == 3:
                    here = jnp.where(low_half, 0.0, jump)
                    turn = here
                elif axis == 1:
                    here = jnp.where(on_y, jnp.take_along_axis(jump, from_y, axis=1), 0.0)
                    turn = jnp.where(j == 0, -here, here)
                elif axis == 2:
                    here = jnp.where(on_z, jnp.take_along_axis(jump, from_z, axis=1), 0.0)
                    turn = jnp.where(k == 0, -here, here)
                if here is not None:
                    value = value + across * turn
                    total = here if total is None else total + here
                loose[pl.ds(base + n4 * 4 + 1 + axis, 32, stride=17), :] = value
            loose[pl.ds(base + n4 * 4, 32, stride=17), :] = by_bulk * div + up * total
        for row in range(32):
            at = (part * 32 + row) * 16
            made[at : at + 16, :] = loose[base + row * 17 : base + row * 17 + 16, :]
        window = pl.ds(part * 512, 512)
        copies.append(pltpu.make_async_copy(made.at[window], out_ref.at[window], sem.at[part]))
        copies[-1].start()
    for copy in copies:
        copy.wait()


def vm():
    return pl.BlockSpec(memory_space=VMEM)


def sm():
    return pl.BlockSpec(memory_space=SMEM)


def shaped(shape, dtype=F32):
    return VMEM(shape, dtype)


def plain(shape, dtype=F32):
    return jax.ShapeDtypeStruct(shape, dtype)


def near(value):
    return pltpu.with_memory_space_constraint(value, VMEM)


def away(value):
    return pltpu.with_memory_space_constraint(value, HBM)


GRANT = pltpu.CompilerParams(vmem_limit_bytes=24 * 1024 * 1024)


def exchange(flat, rows):
    blocks = flat.reshape(DEVS, rows, 1, LANES)
    return lax.all_to_all(blocks, AXES, split_axis=0, concat_axis=0, tiled=True).reshape(flat.shape)


def body(old_state, dest_row, neighbours, orientation, wall_flags, bulk_modulus, density):
    me = (lax.axis_index("grp") * lax.axis_size("dev") + lax.axis_index("dev")).astype(I32).reshape(1)
    dest = dest_row.reshape(2, LANES)
    bulk = away(bulk_modulus.reshape(1, LANES))
    dens = away(density.reshape(1, LANES))
    nbr, wall, orient = away(neighbours), away(wall_flags), away(orientation)
    state = old_state.reshape(256, 4, 4, LANES).transpose(0, 2, 1, 3).reshape(4096, LANES)

    info, pos = pl.pallas_call(
        order_kernel,
        in_specs=[sm()] + [vm()] * 3,
        out_specs=[vm()] * 2,
        out_shape=[shaped((384, LANES), I32), plain((2, LANES), I32)],
        scratch_shapes=[pltpu.VMEM((8, LANES), F32)],
        name="order",
        compiler_params=GRANT,
    )(me, away(dest), nbr, wall)
    heard = exchange(info, 3)
    pieces = pl.pallas_call(
        pack_kernel,
        in_specs=[sm(), sm()] + [vm()] * 3,
        out_specs=vm(),
        out_shape=HBM((4224, LANES), F32),
        scratch_shapes=[pltpu.VMEM((4096, LANES), F32)],
        name="pack",
        compiler_params=GRANT,
    )(pos, dest, away(state), bulk, dens)
    spread = exchange(pieces, 33)
    spots, owners, blocks, rows, labels, cols, index, far = pl.pallas_call(
        table_kernel,
        in_specs=[sm()] + [vm()] * 6,
        out_specs=[vm()] * 8,
        out_shape=[
            shaped((24, LANES), I32),
            shaped((8, LANES), I32),
            shaped((LANES, LANES)),
            shaped((8, LANES), I32),
            shaped((LANES, LANES), I32),
            shaped((LANES, LANES)),
            shaped((384, LANES), I32),
            shaped((384, 2 * LANES), BF16),
        ],
        scratch_shapes=[pltpu.VMEM((LANES, LANES), I32), pltpu.VMEM((8, LANES), F32)],
        name="table",
        compiler_params=GRANT,
    )(me, near(heard), nbr, wall, orient, bulk, dens)
    owners = owners.reshape(1024)
    passed, zeds = pl.pallas_call(
        forward_kernel,
        in_specs=[sm()] * 2 + [vm()] * 3,
        out_specs=[pl.BlockSpec(memory_space=pl.ANY), vm()],
        out_shape=[HBM((2432, LANES), F32), shaped((LANES, LANES))],
        scratch_shapes=[
            pltpu.VMEM((2176, LANES), F32),
            pltpu.VMEM((2432, LANES), F32),
            pltpu.SemaphoreType.DMA((4,)),
        ],
        name="forward",
        compiler_params=GRANT,
    )(me, spots.reshape(3072), near(spread), near(labels), near(blocks))
    arrived = exchange(passed, 19)
    zed_out, close, place = pl.pallas_call(
        across_kernel,
        in_specs=[sm()] * 2 + [vm()] * 4,
        out_specs=[vm()] * 3,
        out_shape=[shaped((384, LANES)), shaped((384, 2 * LANES), BF16), shaped((LANES, LANES), BF16)],
        name="across",
        compiler_params=GRANT,
    )(me, owners, near(zeds), nbr, wall, near(rows))
    result = pl.pallas_call(
        final_kernel,
        in_specs=[vm()] * 10,
        out_specs=pl.BlockSpec(memory_space=pl.ANY),
        out_shape=plain((2048, LANES)),
        scratch_shapes=[
            pltpu.VMEM((2048, LANES), F32),
            pltpu.VMEM((LANES, LANES), F32),
            pltpu.VMEM((384, LANES), F32),
            pltpu.VMEM((2176, LANES), F32),
            pltpu.VMEM((2048, LANES), F32),
            pltpu.SemaphoreType.DMA((4,)),
        ],
        name="final",
        compiler_params=GRANT,
    )(
        near(arrived), near(place), near(cols), near(zed_out), near(close), near(far), near(index),
        jnp.asarray(SIDE3), jnp.asarray(STACKED3), jnp.asarray(COEF),
    )
    return result.reshape(128, 4, 4, LANES).transpose(0, 2, 1, 3).reshape(128, 4, 512)


def solution(mesh):
    both = P(AXES)
    faces = P(None, AXES)
    in_specs = (P(AXES, None, None), both, faces, faces, faces, both, both)
    return jax.shard_map(
        body, mesh=mesh, in_specs=in_specs, out_specs=P(AXES, None, None), check_vma=False
    )
```

```python
import jax
import jax.numpy as jnp
import numpy as np
from jax import lax
from jax.experimental import pallas as pl
from jax.experimental.pallas import tpu as pltpu
from jax.sharding import PartitionSpec as P

NP = 8
DEVS = 128
LANES = 128
AXES = ("grp", "dev")
metric_scale = 0.25
F32 = jnp.float32
I32 = jnp.int32
BF16 = jnp.bfloat16
VMEM = pltpu.MemorySpace.VMEM
SMEM = pltpu.MemorySpace.SMEM
HBM = pltpu.MemorySpace.HBM


def gll_tables(poly_order):
    num_points = poly_order + 1
    points = -np.cos(np.pi * np.arange(num_points) / poly_order)
    legendre = np.zeros((num_points, num_points))
    for sweeps in range(101):
        legendre[:, 0] = 1.0
        legendre[:, 1] = points
        for degree in range(2, num_points):
            legendre[:, degree] = (
                (2 * degree - 1) * points * legendre[:, degree - 1]
                - (degree - 1) * legendre[:, degree - 2]
            ) / degree
        if sweeps < 100:
            points = points - (points * legendre[:, poly_order] - legendre[:, poly_order - 1]) / (
                num_points * legendre[:, poly_order]
            )
    end_values = legendre[:, poly_order]
    weights = 2.0 / (poly_order * num_points * end_values**2)
    distance = points[:, None] - points[None, :] + np.eye(num_points)
    derivative = end_values[:, None] / end_values[None, :] / distance
    derivative = derivative * (1.0 - np.eye(num_points))
    derivative[0, 0] = -poly_order * num_points / 4.0
    derivative[poly_order, poly_order] = poly_order * num_points / 4.0
    return (points, weights, derivative)


POINTS, WEIGHTS, DERIV = gll_tables(NP - 1)
DERIV = DERIV.astype(np.float32)
LIFT = metric_scale / float(WEIGHTS[0])


def derivative_tables():
    eye2, eye8 = np.eye(2, dtype=np.float32), np.eye(8, dtype=np.float32)
    along_y = np.kron(eye2, np.kron(DERIV.T, eye8))
    along_z = np.kron(eye2, np.kron(eye8, DERIV.T))
    side = np.concatenate([along_y, along_z], axis=1)
    stacked = np.concatenate([along_y, along_z], axis=0)
    coef = np.zeros((4, 4, 2, LANES), np.float32)
    for out_chunk in range(4):
        for in_chunk in range(4):
            for half in range(2):
                lanes = slice(64 * half, 64 * half + 64)
                coef[out_chunk, in_chunk, 0, lanes] = DERIV[2 * out_chunk + half, 2 * in_chunk + half]
                coef[out_chunk, in_chunk, 1, lanes] = DERIV[
                    2 * out_chunk + half, 2 * in_chunk + 1 - half
                ]
    return side, stacked, coef.reshape(32, LANES)


SIDE, STACKED, COEF = derivative_tables()


def three_parts(table):
    high = table.astype(jnp.bfloat16)
    low = (table - high.astype(np.float32)).astype(jnp.bfloat16)
    return np.concatenate([high, high, low], axis=0)


SIDE3, STACKED3 = three_parts(SIDE), three_parts(STACKED)


def iota(shape, axis):
    return lax.broadcasted_iota(I32, shape, axis)


def small_dot(left, right):
    return jnp.dot(left.astype(BF16), right.astype(BF16), preferred_element_type=F32)


def split3(value):
    high = value.astype(BF16)
    rest = value - high.astype(F32)
    middle = rest.astype(BF16)
    low = (rest - middle.astype(F32)).astype(BF16)
    return high, middle, low


def pick_dot(pick, value):
    pick = pick.astype(BF16)
    high, middle, low = split3(value)
    total = jnp.dot(pick, high, preferred_element_type=F32)
    total = total + jnp.dot(pick, middle, preferred_element_type=F32)
    return total + jnp.dot(pick, low, preferred_element_type=F32)


def column(row, diag):
    wide = jnp.broadcast_to(row, (LANES, LANES))
    return jnp.sum(jnp.where(diag, wide, 0.0), axis=1, keepdims=True)


def half_sign(shape):
    return jnp.where(iota(shape, 1) < 64, -1.0, 1.0)


def face_pair(chunk, axis, zed):
    lane = iota((LANES, LANES), 1)
    half, face_i, face_b = lane >> 6, (lane >> 3) & 7, lane & 7
    from_y = (face_i & 1) * 64 + half * 56 + face_b
    from_z = (face_i & 1) * 64 + face_b * 8 + half * 7
    values = []
    for field in (0, 1 + axis):
        if axis == 0:
            value = jnp.where(lane < 64, chunk(field, 0), chunk(field, 3))
        else:
            index = from_y if axis == 1 else from_z
            value = jnp.take_along_axis(chunk(field, 0), index, axis=1)
            for n4 in range(1, 4):
                other = jnp.take_along_axis(chunk(field, n4), index, axis=1)
                value = jnp.where(face_i >> 1 == n4, other, value)
        values.append(value)
    normal = half_sign((LANES, LANES)) * values[1]
    return values[0], normal, values[0] + zed * normal


def cross(arrays, bit1, bit0):
    first = [jnp.where(bit0, arrays[t ^ 1], arrays[t]) for t in range(4)]
    return [jnp.where(bit1, first[t ^ 2], first[t]) for t in range(4)]


def lane_bit(lane, bit):
    return ((lane >> bit) & 1) == 1


def regroup(arrays, back):
    lane = iota(arrays[0].shape, 1)
    own = (lane >> 3) & 3
    plain = (lane_bit(lane, 1), lane_bit(lane, 0))
    mixed = (lane_bit(lane ^ (lane >> 3), 1), lane_bit(lane ^ (lane >> 3), 0))
    enter, leave = (plain, mixed) if back else (mixed, plain)
    result = [None] * 16
    for top in range(4):
        four = cross(arrays[4 * top : 4 * top + 4], *enter)
        four = [jnp.take_along_axis(four[t], lane ^ t ^ own, axis=1) for t in range(4)]
        result[4 * top : 4 * top + 4] = cross(four, *leave)
    j2, k2 = lane_bit(lane, 5), lane_bit(lane, 2)
    final = [None] * 16
    for t in range(4):
        final[t::4] = cross(result[t::4], j2, k2)
    return final


def order_kernel(me_ref, dest_ref, nbr_ref, wall_ref, info_ref, pos_ref, scr):
    dest = dest_ref[...]
    sub = iota((LANES, LANES), 0)
    lane = iota((LANES, LANES), 1)
    diag = sub == lane
    key_row, key_col, dest_col = [], [], []
    for half in range(2):
        row = jnp.broadcast_to(dest[half : half + 1, :], (LANES, LANES))
        key = (row >> 7).astype(F32) * 256.0 + (lane + 128 * half).astype(F32)
        key_row.append(key)
        key_col.append(jnp.sum(jnp.where(diag, key, 0.0), axis=1, keepdims=True))
        dest_col.append(jnp.sum(jnp.where(diag, row.astype(F32), 0.0), axis=1, keepdims=True))
    lists = [jnp.zeros((1, LANES), F32), jnp.zeros((1, LANES), F32)]
    for half in range(2):
        before_col = jnp.zeros((LANES, 1), F32)
        before_row = jnp.zeros((1, LANES), F32)
        for other in range(2):
            before_col = before_col + jnp.sum(
                jnp.where(key_row[other] < key_col[half], 1.0, 0.0), axis=1, keepdims=True
            )
            before_row = before_row + jnp.sum(
                jnp.where(key_col[other] < key_row[half], 1.0, 0.0), axis=0, keepdims=True
            )
        pos_ref[half : half + 1, :] = jnp.where(dest[half : half + 1, :] >= 0, before_row.astype(I32), -1)
        place = before_col.astype(I32)
        k = place & 7
        spot = (k & 3) * 32 + (place >> 3)
        for part in range(2):
            hit = (spot == lane) & (k >> 2 == part)
            lists[part] = lists[part] + jnp.sum(jnp.where(hit, dest_col[half], 0.0), axis=0, keepdims=True)
    scr[...] = jnp.full((8, LANES), -1.0, F32)
    owner = nbr_ref[...] >> 7
    remote = (owner != me_ref[0]) & (wall_ref[...] == 0)
    scr[0:6, :] = jnp.where(remote, owner, -1).astype(F32)
    owners = jnp.max(scr[...], axis=1, keepdims=True)
    spread = iota((8, LANES), 0) == iota((8, LANES), 1)
    owner_row = jnp.sum(jnp.where(spread, owners, 0.0), axis=0, keepdims=True)
    for part, row in enumerate((lists[0], lists[1], owner_row)):
        info_ref[pl.ds(part, LANES, stride=3), :] = jnp.broadcast_to(row, (LANES, LANES)).astype(I32)


def pack_kernel(pos_ref, state_ref, bulk_ref, dens_ref, out_ref, rows, made, in_sem, out_sem):
    full = pos_ref[0, 0] >= 0
    loads = []
    for part in range(4):
        window = pl.ds(part * 1024, 1024)
        loads.append(pltpu.make_async_copy(state_ref.at[window], rows.at[window], in_sem.at[part]))

    @pl.when(full)
    def _():
        for load in loads:
            load.start()

    zed = jnp.sqrt(bulk_ref[...] * dens_ref[...])
    made[pl.ds(32, LANES, stride=33), :] = jnp.broadcast_to(zed, (LANES, LANES))

    @pl.when(full)
    def _():
        for part in range(4):
            loads[part].wait()

            def one(step, carry):
                slot = part * 64 + step
                place = pos_ref[slot >> 7, slot & 127]
                start = (place & 7) * 528 + (place >> 3)
                made[pl.ds(start, 16, stride=33), :] = rows[pl.ds(pl.multiple_of(slot * 16, 16), 16), :]
                return carry

            lax.fori_loop(0, 64, one, 0, unroll=8)

    stores = []
    for k in range(8):

        @pl.when(full)
        def _():
            for block in range(4):
                at = [(k * 16 + c) * 33 + block * 8 for c in range(16)]
                groups = regroup([made[a : a + 8, :] for a in at], False)
                for g in range(16):
                    made[at[g] : at[g] + 8, :] = groups[g]

        window = pl.ds(k * 528, 528)
        stores.append(pltpu.make_async_copy(made.at[window], out_ref.at[window], out_sem.at[k]))
        stores[-1].start()
    for store in stores:
        store.wait()


def table_kernel(
    me_ref, info_ref, nbr_ref, wall_ref, orient_ref, bulk_ref, dens_ref,
    spot_ref, owner_ref, column_ref, row_ref, label_ref, cols_ref, index_ref, hot_ref, wide, scr,
):
    shape = (LANES, LANES)
    sub = iota(shape, 0)
    lane = iota(shape, 1)
    diag = sub == lane
    me = me_ref[0]
    bulk = column(bulk_ref[...], diag)
    dens = column(dens_ref[...], diag)
    zed = column(jnp.sqrt(bulk_ref[...] * dens_ref[...]), diag)
    cols_ref[...] = jnp.where(lane == 0, zed, jnp.where(lane == 1, bulk, dens))

    lists = [info_ref[pl.ds(0, LANES, stride=3), :], info_ref[pl.ds(1, LANES, stride=3), :]]
    owners = info_ref[pl.ds(2, LANES, stride=3), :].astype(F32)
    owner_ref[...] = owners.T[0:8, :].astype(I32)
    column_ref[...] = owners
    target = lists[0] >> 7
    my_k = me >> 4
    mine = jnp.where(my_k >= 4, lists[1], lists[0])
    mine = jnp.take_along_axis(mine, (my_k & 3) * 32 + (lane & 31), axis=1) & 127
    present = jnp.zeros(shape, F32)
    label = jnp.zeros(shape, F32)
    mine = mine.astype(F32)
    for j in range(32):
        hit = target[:, j : j + 1] == lane
        present = jnp.where(hit, 1.0, present)
        label = jnp.where(hit, mine[:, j : j + 1], label)
    below = jnp.where(lane < sub, 1.0, 0.0)
    rank = small_dot(below, present)
    safe = jnp.clip(target, 0, LANES - 1)
    slot = safe * 17 + jnp.take_along_axis(rank.astype(I32), safe, axis=1)
    is_source = jnp.broadcast_to(jnp.where(target[:, 0:1] >= 0, 1.0, 0.0), shape)
    source_rank = jnp.where(is_source > 0.0, small_dot(below, is_source), -1.0)
    chosen = jnp.where(source_rank.T == sub.astype(F32), 1.0, 0.0)
    wide[...] = pick_dot(chosen, jnp.where(lane == 32, sub, slot).astype(F32)).astype(I32)
    quarter = iota((16, LANES), 1) >> 5
    spots = wide[pl.ds(0, 16, stride=4), :]
    for part in range(1, 4):
        moved = pltpu.roll(wide[pl.ds(part, 16, stride=4), :], 32 * part, 1)
        spots = jnp.where(quarter == part, moved, spots)
    spot_ref[0:16, :] = spots
    sources = jnp.where(diag, jnp.broadcast_to(wide[:, 32:33], shape).astype(F32), 0.0)
    sources = jnp.sum(sources, axis=0, keepdims=True).astype(I32)
    spot_ref[16:24, :] = jnp.broadcast_to(sources, (8, LANES))
    order = jnp.where(present > 0.0, rank, -1.0)
    labels = jnp.zeros(shape, F32)
    for i in range(16):
        row = jnp.sum(jnp.where(order == float(i), label, 0.0), axis=0, keepdims=True)
        labels = jnp.where(sub == i, row, labels)
    label_ref[...] = labels.T.astype(I32)

    gather = [jnp.where((sub >> 5) + 4 * part == lane >> 4, 1.0, 0.0) for part in range(2)]

    def rows_of(block):
        value = jnp.zeros(shape, F32)
        for part in range(2):
            held = jnp.where(lists[part] >> 7 == block, (lists[part] & 127).astype(F32), 0.0)
            value = value + small_dot(held, gather[part])
        source = jnp.sum(jnp.where(lane == block, order, 0.0), axis=1, keepdims=True)
        chosen = source == (lane & 15).astype(F32)
        return jnp.sum(jnp.where(chosen, value, 0.0), axis=0, keepdims=True)

    row_ref[...] = jnp.broadcast_to(rows_of(me), (8, LANES)).astype(I32)
    scr[...] = jnp.full((8, LANES), -1.0, F32)
    nbr_all = nbr_ref[...]
    away_all = ((nbr_all >> 7) != me) & (wall_ref[...] == 0)
    scr[0:6, :] = jnp.where(away_all, nbr_all >> 7, -1).astype(F32)
    neighbour = jnp.max(scr[...], axis=1, keepdims=True).astype(I32)
    low_half = lane < 64
    for axis in range(3):
        rows = slice(axis * LANES, axis * LANES + LANES)
        codes, aways = [], []
        for side in range(2):
            face = 2 * axis + side
            nbr = nbr_ref[face : face + 1, :]
            is_wall = wall_ref[face : face + 1, :] == 1
            remote = ((nbr >> 7) != me) & jnp.logical_not(is_wall)
            wanted = column(jnp.where(remote, nbr & 127, -1).astype(F32), diag)
            hit = rows_of(neighbour[face : face + 1, :]) == wanted
            hot_ref[rows, side * LANES : (side + 1) * LANES] = jnp.where(hit, 1.0, 0.0).astype(BF16)
            codes.append(column(orient_ref[face : face + 1, :].astype(F32), diag).astype(I32))
            aways.append(wanted)
        code = jnp.where(low_half, codes[0], codes[1])
        a, b = (lane >> 3) & 7, lane & 7
        swap = code >= 4
        a1, b1 = jnp.where(swap, b, a), jnp.where(swap, a, b)
        a2 = jnp.where((code & 1) == 1, 7 - a1, a1)
        b2 = jnp.where((code & 2) == 2, 7 - b1, b1)
        h = jnp.where(low_half, 1, 0)
        if axis == 0:
            top = ((a2 >> 2) ^ h) * 8 + ((b2 >> 2) ^ h) * 4
            group, v = top + ((a2 ^ b2) & 3), a2 & 3
        elif axis == 1:
            top = ((a2 >> 2) ^ h) * 8 + (((a2 >> 1) & 1) ^ (b2 >> 2)) * 4
            group, v = top + ((b2 & 3) ^ (h * 3)), (a2 & 1) * 2 + (b2 >> 2)
        else:
            top = ((a2 >> 2) ^ (b2 >> 2)) * 8 + (((a2 >> 1) & 1) ^ h) * 4
            group, v = top + ((b2 & 3) ^ (h * 3)), (a2 & 1) * 2 + (b2 >> 2)
        is_far = jnp.where(low_half, aways[0], aways[1]) >= 0.0
        index_ref[rows, :] = h * 64 + jnp.where(is_far, v * 16 + group, a2 * 8 + b2)


SHIFT_A, SHIFT_B = (3, 9)


def shift_of(i):
    return (i & 3) ^ ((i >> 2) & 1) * (4 * SHIFT_A) ^ (i >> 3) * (4 * SHIFT_B)


def forward_kernel(me_ref, spot_ref, in_ref, label_ref, column_ref, out_ref, zed_ref, held, made, sem):
    for number in range(DEVS // 2):
        start = spot_ref[2048 + number] * 33
        for j in range(32):
            held[pl.ds(spot_ref[number * 32 + j], 1), :] = in_ref[pl.ds(start + j, 1), :]
    shape = (LANES, LANES)
    lane = iota(shape, 1)
    zeds = in_ref[pl.ds(32, LANES, stride=33), :]
    zed_ref[...] = zeds
    zed = jnp.take_along_axis(zeds, label_ref[...], axis=1)
    me = me_ref[0]
    g3, g2, g1, g0 = (me >> 3) & 1, (me >> 2) & 1, (me >> 1) & 1, me & 1
    lane = iota((8, LANES), 1)
    h, v1, v0 = lane >> 6, (lane >> 1) & 1, lane & 1
    nodes = [
        h * 16 + (g3 ^ h) * 8 + v1 * 4 + v0 * 2 + (g2 ^ h),
        v1 * 16 + h * 14 + v0,
        v1 * 16 + v0 * 8 + (g1 ^ h) * 4 + (g0 ^ h) * 2 + h,
    ]
    here = (lane >> 2) & 15
    shift = (here & 3) ^ ((here >> 2) & 1) * (4 * SHIFT_A) ^ (here >> 3) * (4 * SHIFT_B)
    which = []
    for axis in range(3):
        for field in (0, 1 + axis):
            value = jnp.full((8, LANES), -1, I32)
            for i in range(16):
                spot = lane ^ shift_of(i)
                n = spot >> 2
                i0, j2, j1, j0, k2 = (n >> 4) & 1, (n >> 3) & 1, (n >> 2) & 1, (n >> 1) & 1, n & 1
                if axis == 0:
                    hit = (j2 == g3 ^ i0) & (k2 == g2 ^ i0)
                elif axis == 1:
                    hit = (j2 == j1) & (j1 == j0)
                else:
                    hit = (j1 == g1 ^ k2) & (j0 == g0 ^ k2)
                value = jnp.where(hit & (spot & 3 == field), i, value)
            which.append(value)
    sign = half_sign((8, LANES))
    waves = [[], [], []]
    for quad in range(4):
        blocks = range(quad * 4, quad * 4 + 4)
        merged = [[jnp.zeros((8, LANES), F32)] * 6 for _ in blocks]
        for i in range(16):
            hits = [which[m] == i for m in range(6)]
            for b, block in enumerate(blocks):
                rows = held[pl.ds(block * 136 + i, 8, stride=17), :]
                rows = jnp.take_along_axis(rows, lane ^ shift_of(i), axis=1)
                merged[b] = [jnp.where(hits[m], rows, merged[b][m]) for m in range(6)]
        wide = [
            jnp.take_along_axis(zed[block * 8 : block * 8 + 8, :], here, axis=1) * sign for block in blocks
        ]
        for axis in range(3):
            at = (nodes[axis] * 4) ^ shift
            press = [jnp.take_along_axis(merged[b][2 * axis], at, axis=1) for b in range(4)]
            at = (nodes[axis] * 4 + 1 + axis) ^ shift
            speed = [jnp.take_along_axis(merged[b][2 * axis + 1], at, axis=1) for b in range(4)]
            waves[axis] += [press[b] + wide[b] * speed[b] for b in range(4)]
    low_half = iota(shape, 1) < 64
    lane = iota(shape, 1).astype(F32)
    halos = []
    for axis in range(3):
        wave = jnp.concatenate(waves[axis], axis=0)
        upper = column_ref[:, 2 * axis + 1 : 2 * axis + 2] == lane
        lower = column_ref[:, 2 * axis : 2 * axis + 1] == lane
        pick = jnp.concatenate([jnp.where(upper, 1.0, 0.0), jnp.where(lower, 1.0, 0.0)], axis=1)
        table = jnp.concatenate([jnp.where(low_half, wave, 0.0), jnp.where(low_half, 0.0, wave)], axis=0)
        halos.append(pick_dot(pick, table))
    copies = []
    for part in range(4):
        base = part * 32
        for target in range(base, base + 32):
            made[target * 19 : target * 19 + 16, :] = held[target * 17 : target * 17 + 16, :]
        for axis in range(3):
            made[pl.ds(base * 19 + 16 + axis, 32, stride=19), :] = halos[axis][base : base + 32, :]
        rows = pl.ds(base * 19, 608)
        copies.append(pltpu.make_async_copy(made.at[rows], out_ref.at[rows], sem.at[part]))
        copies[-1].start()
    for copy in copies:
        copy.wait()


def across_kernel(me_ref, owner_ref, zed_ref, nbr_ref, wall_ref, row_ref, out_ref, near_ref, place_ref):
    shape = (LANES, LANES)
    lane = iota(shape, 1)
    diag = iota(shape, 0) == lane
    me = me_ref[0]
    own = zed_ref[pl.ds(me, 1), :]
    for axis in range(3):
        rows = slice(axis * LANES, axis * LANES + LANES)
        zeds = []
        for side in range(2):
            face = 2 * axis + side
            other = zed_ref[pl.ds(jnp.maximum(owner_ref[face * LANES + me], 0), 1), :]
            nbr = nbr_ref[face : face + 1, :]
            is_wall = wall_ref[face : face + 1, :] == 1
            remote = ((nbr >> 7) != me) & jnp.logical_not(is_wall)
            far = column(jnp.where(remote, 1.0, 0.0), diag) > 0.0
            spot = column((nbr & 127).astype(F32), diag) == lane.astype(F32)
            wall = column(jnp.where(is_wall, 1.0, 0.0), diag) > 0.0
            value = jnp.where(spot, jnp.where(far, other, own), 0.0)
            zeds.append(jnp.where(wall, -1.0, jnp.sum(value, axis=1, keepdims=True)))
            local = jnp.where(far | wall, 0.0, jnp.where(spot, 1.0, 0.0))
            near_ref[rows, side * LANES : (side + 1) * LANES] = local.astype(BF16)
        out_ref[rows, :] = jnp.where(lane < 64, zeds[0], zeds[1])
    place_ref[...] = jnp.where(row_ref[0:1, :] == iota(shape, 0), 1.0, 0.0).astype(BF16)


def exchange_lanes(arrays):
    lane = iota(arrays[0].shape, 1)
    bits = (lane_bit(lane, 6), lane_bit(lane, 5), lane_bit(lane, 4))

    def mix(eight):
        for step, bit in zip((1, 2, 4), bits[::-1]):
            eight = [jnp.where(bit, eight[t ^ step], eight[t]) for t in range(8)]
        return eight

    turned = mix(arrays)
    turned = [jnp.take_along_axis(turned[t], lane ^ (t * 16), axis=1) for t in range(8)]
    return mix(turned)


def final_kernel(
    in_ref, place_ref, cols_ref, zed_ref, near_ref, far_ref, index_ref, side_ref, stack_ref, coef_ref,
    out_ref, state, turned, lift, loose, made, sem,
):
    shape = (LANES, LANES)
    lane = iota(shape, 1)
    low_half = lane < 64
    place = place_ref[...]
    place = jnp.concatenate([place, place, place], axis=1)
    for group in range(0, 16, 2):
        pair = []
        for g in (group, group + 1):
            rows = [in_ref[(k * 16 + g) * 19 : (k * 16 + g) * 19 + 16, :] for k in range(8)]
            pair.append(jnp.concatenate(rows, axis=0))
        parts = split3(jnp.concatenate(pair, axis=1))
        moved = jnp.dot(place, jnp.concatenate(parts, axis=0), preferred_element_type=F32)
        state[group * LANES : (group + 1) * LANES, :] = moved[:, 0:LANES]
        state[(group + 1) * LANES : (group + 2) * LANES, :] = moved[:, LANES:]
    for block in range(16):
        at = [c * LANES + block * 8 for c in range(16)]
        chunks = regroup([state[a : a + 8, :] for a in at], True)
        for c in range(16):
            state[at[c] : at[c] + 8, :] = chunks[c]

    def chunk(field, n4):
        start = (n4 * 4 + field) * LANES
        return state[start : start + LANES, :]

    zed = cols_ref[:, 0:1]
    for axis in range(3):
        rows = slice(axis * LANES, axis * LANES + LANES)
        press, norm, wave = face_pair(chunk, axis, zed)
        turned[...] = in_ref[pl.ds(16 + axis, LANES, stride=19), :].T
        parts = [turned[pl.ds(h * 64 + v, 16, stride=4), :] for h in range(2) for v in range(4)]
        far = jnp.concatenate(exchange_lanes(parts), axis=0)
        masked = []
        for value in (wave, far):
            masked.append(jnp.where(low_half, 0.0, value))
            masked.append(jnp.where(low_half, value, 0.0))
        hot = [near_ref[rows, :], far_ref[rows, :]]
        both = jnp.dot(
            jnp.concatenate(hot * 3, axis=1),
            jnp.concatenate(split3(jnp.concatenate(masked, axis=0)), axis=0),
            preferred_element_type=F32,
        )
        wave_out = jnp.take_along_axis(both, index_ref[rows, :], axis=1)
        zed_out = zed_ref[rows, :]
        jump = (wave_out - press + zed_out * norm) / (zed + zed_out)
        lift[rows, :] = jnp.where(zed_out < 0.0, norm, jump)

    lane = iota((32, LANES), 1)
    low_half = lane < 64
    i2, j, k = lane >> 6, (lane >> 3) & 7, lane & 7
    on_y, on_z = (j == 0) | (j == 7), (k == 0) | (k == 7)
    copies = []
    for part in range(4):
        rows = slice(part * 32, part * 32 + 32)
        zed, bulk, dens = cols_ref[rows, 0:1], cols_ref[rows, 1:2], cols_ref[rows, 2:3]
        by_bulk = -metric_scale * bulk
        by_dens = -(metric_scale / dens)
        up = LIFT * bulk
        across = -LIFT * zed / dens
        piece = {}
        for field in range(4):
            for n4 in range(4):
                start = (n4 * 4 + field) * LANES + part * 32
                piece[field, n4] = state[start : start + 32, :]
        cut = []
        for field in (0, 2, 3):
            whole = jnp.concatenate([piece[field, n4] for n4 in range(4)], axis=0)
            high = whole.astype(BF16)
            cut.append((high, (whole - high.astype(F32)).astype(BF16)))
        grad = jnp.dot(
            jnp.concatenate([cut[0][0], cut[0][1], cut[0][0]], axis=1), side_ref[...], preferred_element_type=F32
        )
        across_div = jnp.dot(
            jnp.concatenate([cut[1][0], cut[2][0], cut[1][1], cut[2][1], cut[1][0], cut[2][0]], axis=1),
            stack_ref[...],
            preferred_element_type=F32,
        )
        swapped = {}
        for field in (0, 1):
            for n4 in range(4):
                swapped[field, n4] = pltpu.roll(piece[field, n4], 64, 1)
        jumps = [lift[axis * LANES + part * 32 : axis * LANES + part * 32 + 32, :] for axis in range(3)]
        base = part * 544
        for n4 in range(4):
            along = {}
            for field in (0, 1):
                total = None
                for m4 in range(4):
                    at = (n4 * 4 + m4) * 2
                    term = piece[field, m4] * coef_ref[at : at + 1, :]
                    term = term + swapped[field, m4] * coef_ref[at + 1 : at + 2, :]
                    total = term if total is None else total + term
                along[field] = total
            block = slice(n4 * 32, n4 * 32 + 32)
            div = along[1] + across_div[block, :]
            grads = [along[0], grad[block, 0:LANES], grad[block, LANES:]]
            face_i = 2 * n4 + i2
            from_y = jnp.where(j == 7, 64, 0) + face_i * 8 + k
            from_z = jnp.where(k == 7, 64, 0) + face_i * 8 + j
            total = None
            for axis in range(3):
                jump = jumps[axis]
                value = by_dens * grads[axis]
                here = None
                if axis == 0 and n4 == 0:
                    here = jnp.where(low_half, jump, 0.0)
                    turn = -here
                elif axis == 0 and n4 == 3:
                    here = jnp.where(low_half, 0.0, jump)
                    turn = here
                elif axis == 1:
                    here = jnp.where(on_y, jnp.take_along_axis(jump, from_y, axis=1), 0.0)
                    turn = jnp.where(j == 0, -here, here)
                elif axis == 2:
                    here = jnp.where(on_z, jnp.take_along_axis(jump, from_z, axis=1), 0.0)
                    turn = jnp.where(k == 0, -here, here)
                if here is not None:
                    value = value + across * turn
                    total = here if total is None else total + here
                loose[pl.ds(base + n4 * 4 + 1 + axis, 32, stride=17), :] = value
            loose[pl.ds(base + n4 * 4, 32, stride=17), :] = by_bulk * div + up * total
        for row in range(32):
            at = (part * 32 + row) * 16
            made[at : at + 16, :] = loose[base + row * 17 : base + row * 17 + 16, :]
        window = pl.ds(part * 512, 512)
        copies.append(pltpu.make_async_copy(made.at[window], out_ref.at[window], sem.at[part]))
        copies[-1].start()
    for copy in copies:
        copy.wait()


def vm():
    return pl.BlockSpec(memory_space=VMEM)


def sm():
    return pl.BlockSpec(memory_space=SMEM)


def shaped(shape, dtype=F32):
    return VMEM(shape, dtype)


def plain(shape, dtype=F32):
    return jax.ShapeDtypeStruct(shape, dtype)


def near(value):
    return pltpu.with_memory_space_constraint(value, VMEM)


def away(value):
    return pltpu.with_memory_space_constraint(value, HBM)


GRANT = pltpu.CompilerParams(vmem_limit_bytes=24 * 1024 * 1024)


def exchange(flat, rows):
    blocks = flat.reshape(DEVS, rows, 1, LANES)
    return lax.all_to_all(blocks, AXES, split_axis=0, concat_axis=0, tiled=True).reshape(flat.shape)


def body(old_state, dest_row, neighbours, orientation, wall_flags, bulk_modulus, density):
    me = (lax.axis_index("grp") * lax.axis_size("dev") + lax.axis_index("dev")).astype(I32).reshape(1)
    dest = dest_row.reshape(2, LANES)
    bulk = away(bulk_modulus.reshape(1, LANES))
    dens = away(density.reshape(1, LANES))
    nbr, wall, orient = away(neighbours), away(wall_flags), away(orientation)
    state = old_state.reshape(256, 4, 4, LANES).transpose(0, 2, 1, 3).reshape(4096, LANES)

    info, pos = pl.pallas_call(
        order_kernel,
        in_specs=[sm()] + [vm()] * 3,
        out_specs=[vm()] * 2,
        out_shape=[shaped((384, LANES), I32), plain((2, LANES), I32)],
        scratch_shapes=[pltpu.VMEM((8, LANES), F32)],
        name="order",
        compiler_params=GRANT,
    )(me, away(dest), nbr, wall)
    heard = exchange(info, 3)
    pieces = pl.pallas_call(
        pack_kernel,
        in_specs=[sm(), pl.BlockSpec(memory_space=pl.ANY), vm(), vm()],
        out_specs=pl.BlockSpec(memory_space=pl.ANY),
        out_shape=HBM((4224, LANES), F32),
        scratch_shapes=[
            pltpu.VMEM((4096, LANES), F32),
            pltpu.VMEM((4224, LANES), F32),
            pltpu.SemaphoreType.DMA((4,)),
            pltpu.SemaphoreType.DMA((8,)),
        ],
        name="pack",
        compiler_params=GRANT,
    )(pos, away(state), bulk, dens)
    spread = exchange(pieces, 33)
    spots, owners, blocks, rows, labels, cols, index, far = pl.pallas_call(
        table_kernel,
        in_specs=[sm()] + [vm()] * 6,
        out_specs=[vm()] * 8,
        out_shape=[
            shaped((24, LANES), I32),
            shaped((8, LANES), I32),
            shaped((LANES, LANES)),
            shaped((8, LANES), I32),
            shaped((LANES, LANES), I32),
            shaped((LANES, LANES)),
            shaped((384, LANES), I32),
            shaped((384, 2 * LANES), BF16),
        ],
        scratch_shapes=[pltpu.VMEM((LANES, LANES), I32), pltpu.VMEM((8, LANES), F32)],
        name="table",
        compiler_params=GRANT,
    )(me, near(heard), nbr, wall, orient, bulk, dens)
    owners = owners.reshape(1024)
    passed, zeds = pl.pallas_call(
        forward_kernel,
        in_specs=[sm()] * 2 + [vm()] * 3,
        out_specs=[pl.BlockSpec(memory_space=pl.ANY), vm()],
        out_shape=[HBM((2432, LANES), F32), shaped((LANES, LANES))],
        scratch_shapes=[
            pltpu.VMEM((2176, LANES), F32),
            pltpu.VMEM((2432, LANES), F32),
            pltpu.SemaphoreType.DMA((4,)),
        ],
        name="forward",
        compiler_params=GRANT,
    )(me, spots.reshape(3072), near(spread), near(labels), near(blocks))
    arrived = exchange(passed, 19)
    zed_out, close, place = pl.pallas_call(
        across_kernel,
        in_specs=[sm()] * 2 + [vm()] * 4,
        out_specs=[vm()] * 3,
        out_shape=[shaped((384, LANES)), shaped((384, 2 * LANES), BF16), shaped((LANES, LANES), BF16)],
        name="across",
        compiler_params=GRANT,
    )(me, owners, near(zeds), nbr, wall, near(rows))
    result = pl.pallas_call(
        final_kernel,
        in_specs=[vm()] * 10,
        out_specs=pl.BlockSpec(memory_space=pl.ANY),
        out_shape=plain((2048, LANES)),
        scratch_shapes=[
            pltpu.VMEM((2048, LANES), F32),
            pltpu.VMEM((LANES, LANES), F32),
            pltpu.VMEM((384, LANES), F32),
            pltpu.VMEM((2176, LANES), F32),
            pltpu.VMEM((2048, LANES), F32),
            pltpu.SemaphoreType.DMA((4,)),
        ],
        name="final",
        compiler_params=GRANT,
    )(
        near(arrived), near(place), near(cols), near(zed_out), near(close), near(far), near(index),
        jnp.asarray(SIDE3), jnp.asarray(STACKED3), jnp.asarray(COEF),
    )
    return result.reshape(128, 4, 4, LANES).transpose(0, 2, 1, 3).reshape(128, 4, 512)


def solution(mesh):
    both = P(AXES)
    faces = P(None, AXES)
    in_specs = (P(AXES, None, None), both, faces, faces, faces, both, both)
    return jax.shard_map(
        body, mesh=mesh, in_specs=in_specs, out_specs=P(AXES, None, None), check_vma=False
    )
```

```python
import jax
import jax.numpy as jnp
import numpy as np
from jax import lax
from jax.experimental import pallas as pl
from jax.experimental.pallas import tpu as pltpu
from jax.sharding import PartitionSpec as P

NP = 8
DEVS = 128
LANES = 128
AXES = ("grp", "dev")
metric_scale = 0.25
F32 = jnp.float32
I32 = jnp.int32
BF16 = jnp.bfloat16
VMEM = pltpu.MemorySpace.VMEM
SMEM = pltpu.MemorySpace.SMEM
HBM = pltpu.MemorySpace.HBM


def gll_tables(poly_order):
    num_points = poly_order + 1
    points = -np.cos(np.pi * np.arange(num_points) / poly_order)
    legendre = np.zeros((num_points, num_points))
    for sweeps in range(101):
        legendre[:, 0] = 1.0
        legendre[:, 1] = points
        for degree in range(2, num_points):
            legendre[:, degree] = (
                (2 * degree - 1) * points * legendre[:, degree - 1]
                - (degree - 1) * legendre[:, degree - 2]
            ) / degree
        if sweeps < 100:
            points = points - (points * legendre[:, poly_order] - legendre[:, poly_order - 1]) / (
                num_points * legendre[:, poly_order]
            )
    end_values = legendre[:, poly_order]
    weights = 2.0 / (poly_order * num_points * end_values**2)
    distance = points[:, None] - points[None, :] + np.eye(num_points)
    derivative = end_values[:, None] / end_values[None, :] / distance
    derivative = derivative * (1.0 - np.eye(num_points))
    derivative[0, 0] = -poly_order * num_points / 4.0
    derivative[poly_order, poly_order] = poly_order * num_points / 4.0
    return (points, weights, derivative)


POINTS, WEIGHTS, DERIV = gll_tables(NP - 1)
DERIV = DERIV.astype(np.float32)
LIFT = metric_scale / float(WEIGHTS[0])


def derivative_tables():
    eye2, eye8 = np.eye(2, dtype=np.float32), np.eye(8, dtype=np.float32)
    along_y = np.kron(eye2, np.kron(DERIV.T, eye8))
    along_z = np.kron(eye2, np.kron(eye8, DERIV.T))
    side = np.concatenate([along_y, along_z], axis=1)
    stacked = np.concatenate([along_y, along_z], axis=0)
    coef = np.zeros((4, 4, 2, LANES), np.float32)
    for out_chunk in range(4):
        for in_chunk in range(4):
            for half in range(2):
                lanes = slice(64 * half, 64 * half + 64)
                coef[out_chunk, in_chunk, 0, lanes] = DERIV[2 * out_chunk + half, 2 * in_chunk + half]
                coef[out_chunk, in_chunk, 1, lanes] = DERIV[
                    2 * out_chunk + half, 2 * in_chunk + 1 - half
                ]
    return side, stacked, coef.reshape(32, LANES)


SIDE, STACKED, COEF = derivative_tables()


def three_parts(table):
    high = table.astype(jnp.bfloat16)
    low = (table - high.astype(np.float32)).astype(jnp.bfloat16)
    return np.concatenate([high, high, low], axis=0)


SIDE3, STACKED3 = three_parts(SIDE), three_parts(STACKED)


def iota(shape, axis):
    return lax.broadcasted_iota(I32, shape, axis)


def small_dot(left, right):
    return jnp.dot(left.astype(BF16), right.astype(BF16), preferred_element_type=F32)


def split3(value):
    high = value.astype(BF16)
    rest = value - high.astype(F32)
    middle = rest.astype(BF16)
    low = (rest - middle.astype(F32)).astype(BF16)
    return high, middle, low


def pick_dot(pick, value):
    pick = pick.astype(BF16)
    high, middle, low = split3(value)
    total = jnp.dot(pick, high, preferred_element_type=F32)
    total = total + jnp.dot(pick, middle, preferred_element_type=F32)
    return total + jnp.dot(pick, low, preferred_element_type=F32)


def column(row, diag):
    wide = jnp.broadcast_to(row, (LANES, LANES))
    return jnp.sum(jnp.where(diag, wide, 0.0), axis=1, keepdims=True)


def half_sign(shape):
    return jnp.where(iota(shape, 1) < 64, -1.0, 1.0)


def face_pair(chunk, axis, zed):
    lane = iota((LANES, LANES), 1)
    half, face_i, face_b = lane >> 6, (lane >> 3) & 7, lane & 7
    from_y = (face_i & 1) * 64 + half * 56 + face_b
    from_z = (face_i & 1) * 64 + face_b * 8 + half * 7
    values = []
    for field in (0, 1 + axis):
        if axis == 0:
            value = jnp.where(lane < 64, chunk(field, 0), chunk(field, 3))
        else:
            index = from_y if axis == 1 else from_z
            value = jnp.take_along_axis(chunk(field, 0), index, axis=1)
            for n4 in range(1, 4):
                other = jnp.take_along_axis(chunk(field, n4), index, axis=1)
                value = jnp.where(face_i >> 1 == n4, other, value)
        values.append(value)
    normal = half_sign((LANES, LANES)) * values[1]
    return values[0], normal, values[0] + zed * normal


def cross(arrays, bit1, bit0):
    first = [jnp.where(bit0, arrays[t ^ 1], arrays[t]) for t in range(4)]
    return [jnp.where(bit1, first[t ^ 2], first[t]) for t in range(4)]


def lane_bit(lane, bit):
    return ((lane >> bit) & 1) == 1


def regroup(arrays, back):
    lane = iota(arrays[0].shape, 1)
    own = (lane >> 3) & 3
    plain = (lane_bit(lane, 1), lane_bit(lane, 0))
    mixed = (lane_bit(lane ^ (lane >> 3), 1), lane_bit(lane ^ (lane >> 3), 0))
    enter, leave = (plain, mixed) if back else (mixed, plain)
    result = [None] * 16
    for top in range(4):
        four = cross(arrays[4 * top : 4 * top + 4], *enter)
        four = [jnp.take_along_axis(four[t], lane ^ t ^ own, axis=1) for t in range(4)]
        result[4 * top : 4 * top + 4] = cross(four, *leave)
    j2, k2 = lane_bit(lane, 5), lane_bit(lane, 2)
    final = [None] * 16
    for t in range(4):
        final[t::4] = cross(result[t::4], j2, k2)
    return final


def order_kernel(
    me_ref, dest_ref, nbr_ref, wall_ref, bulk_ref, dens_ref, info_ref, pos_ref, zed_ref, scr
):
    zed_ref[...] = jnp.broadcast_to(jnp.sqrt(bulk_ref[...] * dens_ref[...]), (8, LANES))
    dest = dest_ref[...]
    sub = iota((LANES, LANES), 0)
    lane = iota((LANES, LANES), 1)
    diag = sub == lane
    key_row, key_col, dest_col = [], [], []
    for half in range(2):
        row = jnp.broadcast_to(dest[half : half + 1, :], (LANES, LANES))
        key = (row >> 7).astype(F32) * 256.0 + (lane + 128 * half).astype(F32)
        key_row.append(key)
        key_col.append(jnp.sum(jnp.where(diag, key, 0.0), axis=1, keepdims=True))
        dest_col.append(jnp.sum(jnp.where(diag, row.astype(F32), 0.0), axis=1, keepdims=True))
    lists = [jnp.zeros((1, LANES), F32), jnp.zeros((1, LANES), F32)]
    for half in range(2):
        before_col = jnp.zeros((LANES, 1), F32)
        before_row = jnp.zeros((1, LANES), F32)
        for other in range(2):
            before_col = before_col + jnp.sum(
                jnp.where(key_row[other] < key_col[half], 1.0, 0.0), axis=1, keepdims=True
            )
            before_row = before_row + jnp.sum(
                jnp.where(key_col[other] < key_row[half], 1.0, 0.0), axis=0, keepdims=True
            )
        spot = before_row.astype(I32)
        spot = (spot & 7) * 528 + (spot >> 3)
        pos_ref[half : half + 1, :] = jnp.where(dest[half : half + 1, :] >= 0, spot, -1)
        place = before_col.astype(I32)
        k = place & 7
        spot = (k & 3) * 32 + (place >> 3)
        for part in range(2):
            hit = (spot == lane) & (k >> 2 == part)
            lists[part] = lists[part] + jnp.sum(jnp.where(hit, dest_col[half], 0.0), axis=0, keepdims=True)
    scr[...] = jnp.full((8, LANES), -1.0, F32)
    owner = nbr_ref[...] >> 7
    remote = (owner != me_ref[0]) & (wall_ref[...] == 0)
    scr[0:6, :] = jnp.where(remote, owner, -1).astype(F32)
    owners = jnp.max(scr[...], axis=1, keepdims=True)
    spread = iota((8, LANES), 0) == iota((8, LANES), 1)
    owner_row = jnp.sum(jnp.where(spread, owners, 0.0), axis=0, keepdims=True)
    for part, row in enumerate((lists[0], lists[1], owner_row)):
        info_ref[pl.ds(part, LANES, stride=3), :] = jnp.broadcast_to(row, (LANES, LANES)).astype(I32)


def pack_kernel(pos_ref, state_ref, zed_ref, out_ref, rows, made, in_sem, out_sem):
    full = pos_ref[0] >= 0
    loads = []
    for part in range(4):
        window = pl.ds(part * 1024, 1024)
        loads.append(pltpu.make_async_copy(state_ref.at[window], rows.at[window], in_sem.at[part]))

    @pl.when(full)
    def _():
        for load in loads:
            load.start()

    made[pl.ds(32, LANES, stride=33), :] = jnp.broadcast_to(zed_ref[0:1, :], (LANES, LANES))

    @pl.when(full)
    def _():
        def one(slot, carry):
            made[pl.ds(pos_ref[slot], 16, stride=33), :] = rows[pl.ds(pl.multiple_of(slot * 16, 16), 16), :]
            return carry

        for part in range(4):
            loads[part].wait()
            lax.fori_loop(part * 64, part * 64 + 64, one, 0, unroll=16)

    stores = []
    for k in range(8):

        @pl.when(full)
        def _():
            for block in range(4):
                at = [(k * 16 + c) * 33 + block * 8 for c in range(16)]
                groups = regroup([made[a : a + 8, :] for a in at], False)
                for g in range(16):
                    made[at[g] : at[g] + 8, :] = groups[g]

        window = pl.ds(k * 528, 528)
        stores.append(pltpu.make_async_copy(made.at[window], out_ref.at[window], out_sem.at[k]))
        stores[-1].start()
    for store in stores:
        store.wait()


def table_kernel(
    me_ref, info_ref, nbr_ref, wall_ref, orient_ref, bulk_ref, dens_ref,
    spot_ref, owner_ref, column_ref, label_ref, cols_ref, index_ref, hot_ref, near_ref, place_ref, wide, scr,
):
    shape = (LANES, LANES)
    sub = iota(shape, 0)
    lane = iota(shape, 1)
    diag = sub == lane
    me = me_ref[0]
    bulk = column(bulk_ref[...], diag)
    dens = column(dens_ref[...], diag)
    zed = column(jnp.sqrt(bulk_ref[...] * dens_ref[...]), diag)
    cols = jnp.where(lane == 0, zed, jnp.where(lane == 1, bulk, dens))

    lists = [info_ref[pl.ds(0, LANES, stride=3), :], info_ref[pl.ds(1, LANES, stride=3), :]]
    owners = info_ref[pl.ds(2, LANES, stride=3), :].astype(F32)
    owner_ref[...] = owners.T[0:8, :].astype(I32)
    column_ref[...] = owners
    target = lists[0] >> 7
    my_k = me >> 4
    mine = jnp.where(my_k >= 4, lists[1], lists[0])
    mine = jnp.take_along_axis(mine, (my_k & 3) * 32 + (lane & 31), axis=1) & 127
    present = jnp.zeros(shape, F32)
    label = jnp.zeros(shape, F32)
    mine = mine.astype(F32)
    for j in range(32):
        hit = target[:, j : j + 1] == lane
        present = jnp.where(hit, 1.0, present)
        label = jnp.where(hit, mine[:, j : j + 1], label)
    below = jnp.where(lane < sub, 1.0, 0.0)
    rank = small_dot(below, present)
    safe = jnp.clip(target, 0, LANES - 1)
    slot = safe * 17 + jnp.take_along_axis(rank.astype(I32), safe, axis=1)
    is_source = jnp.broadcast_to(jnp.where(target[:, 0:1] >= 0, 1.0, 0.0), shape)
    source_rank = jnp.where(is_source > 0.0, small_dot(below, is_source), -1.0)
    chosen = jnp.where(source_rank.T == sub.astype(F32), 1.0, 0.0)
    wide[...] = pick_dot(chosen, jnp.where(lane == 32, sub, slot).astype(F32)).astype(I32)
    quarter = iota((16, LANES), 1) >> 5
    spots = wide[pl.ds(0, 16, stride=4), :]
    for part in range(1, 4):
        moved = pltpu.roll(wide[pl.ds(part, 16, stride=4), :], 32 * part, 1)
        spots = jnp.where(quarter == part, moved, spots)
    spot_ref[0:16, :] = spots
    sources = jnp.where(diag, jnp.broadcast_to(wide[:, 32:33], shape).astype(F32), 0.0)
    sources = jnp.sum(sources, axis=0, keepdims=True).astype(I32)
    spot_ref[16:24, :] = jnp.broadcast_to(sources, (8, LANES))
    order = jnp.where(present > 0.0, rank, -1.0)
    labels = jnp.zeros(shape, F32)
    for i in range(16):
        row = jnp.sum(jnp.where(order == float(i), label, 0.0), axis=0, keepdims=True)
        labels = jnp.where(sub == i, row, labels)
    label_ref[...] = labels.T.astype(I32)

    gather = [jnp.where((sub >> 5) + 4 * part == lane >> 4, 1.0, 0.0) for part in range(2)]

    def rows_of(block):
        value = jnp.zeros(shape, F32)
        for part in range(2):
            held = jnp.where(lists[part] >> 7 == block, (lists[part] & 127).astype(F32), 0.0)
            value = value + small_dot(held, gather[part])
        source = jnp.sum(jnp.where(lane == block, order, 0.0), axis=1, keepdims=True)
        chosen = source == (lane & 15).astype(F32)
        return jnp.sum(jnp.where(chosen, value, 0.0), axis=0, keepdims=True)

    place_ref[...] = jnp.where(rows_of(me) == sub.astype(F32), 1.0, 0.0).astype(BF16)
    scr[...] = jnp.full((8, LANES), -1.0, F32)
    nbr_all = nbr_ref[...]
    away_all = ((nbr_all >> 7) != me) & (wall_ref[...] == 0)
    scr[0:6, :] = jnp.where(away_all, nbr_all >> 7, -1).astype(F32)
    neighbour = jnp.max(scr[...], axis=1, keepdims=True).astype(I32)
    low_half = lane < 64
    for axis in range(3):
        rows = slice(axis * LANES, axis * LANES + LANES)
        codes, aways = [], []
        for side in range(2):
            face = 2 * axis + side
            nbr = nbr_ref[face : face + 1, :]
            is_wall = wall_ref[face : face + 1, :] == 1
            remote = ((nbr >> 7) != me) & jnp.logical_not(is_wall)
            wanted = column(jnp.where(remote, nbr & 127, -1).astype(F32), diag)
            hit = rows_of(neighbour[face : face + 1, :]) == wanted
            hot_ref[rows, side * LANES : (side + 1) * LANES] = jnp.where(hit, 1.0, 0.0).astype(BF16)
            codes.append(column(orient_ref[face : face + 1, :].astype(F32), diag).astype(I32))
            aways.append(wanted)
            wall = column(jnp.where(is_wall, 1.0, 0.0), diag) > 0.0
            spot = column((nbr & 127).astype(F32), diag)
            far = wanted >= 0.0
            local = jnp.where(far | wall, 0.0, jnp.where(spot == lane.astype(F32), 1.0, 0.0))
            near_ref[rows, side * LANES : (side + 1) * LANES] = local.astype(BF16)
            cols = jnp.where(lane == 8 + face, spot, cols)
            cols = jnp.where(lane == 16 + face, jnp.where(wall, -1.0, jnp.where(far, 1.0, 0.0)), cols)
        code = jnp.where(low_half, codes[0], codes[1])
        a, b = (lane >> 3) & 7, lane & 7
        swap = code >= 4
        a1, b1 = jnp.where(swap, b, a), jnp.where(swap, a, b)
        a2 = jnp.where((code & 1) == 1, 7 - a1, a1)
        b2 = jnp.where((code & 2) == 2, 7 - b1, b1)
        h = jnp.where(low_half, 1, 0)
        if axis == 0:
            top = ((a2 >> 2) ^ h) * 8 + ((b2 >> 2) ^ h) * 4
            group, v = top + ((a2 ^ b2) & 3), a2 & 3
        elif axis == 1:
            top = ((a2 >> 2) ^ h) * 8 + (((a2 >> 1) & 1) ^ (b2 >> 2)) * 4
            group, v = top + ((b2 & 3) ^ (h * 3)), (a2 & 1) * 2 + (b2 >> 2)
        else:
            top = ((a2 >> 2) ^ (b2 >> 2)) * 8 + (((a2 >> 1) & 1) ^ h) * 4
            group, v = top + ((b2 & 3) ^ (h * 3)), (a2 & 1) * 2 + (b2 >> 2)
        is_far = jnp.where(low_half, aways[0], aways[1]) >= 0.0
        index_ref[rows, :] = h * 64 + jnp.where(is_far, v * 16 + group, a2 * 8 + b2)
    cols_ref[...] = cols


SHIFT_A, SHIFT_B = (3, 9)


def shift_of(i):
    return (i & 3) ^ ((i >> 2) & 1) * (4 * SHIFT_A) ^ (i >> 3) * (4 * SHIFT_B)


def forward_kernel(me_ref, spot_ref, owner_ref, in_ref, label_ref, column_ref, cols_ref, out_ref, zed_ref, held):
    for number in range(DEVS // 2):
        start = spot_ref[2048 + number] * 33
        for j in range(32):
            held[pl.ds(spot_ref[number * 32 + j], 1), :] = in_ref[pl.ds(start + j, 1), :]
    shape = (LANES, LANES)
    lane = iota(shape, 1)
    zeds = in_ref[pl.ds(32, LANES, stride=33), :]
    me = me_ref[0]
    own = in_ref[pl.ds(me * 33 + 32, 1), :]
    for axis in range(3):
        values = []
        for face in (2 * axis, 2 * axis + 1):
            other = in_ref[pl.ds(jnp.maximum(owner_ref[face * LANES + me], 0) * 33 + 32, 1), :]
            kind = cols_ref[:, 16 + face : 17 + face]
            hit = cols_ref[:, 8 + face : 9 + face] == lane.astype(F32)
            value = jnp.where(hit, jnp.where(kind > 0.0, other, own), 0.0)
            values.append(jnp.where(kind < 0.0, -1.0, jnp.sum(value, axis=1, keepdims=True)))
        zed_ref[axis * LANES : axis * LANES + LANES, :] = jnp.where(lane < 64, values[0], values[1])
    zed = jnp.take_along_axis(zeds, label_ref[...], axis=1)
    me = me_ref[0]
    g3, g2, g1, g0 = (me >> 3) & 1, (me >> 2) & 1, (me >> 1) & 1, me & 1
    lane = iota((8, LANES), 1)
    h, v1, v0 = lane >> 6, (lane >> 1) & 1, lane & 1
    nodes = [
        h * 16 + (g3 ^ h) * 8 + v1 * 4 + v0 * 2 + (g2 ^ h),
        v1 * 16 + h * 14 + v0,
        v1 * 16 + v0 * 8 + (g1 ^ h) * 4 + (g0 ^ h) * 2 + h,
    ]
    here = (lane >> 2) & 15
    shift = (here & 3) ^ ((here >> 2) & 1) * (4 * SHIFT_A) ^ (here >> 3) * (4 * SHIFT_B)
    which = []
    for axis in range(3):
        for field in (0, 1 + axis):
            value = jnp.full((8, LANES), -1, I32)
            for i in range(16):
                spot = lane ^ shift_of(i)
                n = spot >> 2
                i0, j2, j1, j0, k2 = (n >> 4) & 1, (n >> 3) & 1, (n >> 2) & 1, (n >> 1) & 1, n & 1
                if axis == 0:
                    hit = (j2 == g3 ^ i0) & (k2 == g2 ^ i0)
                elif axis == 1:
                    hit = (j2 == j1) & (j1 == j0)
                else:
                    hit = (j1 == g1 ^ k2) & (j0 == g0 ^ k2)
                value = jnp.where(hit & (spot & 3 == field), i, value)
            which.append(value)
    sign = half_sign((8, LANES))
    waves = [[], [], []]
    for quad in range(4):
        blocks = range(quad * 4, quad * 4 + 4)
        merged = [[jnp.zeros((8, LANES), F32)] * 6 for _ in blocks]
        for i in range(16):
            hits = [which[m] == i for m in range(6)]
            for b, block in enumerate(blocks):
                rows = held[pl.ds(block * 136 + i, 8, stride=17), :]
                rows = jnp.take_along_axis(rows, lane ^ shift_of(i), axis=1)
                merged[b] = [jnp.where(hits[m], rows, merged[b][m]) for m in range(6)]
        wide = [
            jnp.take_along_axis(zed[block * 8 : block * 8 + 8, :], here, axis=1) * sign for block in blocks
        ]
        for axis in range(3):
            at = (nodes[axis] * 4) ^ shift
            press = [jnp.take_along_axis(merged[b][2 * axis], at, axis=1) for b in range(4)]
            at = (nodes[axis] * 4 + 1 + axis) ^ shift
            speed = [jnp.take_along_axis(merged[b][2 * axis + 1], at, axis=1) for b in range(4)]
            waves[axis] += [press[b] + wide[b] * speed[b] for b in range(4)]
    low_half = iota(shape, 1) < 64
    lane = iota(shape, 1).astype(F32)
    halos = []
    for axis in range(3):
        wave = jnp.concatenate(waves[axis], axis=0)
        upper = column_ref[:, 2 * axis + 1 : 2 * axis + 2] == lane
        lower = column_ref[:, 2 * axis : 2 * axis + 1] == lane
        pick = jnp.concatenate([jnp.where(upper, 1.0, 0.0), jnp.where(lower, 1.0, 0.0)], axis=1)
        table = jnp.concatenate([jnp.where(low_half, wave, 0.0), jnp.where(low_half, 0.0, wave)], axis=0)
        halos.append(pick_dot(pick, table))
    for target in range(DEVS):
        out_ref[target * 19 : target * 19 + 16, :] = held[target * 17 : target * 17 + 16, :]
    for axis in range(3):
        out_ref[pl.ds(16 + axis, LANES, stride=19), :] = halos[axis]


def exchange_lanes(arrays):
    lane = iota(arrays[0].shape, 1)
    bits = (lane_bit(lane, 6), lane_bit(lane, 5), lane_bit(lane, 4))

    def mix(eight):
        for step, bit in zip((1, 2, 4), bits[::-1]):
            eight = [jnp.where(bit, eight[t ^ step], eight[t]) for t in range(8)]
        return eight

    turned = mix(arrays)
    turned = [jnp.take_along_axis(turned[t], lane ^ (t * 16), axis=1) for t in range(8)]
    return mix(turned)


def final_kernel(
    in_ref, place_ref, cols_ref, zed_ref, near_ref, far_ref, index_ref, side_ref, stack_ref, coef_ref,
    out_ref, state, turned, lift, loose, made, sem,
):
    shape = (LANES, LANES)
    lane = iota(shape, 1)
    low_half = lane < 64
    place = place_ref[...]
    place = jnp.concatenate([place, place, place], axis=1)
    for group in range(0, 16, 2):
        pair = []
        for g in (group, group + 1):
            rows = [in_ref[(k * 16 + g) * 19 : (k * 16 + g) * 19 + 16, :] for k in range(8)]
            pair.append(jnp.concatenate(rows, axis=0))
        parts = split3(jnp.concatenate(pair, axis=1))
        moved = jnp.dot(place, jnp.concatenate(parts, axis=0), preferred_element_type=F32)
        state[group * LANES : (group + 1) * LANES, :] = moved[:, 0:LANES]
        state[(group + 1) * LANES : (group + 2) * LANES, :] = moved[:, LANES:]
    for block in range(16):
        at = [c * LANES + block * 8 for c in range(16)]
        chunks = regroup([state[a : a + 8, :] for a in at], True)
        for c in range(16):
            state[at[c] : at[c] + 8, :] = chunks[c]

    def chunk(field, n4):
        start = (n4 * 4 + field) * LANES
        return state[start : start + LANES, :]

    zed = cols_ref[:, 0:1]
    for axis in range(3):
        rows = slice(axis * LANES, axis * LANES + LANES)
        press, norm, wave = face_pair(chunk, axis, zed)
        turned[...] = in_ref[pl.ds(16 + axis, LANES, stride=19), :].T
        parts = [turned[pl.ds(h * 64 + v, 16, stride=4), :] for h in range(2) for v in range(4)]
        far = jnp.concatenate(exchange_lanes(parts), axis=0)
        masked = []
        for value in (wave, far):
            masked.append(jnp.where(low_half, 0.0, value))
            masked.append(jnp.where(low_half, value, 0.0))
        hot = [near_ref[rows, :], far_ref[rows, :]]
        both = jnp.dot(
            jnp.concatenate(hot * 3, axis=1),
            jnp.concatenate(split3(jnp.concatenate(masked, axis=0)), axis=0),
            preferred_element_type=F32,
        )
        wave_out = jnp.take_along_axis(both, index_ref[rows, :], axis=1)
        zed_out = zed_ref[rows, :]
        jump = (wave_out - press + zed_out * norm) / (zed + zed_out)
        lift[rows, :] = jnp.where(zed_out < 0.0, norm, jump)

    lane = iota((32, LANES), 1)
    low_half = lane < 64
    i2, j, k = lane >> 6, (lane >> 3) & 7, lane & 7
    on_y, on_z = (j == 0) | (j == 7), (k == 0) | (k == 7)
    copies = []
    for part in range(4):
        rows = slice(part * 32, part * 32 + 32)
        zed, bulk, dens = cols_ref[rows, 0:1], cols_ref[rows, 1:2], cols_ref[rows, 2:3]
        by_bulk = -metric_scale * bulk
        by_dens = -(metric_scale / dens)
        up = LIFT * bulk
        across = -LIFT * zed / dens
        piece = {}
        for field in range(4):
            for n4 in range(4):
                start = (n4 * 4 + field) * LANES + part * 32
                piece[field, n4] = state[start : start + 32, :]
        cut = []
        for field in (0, 2, 3):
            whole = jnp.concatenate([piece[field, n4] for n4 in range(4)], axis=0)
            high = whole.astype(BF16)
            cut.append((high, (whole - high.astype(F32)).astype(BF16)))
        grad = jnp.dot(
            jnp.concatenate([cut[0][0], cut[0][1], cut[0][0]], axis=1), side_ref[...], preferred_element_type=F32
        )
        across_div = jnp.dot(
            jnp.concatenate([cut[1][0], cut[2][0], cut[1][1], cut[2][1], cut[1][0], cut[2][0]], axis=1),
            stack_ref[...],
            preferred_element_type=F32,
        )
        swapped = {}
        for field in (0, 1):
            for n4 in range(4):
                swapped[field, n4] = pltpu.roll(piece[field, n4], 64, 1)
        jumps = [lift[axis * LANES + part * 32 : axis * LANES + part * 32 + 32, :] for axis in range(3)]
        base = part * 544
        for n4 in range(4):
            along = {}
            for field in (0, 1):
                total = None
                for m4 in range(4):
                    at = (n4 * 4 + m4) * 2
                    term = piece[field, m4] * coef_ref[at : at + 1, :]
                    term = term + swapped[field, m4] * coef_ref[at + 1 : at + 2, :]
                    total = term if total is None else total + term
                along[field] = total
            block = slice(n4 * 32, n4 * 32 + 32)
            div = along[1] + across_div[block, :]
            grads = [along[0], grad[block, 0:LANES], grad[block, LANES:]]
            face_i = 2 * n4 + i2
            from_y = jnp.where(j == 7, 64, 0) + face_i * 8 + k
            from_z = jnp.where(k == 7, 64, 0) + face_i * 8 + j
            total = None
            for axis in range(3):
                jump = jumps[axis]
                value = by_dens * grads[axis]
                here = None
                if axis == 0 and n4 == 0:
                    here = jnp.where(low_half, jump, 0.0)
                    turn = -here
                elif axis == 0 and n4 == 3:
                    here = jnp.where(low_half, 0.0, jump)
                    turn = here
                elif axis == 1:
                    here = jnp.where(on_y, jnp.take_along_axis(jump, from_y, axis=1), 0.0)
                    turn = jnp.where(j == 0, -here, here)
                elif axis == 2:
                    here = jnp.where(on_z, jnp.take_along_axis(jump, from_z, axis=1), 0.0)
                    turn = jnp.where(k == 0, -here, here)
                if here is not None:
                    value = value + across * turn
                    total = here if total is None else total + here
                loose[pl.ds(base + n4 * 4 + 1 + axis, 32, stride=17), :] = value
            loose[pl.ds(base + n4 * 4, 32, stride=17), :] = by_bulk * div + up * total
        for row in range(32):
            at = (part * 32 + row) * 16
            made[at : at + 16, :] = loose[base + row * 17 : base + row * 17 + 16, :]
        window = pl.ds(part * 512, 512)
        copies.append(pltpu.make_async_copy(made.at[window], out_ref.at[window], sem.at[part]))
        copies[-1].start()
    for copy in copies:
        copy.wait()


def vm():
    return pl.BlockSpec(memory_space=VMEM)


def sm():
    return pl.BlockSpec(memory_space=SMEM)


def shaped(shape, dtype=F32):
    return VMEM(shape, dtype)


def plain(shape, dtype=F32):
    return jax.ShapeDtypeStruct(shape, dtype)


def near(value):
    return pltpu.with_memory_space_constraint(value, VMEM)


def away(value):
    return pltpu.with_memory_space_constraint(value, HBM)


GRANT = pltpu.CompilerParams(vmem_limit_bytes=24 * 1024 * 1024)


def exchange(flat, rows):
    blocks = flat.reshape(DEVS, rows, 1, LANES)
    return lax.all_to_all(blocks, AXES, split_axis=0, concat_axis=0, tiled=True).reshape(flat.shape)


def body(old_state, dest_row, neighbours, orientation, wall_flags, bulk_modulus, density):
    me = (lax.axis_index("grp") * lax.axis_size("dev") + lax.axis_index("dev")).astype(I32).reshape(1)
    dest = dest_row.reshape(2, LANES)
    bulk = away(bulk_modulus.reshape(1, LANES))
    dens = away(density.reshape(1, LANES))
    nbr, wall, orient = away(neighbours), away(wall_flags), away(orientation)
    state = old_state.reshape(256, 4, 4, LANES).transpose(0, 2, 1, 3).reshape(4096, LANES)

    info, pos, zed = pl.pallas_call(
        order_kernel,
        in_specs=[sm()] + [vm()] * 5,
        out_specs=[vm()] * 3,
        out_shape=[
            shaped((384, LANES), I32),
            shaped((2, LANES), I32),
            shaped((8, LANES)),
        ],
        scratch_shapes=[pltpu.VMEM((8, LANES), F32)],
        name="order",
        compiler_params=GRANT,
    )(me, away(dest), nbr, wall, bulk, dens)
    heard = exchange(info, 3)
    pieces = pl.pallas_call(
        pack_kernel,
        in_specs=[sm(), pl.BlockSpec(memory_space=pl.ANY), vm()],
        out_specs=pl.BlockSpec(memory_space=pl.ANY),
        out_shape=HBM((4224, LANES), F32),
        scratch_shapes=[
            pltpu.VMEM((4096, LANES), F32),
            pltpu.VMEM((4224, LANES), F32),
            pltpu.SemaphoreType.DMA((4,)),
            pltpu.SemaphoreType.DMA((8,)),
        ],
        name="pack",
        compiler_params=GRANT,
    )(pos.reshape(256), away(state), near(zed))
    spread = exchange(pieces, 33)
    spots, owners, blocks, labels, cols, index, far, close, place = pl.pallas_call(
        table_kernel,
        in_specs=[sm()] + [vm()] * 6,
        out_specs=[vm()] * 9,
        out_shape=[
            shaped((24, LANES), I32),
            shaped((8, LANES), I32),
            shaped((LANES, LANES)),
            shaped((LANES, LANES), I32),
            shaped((LANES, LANES)),
            shaped((384, LANES), I32),
            shaped((384, 2 * LANES), BF16),
            shaped((384, 2 * LANES), BF16),
            shaped((LANES, LANES), BF16),
        ],
        scratch_shapes=[pltpu.VMEM((LANES, LANES), I32), pltpu.VMEM((8, LANES), F32)],
        name="table",
        compiler_params=GRANT,
    )(me, near(heard), nbr, wall, orient, bulk, dens)
    owners = owners.reshape(1024)
    passed, zed_out = pl.pallas_call(
        forward_kernel,
        in_specs=[sm()] * 3 + [vm()] * 4,
        out_specs=[vm()] * 2,
        out_shape=[shaped((2432, LANES)), shaped((384, LANES))],
        scratch_shapes=[pltpu.VMEM((2176, LANES), F32)],
        name="forward",
        compiler_params=GRANT,
    )(me, spots.reshape(3072), owners, near(spread), near(labels), near(blocks), near(cols))
    arrived = exchange(passed, 19)
    result = pl.pallas_call(
        final_kernel,
        in_specs=[vm()] * 10,
        out_specs=pl.BlockSpec(memory_space=pl.ANY),
        out_shape=plain((2048, LANES)),
        scratch_shapes=[
            pltpu.VMEM((2048, LANES), F32),
            pltpu.VMEM((LANES, LANES), F32),
            pltpu.VMEM((384, LANES), F32),
            pltpu.VMEM((2176, LANES), F32),
            pltpu.VMEM((2048, LANES), F32),
            pltpu.SemaphoreType.DMA((4,)),
        ],
        name="final",
        compiler_params=GRANT,
    )(
        near(arrived), near(place), near(cols), near(zed_out), near(close), near(far), near(index),
        jnp.asarray(SIDE3), jnp.asarray(STACKED3), jnp.asarray(COEF),
    )
    return result.reshape(128, 4, 4, LANES).transpose(0, 2, 1, 3).reshape(128, 4, 512)


def solution(mesh):
    both = P(AXES)
    faces = P(None, AXES)
    in_specs = (P(AXES, None, None), both, faces, faces, faces, both, both)
    return jax.shard_map(
        body, mesh=mesh, in_specs=in_specs, out_specs=P(AXES, None, None), check_vma=False
    )
```

```python
import jax
import jax.numpy as jnp
import numpy as np
from jax import lax
from jax.experimental import pallas as pl
from jax.experimental.pallas import tpu as pltpu
from jax.sharding import PartitionSpec as P

NP = 8
DEVS = 128
LANES = 128
AXES = ("grp", "dev")
metric_scale = 0.25
F32 = jnp.float32
I32 = jnp.int32
BF16 = jnp.bfloat16
VMEM = pltpu.MemorySpace.VMEM
SMEM = pltpu.MemorySpace.SMEM
HBM = pltpu.MemorySpace.HBM


def gll_tables(poly_order):
    num_points = poly_order + 1
    points = -np.cos(np.pi * np.arange(num_points) / poly_order)
    legendre = np.zeros((num_points, num_points))
    for sweeps in range(101):
        legendre[:, 0] = 1.0
        legendre[:, 1] = points
        for degree in range(2, num_points):
            legendre[:, degree] = (
                (2 * degree - 1) * points * legendre[:, degree - 1]
                - (degree - 1) * legendre[:, degree - 2]
            ) / degree
        if sweeps < 100:
            points = points - (points * legendre[:, poly_order] - legendre[:, poly_order - 1]) / (
                num_points * legendre[:, poly_order]
            )
    end_values = legendre[:, poly_order]
    weights = 2.0 / (poly_order * num_points * end_values**2)
    distance = points[:, None] - points[None, :] + np.eye(num_points)
    derivative = end_values[:, None] / end_values[None, :] / distance
    derivative = derivative * (1.0 - np.eye(num_points))
    derivative[0, 0] = -poly_order * num_points / 4.0
    derivative[poly_order, poly_order] = poly_order * num_points / 4.0
    return (points, weights, derivative)


POINTS, WEIGHTS, DERIV = gll_tables(NP - 1)
DERIV = DERIV.astype(np.float32)
LIFT = metric_scale / float(WEIGHTS[0])


def derivative_tables():
    eye2, eye8 = np.eye(2, dtype=np.float32), np.eye(8, dtype=np.float32)
    along_y = np.kron(eye2, np.kron(DERIV.T, eye8))
    along_z = np.kron(eye2, np.kron(eye8, DERIV.T))
    side = np.concatenate([along_y, along_z], axis=1)
    stacked = np.concatenate([along_y, along_z], axis=0)
    coef = np.zeros((4, 4, 2, LANES), np.float32)
    for out_chunk in range(4):
        for in_chunk in range(4):
            for half in range(2):
                lanes = slice(64 * half, 64 * half + 64)
                coef[out_chunk, in_chunk, 0, lanes] = DERIV[2 * out_chunk + half, 2 * in_chunk + half]
                coef[out_chunk, in_chunk, 1, lanes] = DERIV[
                    2 * out_chunk + half, 2 * in_chunk + 1 - half
                ]
    return side, stacked, coef.reshape(32, LANES)


SIDE, STACKED, COEF = derivative_tables()


def six_parts(table):
    high = table.astype(jnp.bfloat16)
    rest = table - high.astype(np.float32)
    middle = rest.astype(jnp.bfloat16)
    low = (rest - middle.astype(np.float32)).astype(jnp.bfloat16)
    return np.concatenate([high, high, high, middle, middle, low], axis=0)


SIDE6, STACKED6 = six_parts(SIDE), six_parts(STACKED)


def iota(shape, axis):
    return lax.broadcasted_iota(I32, shape, axis)


def small_dot(left, right):
    return jnp.dot(left.astype(BF16), right.astype(BF16), preferred_element_type=F32)


def split3(value):
    high = value.astype(BF16)
    rest = value - high.astype(F32)
    middle = rest.astype(BF16)
    low = (rest - middle.astype(F32)).astype(BF16)
    return high, middle, low


def pick_dot(pick, value):
    pick = pick.astype(BF16)
    high, middle, low = split3(value)
    total = jnp.dot(pick, high, preferred_element_type=F32)
    total = total + jnp.dot(pick, middle, preferred_element_type=F32)
    return total + jnp.dot(pick, low, preferred_element_type=F32)


def column(row, diag):
    wide = jnp.broadcast_to(row, (LANES, LANES))
    return jnp.sum(jnp.where(diag, wide, 0.0), axis=1, keepdims=True)


def half_sign(shape):
    return jnp.where(iota(shape, 1) < 64, -1.0, 1.0)


def face_pair(chunk, axis, zed):
    lane = iota((LANES, LANES), 1)
    half, face_i, face_b = lane >> 6, (lane >> 3) & 7, lane & 7
    from_y = (face_i & 1) * 64 + half * 56 + face_b
    from_z = (face_i & 1) * 64 + face_b * 8 + half * 7
    values = []
    for field in (0, 1 + axis):
        if axis == 0:
            value = jnp.where(lane < 64, chunk(field, 0), chunk(field, 3))
        else:
            index = from_y if axis == 1 else from_z
            value = jnp.take_along_axis(chunk(field, 0), index, axis=1)
            for n4 in range(1, 4):
                other = jnp.take_along_axis(chunk(field, n4), index, axis=1)
                value = jnp.where(face_i >> 1 == n4, other, value)
        values.append(value)
    normal = half_sign((LANES, LANES)) * values[1]
    return values[0], normal, values[0] + zed * normal


def cross(arrays, bit1, bit0):
    first = [jnp.where(bit0, arrays[t ^ 1], arrays[t]) for t in range(4)]
    return [jnp.where(bit1, first[t ^ 2], first[t]) for t in range(4)]


def lane_bit(lane, bit):
    return ((lane >> bit) & 1) == 1


def regroup(arrays, back):
    lane = iota(arrays[0].shape, 1)
    own = (lane >> 3) & 3
    plain = (lane_bit(lane, 1), lane_bit(lane, 0))
    mixed = (lane_bit(lane ^ (lane >> 3), 1), lane_bit(lane ^ (lane >> 3), 0))
    enter, leave = (plain, mixed) if back else (mixed, plain)
    result = [None] * 16
    for top in range(4):
        four = cross(arrays[4 * top : 4 * top + 4], *enter)
        four = [jnp.take_along_axis(four[t], lane ^ t ^ own, axis=1) for t in range(4)]
        result[4 * top : 4 * top + 4] = cross(four, *leave)
    j2, k2 = lane_bit(lane, 5), lane_bit(lane, 2)
    final = [None] * 16
    for t in range(4):
        final[t::4] = cross(result[t::4], j2, k2)
    return final


def order_kernel(
    me_ref, dest_ref, nbr_ref, wall_ref, bulk_ref, dens_ref, info_ref, pos_ref, zed_ref, scr
):
    zed_ref[...] = jnp.broadcast_to(jnp.sqrt(bulk_ref[...] * dens_ref[...]), (8, LANES))
    dest = dest_ref[...]
    sub = iota((LANES, LANES), 0)
    lane = iota((LANES, LANES), 1)
    diag = sub == lane
    key_row, key_col, dest_col = [], [], []
    for half in range(2):
        row = jnp.broadcast_to(dest[half : half + 1, :], (LANES, LANES))
        key = (row >> 7).astype(F32) * 256.0 + (lane + 128 * half).astype(F32)
        key_row.append(key)
        key_col.append(jnp.sum(jnp.where(diag, key, 0.0), axis=1, keepdims=True))
        dest_col.append(jnp.sum(jnp.where(diag, row.astype(F32), 0.0), axis=1, keepdims=True))
    lists = [jnp.zeros((1, LANES), F32), jnp.zeros((1, LANES), F32)]
    for half in range(2):
        before_col = jnp.zeros((LANES, 1), F32)
        before_row = jnp.zeros((1, LANES), F32)
        for other in range(2):
            before_col = before_col + jnp.sum(
                jnp.where(key_row[other] < key_col[half], 1.0, 0.0), axis=1, keepdims=True
            )
            before_row = before_row + jnp.sum(
                jnp.where(key_col[other] < key_row[half], 1.0, 0.0), axis=0, keepdims=True
            )
        spot = before_row.astype(I32)
        spot = (spot & 7) * 528 + (spot >> 3)
        pos_ref[half : half + 1, :] = jnp.where(dest[half : half + 1, :] >= 0, spot, -1)
        place = before_col.astype(I32)
        k = place & 7
        spot = (k & 3) * 32 + (place >> 3)
        for part in range(2):
            hit = (spot == lane) & (k >> 2 == part)
            lists[part] = lists[part] + jnp.sum(jnp.where(hit, dest_col[half], 0.0), axis=0, keepdims=True)
    scr[...] = jnp.full((8, LANES), -1.0, F32)
    owner = nbr_ref[...] >> 7
    remote = (owner != me_ref[0]) & (wall_ref[...] == 0)
    scr[0:6, :] = jnp.where(remote, owner, -1).astype(F32)
    owners = jnp.max(scr[...], axis=1, keepdims=True)
    spread = iota((8, LANES), 0) == iota((8, LANES), 1)
    owner_row = jnp.sum(jnp.where(spread, owners, 0.0), axis=0, keepdims=True)
    for part, row in enumerate((lists[0], lists[1], owner_row)):
        info_ref[pl.ds(part, LANES, stride=3), :] = jnp.broadcast_to(row, (LANES, LANES)).astype(I32)


def pack_kernel(pos_ref, state_ref, zed_ref, out_ref, rows, made, in_sem, out_sem):
    full = pos_ref[0] >= 0
    loads = []
    for part in range(4):
        window = pl.ds(part * 1024, 1024)
        loads.append(pltpu.make_async_copy(state_ref.at[window], rows.at[window], in_sem.at[part]))

    @pl.when(full)
    def _():
        for load in loads:
            load.start()

    made[pl.ds(32, LANES, stride=33), :] = jnp.broadcast_to(zed_ref[0:1, :], (LANES, LANES))

    @pl.when(full)
    def _():
        def one(slot, carry):
            made[pl.ds(pos_ref[slot], 16, stride=33), :] = rows[pl.ds(pl.multiple_of(slot * 16, 16), 16), :]
            return carry

        for part in range(4):
            loads[part].wait()
            lax.fori_loop(part * 64, part * 64 + 64, one, 0, unroll=16)

    stores = []
    for k in range(8):

        @pl.when(full)
        def _():
            for block in range(4):
                at = [(k * 16 + c) * 33 + block * 8 for c in range(16)]
                groups = regroup([made[a : a + 8, :] for a in at], False)
                for g in range(16):
                    made[at[g] : at[g] + 8, :] = groups[g]

        window = pl.ds(k * 528, 528)
        stores.append(pltpu.make_async_copy(made.at[window], out_ref.at[window], out_sem.at[k]))
        stores[-1].start()
    for store in stores:
        store.wait()


def table_kernel(
    me_ref, info_ref, nbr_ref, wall_ref, orient_ref, bulk_ref, dens_ref,
    spot_ref, owner_ref, column_ref, label_ref, cols_ref, index_ref, hot_ref, near_ref, place_ref, wide, scr,
):
    shape = (LANES, LANES)
    sub = iota(shape, 0)
    lane = iota(shape, 1)
    diag = sub == lane
    me = me_ref[0]
    bulk = column(bulk_ref[...], diag)
    dens = column(dens_ref[...], diag)
    zed = column(jnp.sqrt(bulk_ref[...] * dens_ref[...]), diag)
    cols = jnp.where(lane == 0, zed, jnp.where(lane == 1, bulk, dens))

    lists = [info_ref[pl.ds(0, LANES, stride=3), :], info_ref[pl.ds(1, LANES, stride=3), :]]
    owners = info_ref[pl.ds(2, LANES, stride=3), :].astype(F32)
    owner_ref[...] = owners.T[0:8, :].astype(I32)
    column_ref[...] = owners
    target = lists[0] >> 7
    my_k = me >> 4
    mine = jnp.where(my_k >= 4, lists[1], lists[0])
    mine = jnp.take_along_axis(mine, (my_k & 3) * 32 + (lane & 31), axis=1) & 127
    present = jnp.zeros(shape, F32)
    label = jnp.zeros(shape, F32)
    mine = mine.astype(F32)
    for j in range(32):
        hit = target[:, j : j + 1] == lane
        present = jnp.where(hit, 1.0, present)
        label = jnp.where(hit, mine[:, j : j + 1], label)
    below = jnp.where(lane < sub, 1.0, 0.0)
    rank = small_dot(below, present)
    safe = jnp.clip(target, 0, LANES - 1)
    slot = safe * 17 + jnp.take_along_axis(rank.astype(I32), safe, axis=1)
    is_source = jnp.broadcast_to(jnp.where(target[:, 0:1] >= 0, 1.0, 0.0), shape)
    source_rank = jnp.where(is_source > 0.0, small_dot(below, is_source), -1.0)
    chosen = jnp.where(source_rank.T == sub.astype(F32), 1.0, 0.0)
    wide[...] = pick_dot(chosen, jnp.where(lane == 32, sub, slot).astype(F32)).astype(I32)
    quarter = iota((16, LANES), 1) >> 5
    spots = wide[pl.ds(0, 16, stride=4), :]
    for part in range(1, 4):
        moved = pltpu.roll(wide[pl.ds(part, 16, stride=4), :], 32 * part, 1)
        spots = jnp.where(quarter == part, moved, spots)
    spot_ref[0:16, :] = spots
    sources = jnp.where(diag, jnp.broadcast_to(wide[:, 32:33], shape).astype(F32), 0.0)
    sources = jnp.sum(sources, axis=0, keepdims=True).astype(I32)
    spot_ref[16:24, :] = jnp.broadcast_to(sources, (8, LANES))
    order = jnp.where(present > 0.0, rank, -1.0)
    labels = jnp.zeros(shape, F32)
    for i in range(16):
        row = jnp.sum(jnp.where(order == float(i), label, 0.0), axis=0, keepdims=True)
        labels = jnp.where(sub == i, row, labels)
    label_ref[...] = labels.T.astype(I32)

    gather = [jnp.where((sub >> 5) + 4 * part == lane >> 4, 1.0, 0.0) for part in range(2)]

    def rows_of(block):
        value = jnp.zeros(shape, F32)
        for part in range(2):
            held = jnp.where(lists[part] >> 7 == block, (lists[part] & 127).astype(F32), 0.0)
            value = value + small_dot(held, gather[part])
        source = jnp.sum(jnp.where(lane == block, order, 0.0), axis=1, keepdims=True)
        chosen = source == (lane & 15).astype(F32)
        return jnp.sum(jnp.where(chosen, value, 0.0), axis=0, keepdims=True)

    place_ref[...] = jnp.where(rows_of(me) == sub.astype(F32), 1.0, 0.0).astype(BF16)
    scr[...] = jnp.full((8, LANES), -1.0, F32)
    nbr_all = nbr_ref[...]
    away_all = ((nbr_all >> 7) != me) & (wall_ref[...] == 0)
    scr[0:6, :] = jnp.where(away_all, nbr_all >> 7, -1).astype(F32)
    neighbour = jnp.max(scr[...], axis=1, keepdims=True).astype(I32)
    low_half = lane < 64
    for axis in range(3):
        rows = slice(axis * LANES, axis * LANES + LANES)
        codes, aways = [], []
        for side in range(2):
            face = 2 * axis + side
            nbr = nbr_ref[face : face + 1, :]
            is_wall = wall_ref[face : face + 1, :] == 1
            remote = ((nbr >> 7) != me) & jnp.logical_not(is_wall)
            wanted = column(jnp.where(remote, nbr & 127, -1).astype(F32), diag)
            hit = rows_of(neighbour[face : face + 1, :]) == wanted
            hot_ref[rows, side * LANES : (side + 1) * LANES] = jnp.where(hit, 1.0, 0.0).astype(BF16)
            codes.append(column(orient_ref[face : face + 1, :].astype(F32), diag).astype(I32))
            aways.append(wanted)
            wall = column(jnp.where(is_wall, 1.0, 0.0), diag) > 0.0
            spot = column((nbr & 127).astype(F32), diag)
            far = wanted >= 0.0
            local = jnp.where(far | wall, 0.0, jnp.where(spot == lane.astype(F32), 1.0, 0.0))
            near_ref[rows, side * LANES : (side + 1) * LANES] = local.astype(BF16)
            cols = jnp.where(lane == 8 + face, spot, cols)
            cols = jnp.where(lane == 16 + face, jnp.where(wall, -1.0, jnp.where(far, 1.0, 0.0)), cols)
        code = jnp.where(low_half, codes[0], codes[1])
        a, b = (lane >> 3) & 7, lane & 7
        swap = code >= 4
        a1, b1 = jnp.where(swap, b, a), jnp.where(swap, a, b)
        a2 = jnp.where((code & 1) == 1, 7 - a1, a1)
        b2 = jnp.where((code & 2) == 2, 7 - b1, b1)
        h = jnp.where(low_half, 1, 0)
        if axis == 0:
            top = ((a2 >> 2) ^ h) * 8 + ((b2 >> 2) ^ h) * 4
            group, v = top + ((a2 ^ b2) & 3), a2 & 3
        elif axis == 1:
            top = ((a2 >> 2) ^ h) * 8 + (((a2 >> 1) & 1) ^ (b2 >> 2)) * 4
            group, v = top + ((b2 & 3) ^ (h * 3)), (a2 & 1) * 2 + (b2 >> 2)
        else:
            top = ((a2 >> 2) ^ (b2 >> 2)) * 8 + (((a2 >> 1) & 1) ^ h) * 4
            group, v = top + ((b2 & 3) ^ (h * 3)), (a2 & 1) * 2 + (b2 >> 2)
        is_far = jnp.where(low_half, aways[0], aways[1]) >= 0.0
        index_ref[rows, :] = h * 64 + jnp.where(is_far, v * 16 + group, a2 * 8 + b2)
    cols_ref[...] = cols


SHIFT_A, SHIFT_B = (3, 9)


def shift_of(i):
    return (i & 3) ^ ((i >> 2) & 1) * (4 * SHIFT_A) ^ (i >> 3) * (4 * SHIFT_B)


def forward_kernel(me_ref, spot_ref, owner_ref, in_ref, label_ref, column_ref, cols_ref, out_ref, zed_ref, held):
    for number in range(DEVS // 2):
        start = spot_ref[2048 + number] * 33
        for j in range(32):
            held[pl.ds(spot_ref[number * 32 + j], 1), :] = in_ref[pl.ds(start + j, 1), :]
    shape = (LANES, LANES)
    lane = iota(shape, 1)
    zeds = in_ref[pl.ds(32, LANES, stride=33), :]
    me = me_ref[0]
    own = in_ref[pl.ds(me * 33 + 32, 1), :]
    for axis in range(3):
        values = []
        for face in (2 * axis, 2 * axis + 1):
            other = in_ref[pl.ds(jnp.maximum(owner_ref[face * LANES + me], 0) * 33 + 32, 1), :]
            kind = cols_ref[:, 16 + face : 17 + face]
            hit = cols_ref[:, 8 + face : 9 + face] == lane.astype(F32)
            value = jnp.where(hit, jnp.where(kind > 0.0, other, own), 0.0)
            values.append(jnp.where(kind < 0.0, -1.0, jnp.sum(value, axis=1, keepdims=True)))
        zed_ref[axis * LANES : axis * LANES + LANES, :] = jnp.where(lane < 64, values[0], values[1])
    zed = jnp.take_along_axis(zeds, label_ref[...], axis=1)
    me = me_ref[0]
    g3, g2, g1, g0 = (me >> 3) & 1, (me >> 2) & 1, (me >> 1) & 1, me & 1
    lane = iota((8, LANES), 1)
    h, v1, v0 = lane >> 6, (lane >> 1) & 1, lane & 1
    nodes = [
        h * 16 + (g3 ^ h) * 8 + v1 * 4 + v0 * 2 + (g2 ^ h),
        v1 * 16 + h * 14 + v0,
        v1 * 16 + v0 * 8 + (g1 ^ h) * 4 + (g0 ^ h) * 2 + h,
    ]
    here = (lane >> 2) & 15
    shift = (here & 3) ^ ((here >> 2) & 1) * (4 * SHIFT_A) ^ (here >> 3) * (4 * SHIFT_B)
    which = []
    for axis in range(3):
        for field in (0, 1 + axis):
            value = jnp.full((8, LANES), -1, I32)
            for i in range(16):
                spot = lane ^ shift_of(i)
                n = spot >> 2
                i0, j2, j1, j0, k2 = (n >> 4) & 1, (n >> 3) & 1, (n >> 2) & 1, (n >> 1) & 1, n & 1
                if axis == 0:
                    hit = (j2 == g3 ^ i0) & (k2 == g2 ^ i0)
                elif axis == 1:
                    hit = (j2 == j1) & (j1 == j0)
                else:
                    hit = (j1 == g1 ^ k2) & (j0 == g0 ^ k2)
                value = jnp.where(hit & (spot & 3 == field), i, value)
            which.append(value)
    sign = half_sign((8, LANES))
    waves = [[], [], []]
    for quad in range(4):
        blocks = range(quad * 4, quad * 4 + 4)
        merged = [[jnp.zeros((8, LANES), F32)] * 6 for _ in blocks]
        for i in range(16):
            hits = [which[m] == i for m in range(6)]
            for b, block in enumerate(blocks):
                rows = held[pl.ds(block * 136 + i, 8, stride=17), :]
                rows = jnp.take_along_axis(rows, lane ^ shift_of(i), axis=1)
                merged[b] = [jnp.where(hits[m], rows, merged[b][m]) for m in range(6)]
        wide = [
            jnp.take_along_axis(zed[block * 8 : block * 8 + 8, :], here, axis=1) * sign for block in blocks
        ]
        for axis in range(3):
            at = (nodes[axis] * 4) ^ shift
            press = [jnp.take_along_axis(merged[b][2 * axis], at, axis=1) for b in range(4)]
            at = (nodes[axis] * 4 + 1 + axis) ^ shift
            speed = [jnp.take_along_axis(merged[b][2 * axis + 1], at, axis=1) for b in range(4)]
            waves[axis] += [press[b] + wide[b] * speed[b] for b in range(4)]
    low_half = iota(shape, 1) < 64
    lane = iota(shape, 1).astype(F32)
    halos = []
    for axis in range(3):
        wave = jnp.concatenate(waves[axis], axis=0)
        upper = column_ref[:, 2 * axis + 1 : 2 * axis + 2] == lane
        lower = column_ref[:, 2 * axis : 2 * axis + 1] == lane
        pick = jnp.concatenate([jnp.where(upper, 1.0, 0.0), jnp.where(lower, 1.0, 0.0)], axis=1)
        table = jnp.concatenate([jnp.where(low_half, wave, 0.0), jnp.where(low_half, 0.0, wave)], axis=0)
        halos.append(pick_dot(pick, table))
    for target in range(DEVS):
        out_ref[target * 19 : target * 19 + 16, :] = held[target * 17 : target * 17 + 16, :]
    for axis in range(3):
        out_ref[pl.ds(16 + axis, LANES, stride=19), :] = halos[axis]


def exchange_lanes(arrays):
    lane = iota(arrays[0].shape, 1)
    bits = (lane_bit(lane, 6), lane_bit(lane, 5), lane_bit(lane, 4))

    def mix(eight):
        for step, bit in zip((1, 2, 4), bits[::-1]):
            eight = [jnp.where(bit, eight[t ^ step], eight[t]) for t in range(8)]
        return eight

    turned = mix(arrays)
    turned = [jnp.take_along_axis(turned[t], lane ^ (t * 16), axis=1) for t in range(8)]
    return mix(turned)


def final_kernel(
    in_ref, place_ref, cols_ref, zed_ref, near_ref, far_ref, index_ref, side_ref, stack_ref, coef_ref,
    out_ref, state, turned, lift, loose, made, sem,
):
    shape = (LANES, LANES)
    lane = iota(shape, 1)
    low_half = lane < 64
    place = place_ref[...]
    place = jnp.concatenate([place, place, place], axis=1)
    for group in range(0, 16, 2):
        pair = []
        for g in (group, group + 1):
            rows = [in_ref[(k * 16 + g) * 19 : (k * 16 + g) * 19 + 16, :] for k in range(8)]
            pair.append(jnp.concatenate(rows, axis=0))
        parts = split3(jnp.concatenate(pair, axis=1))
        moved = jnp.dot(place, jnp.concatenate(parts, axis=0), preferred_element_type=F32)
        state[group * LANES : (group + 1) * LANES, :] = moved[:, 0:LANES]
        state[(group + 1) * LANES : (group + 2) * LANES, :] = moved[:, LANES:]
    for block in range(16):
        at = [c * LANES + block * 8 for c in range(16)]
        chunks = regroup([state[a : a + 8, :] for a in at], True)
        for c in range(16):
            state[at[c] : at[c] + 8, :] = chunks[c]

    def chunk(field, n4):
        start = (n4 * 4 + field) * LANES
        return state[start : start + LANES, :]

    zed = cols_ref[:, 0:1]
    for axis in range(3):
        rows = slice(axis * LANES, axis * LANES + LANES)
        press, norm, wave = face_pair(chunk, axis, zed)
        turned[...] = in_ref[pl.ds(16 + axis, LANES, stride=19), :].T
        parts = [turned[pl.ds(h * 64 + v, 16, stride=4), :] for h in range(2) for v in range(4)]
        far = jnp.concatenate(exchange_lanes(parts), axis=0)
        masked = []
        for value in (wave, far):
            masked.append(jnp.where(low_half, 0.0, value))
            masked.append(jnp.where(low_half, value, 0.0))
        hot = [near_ref[rows, :], far_ref[rows, :]]
        both = jnp.dot(
            jnp.concatenate(hot * 3, axis=1),
            jnp.concatenate(split3(jnp.concatenate(masked, axis=0)), axis=0),
            preferred_element_type=F32,
        )
        wave_out = jnp.take_along_axis(both, index_ref[rows, :], axis=1)
        zed_out = zed_ref[rows, :]
        jump = (wave_out - press + zed_out * norm) / (zed + zed_out)
        lift[rows, :] = jnp.where(zed_out < 0.0, norm, jump)

    lane = iota((64, LANES), 1)
    low_half = lane < 64
    i2, j, k = lane >> 6, (lane >> 3) & 7, lane & 7
    on_y, on_z = (j == 0) | (j == 7), (k == 0) | (k == 7)
    copies = []
    for part in range(2):
        rows = slice(part * 64, part * 64 + 64)
        zed, bulk, dens = cols_ref[rows, 0:1], cols_ref[rows, 1:2], cols_ref[rows, 2:3]
        by_bulk = -metric_scale * bulk
        by_dens = -(metric_scale / dens)
        up = LIFT * bulk
        across = -LIFT * zed / dens
        piece = {}
        for field in range(4):
            for n4 in range(4):
                start = (n4 * 4 + field) * LANES + part * 64
                piece[field, n4] = state[start : start + 64, :]
        cut = []
        for fields in ((0,), (2, 3)):
            whole = [jnp.concatenate([piece[field, n4] for n4 in range(4)], axis=0) for field in fields]
            high, middle, low = split3(jnp.concatenate(whole, axis=1))
            cut.append(jnp.concatenate([high, middle, low, high, middle, high], axis=1))
        grad = jnp.dot(cut[0], side_ref[...], preferred_element_type=F32)
        across_div = jnp.dot(cut[1], stack_ref[...], preferred_element_type=F32)
        swapped = {}
        for field in (0, 1):
            for n4 in range(4):
                swapped[field, n4] = pltpu.roll(piece[field, n4], 64, 1)
        jumps = [lift[axis * LANES + part * 64 : axis * LANES + part * 64 + 64, :] for axis in range(3)]
        base = part * 1088
        for n4 in range(4):
            along = {}
            for field in (0, 1):
                total = None
                for m4 in range(4):
                    at = (n4 * 4 + m4) * 2
                    term = piece[field, m4] * coef_ref[at : at + 1, :]
                    term = term + swapped[field, m4] * coef_ref[at + 1 : at + 2, :]
                    total = term if total is None else total + term
                along[field] = total
            block = slice(n4 * 64, n4 * 64 + 64)
            div = along[1] + across_div[block, :]
            grads = [along[0], grad[block, 0:LANES], grad[block, LANES:]]
            face_i = 2 * n4 + i2
            from_y = jnp.where(j == 7, 64, 0) + face_i * 8 + k
            from_z = jnp.where(k == 7, 64, 0) + face_i * 8 + j
            total = None
            for axis in range(3):
                jump = jumps[axis]
                value = by_dens * grads[axis]
                here = None
                if axis == 0 and n4 == 0:
                    here = jnp.where(low_half, jump, 0.0)
                    turn = -here
                elif axis == 0 and n4 == 3:
                    here = jnp.where(low_half, 0.0, jump)
                    turn = here
                elif axis == 1:
                    here = jnp.where(on_y, jnp.take_along_axis(jump, from_y, axis=1), 0.0)
                    turn = jnp.where(j == 0, -here, here)
                elif axis == 2:
                    here = jnp.where(on_z, jnp.take_along_axis(jump, from_z, axis=1), 0.0)
                    turn = jnp.where(k == 0, -here, here)
                if here is not None:
                    value = value + across * turn
                    total = here if total is None else total + here
                loose[pl.ds(base + n4 * 4 + 1 + axis, 64, stride=17), :] = value
            loose[pl.ds(base + n4 * 4, 64, stride=17), :] = by_bulk * div + up * total
        for row in range(64):
            at = (part * 64 + row) * 16
            made[at : at + 16, :] = loose[base + row * 17 : base + row * 17 + 16, :]
        window = pl.ds(part * 1024, 1024)
        copies.append(pltpu.make_async_copy(made.at[window], out_ref.at[window], sem.at[part]))
        copies[-1].start()
    for copy in copies:
        copy.wait()


def vm():
    return pl.BlockSpec(memory_space=VMEM)


def sm():
    return pl.BlockSpec(memory_space=SMEM)


def shaped(shape, dtype=F32):
    return VMEM(shape, dtype)


def plain(shape, dtype=F32):
    return jax.ShapeDtypeStruct(shape, dtype)


def near(value):
    return pltpu.with_memory_space_constraint(value, VMEM)


def away(value):
    return pltpu.with_memory_space_constraint(value, HBM)


GRANT = pltpu.CompilerParams(vmem_limit_bytes=24 * 1024 * 1024)


def exchange(flat, rows):
    blocks = flat.reshape(DEVS, rows, 1, LANES)
    return lax.all_to_all(blocks, AXES, split_axis=0, concat_axis=0, tiled=True).reshape(flat.shape)


def body(old_state, dest_row, neighbours, orientation, wall_flags, bulk_modulus, density):
    me = (lax.axis_index("grp") * lax.axis_size("dev") + lax.axis_index("dev")).astype(I32).reshape(1)
    dest = dest_row.reshape(2, LANES)
    bulk = away(bulk_modulus.reshape(1, LANES))
    dens = away(density.reshape(1, LANES))
    nbr, wall, orient = away(neighbours), away(wall_flags), away(orientation)
    state = old_state.reshape(256, 4, 4, LANES).transpose(0, 2, 1, 3).reshape(4096, LANES)

    info, pos, zed = pl.pallas_call(
        order_kernel,
        in_specs=[sm()] + [vm()] * 5,
        out_specs=[vm()] * 3,
        out_shape=[
            shaped((384, LANES), I32),
            shaped((2, LANES), I32),
            shaped((8, LANES)),
        ],
        scratch_shapes=[pltpu.VMEM((8, LANES), F32)],
        name="order",
        compiler_params=GRANT,
    )(me, away(dest), nbr, wall, bulk, dens)
    heard = exchange(info, 3)
    pieces = pl.pallas_call(
        pack_kernel,
        in_specs=[sm(), pl.BlockSpec(memory_space=pl.ANY), vm()],
        out_specs=pl.BlockSpec(memory_space=pl.ANY),
        out_shape=HBM((4224, LANES), F32),
        scratch_shapes=[
            pltpu.VMEM((4096, LANES), F32),
            pltpu.VMEM((4224, LANES), F32),
            pltpu.SemaphoreType.DMA((4,)),
            pltpu.SemaphoreType.DMA((8,)),
        ],
        name="pack",
        compiler_params=GRANT,
    )(pos.reshape(256), away(state), near(zed))
    spread = exchange(pieces, 33)
    spots, owners, blocks, labels, cols, index, far, close, place = pl.pallas_call(
        table_kernel,
        in_specs=[sm()] + [vm()] * 6,
        out_specs=[vm()] * 9,
        out_shape=[
            shaped((24, LANES), I32),
            shaped((8, LANES), I32),
            shaped((LANES, LANES)),
            shaped((LANES, LANES), I32),
            shaped((LANES, LANES)),
            shaped((384, LANES), I32),
            shaped((384, 2 * LANES), BF16),
            shaped((384, 2 * LANES), BF16),
            shaped((LANES, LANES), BF16),
        ],
        scratch_shapes=[pltpu.VMEM((LANES, LANES), I32), pltpu.VMEM((8, LANES), F32)],
        name="table",
        compiler_params=GRANT,
    )(me, near(heard), nbr, wall, orient, bulk, dens)
    owners = owners.reshape(1024)
    passed, zed_out = pl.pallas_call(
        forward_kernel,
        in_specs=[sm()] * 3 + [vm()] * 4,
        out_specs=[vm()] * 2,
        out_shape=[shaped((2432, LANES)), shaped((384, LANES))],
        scratch_shapes=[pltpu.VMEM((2176, LANES), F32)],
        name="forward",
        compiler_params=GRANT,
    )(me, spots.reshape(3072), owners, near(spread), near(labels), near(blocks), near(cols))
    arrived = exchange(passed, 19)
    result = pl.pallas_call(
        final_kernel,
        in_specs=[vm()] * 10,
        out_specs=pl.BlockSpec(memory_space=pl.ANY),
        out_shape=plain((2048, LANES)),
        scratch_shapes=[
            pltpu.VMEM((2048, LANES), F32),
            pltpu.VMEM((LANES, LANES), F32),
            pltpu.VMEM((384, LANES), F32),
            pltpu.VMEM((2176, LANES), F32),
            pltpu.VMEM((2048, LANES), F32),
            pltpu.SemaphoreType.DMA((2,)),
        ],
        name="final",
        compiler_params=GRANT,
    )(
        near(arrived), near(place), near(cols), near(zed_out), near(close), near(far), near(index),
        jnp.asarray(SIDE6), jnp.asarray(STACKED6), jnp.asarray(COEF),
    )
    return result.reshape(128, 4, 4, LANES).transpose(0, 2, 1, 3).reshape(128, 4, 512)


def solution(mesh):
    both = P(AXES)
    faces = P(None, AXES)
    in_specs = (P(AXES, None, None), both, faces, faces, faces, both, both)
    return jax.shard_map(
        body, mesh=mesh, in_specs=in_specs, out_specs=P(AXES, None, None), check_vma=False
    )
```
